8 devices in a mesh: data: 2 (over z, y), ctx: 4 (over x, core).
Axes of the slice: x: 2, y: 2, z: 1, core: 2. Of those that a mesh axis runs over, the one named last changes fastest.
Arguments:
- hidden: bfloat16 [256, 3584], P(('data', 'ctx')), parts along dimension 0
- seq_lens: int32 [256], P(('data', 'ctx')), parts along dimension 0
- w_query: bfloat16 [16, 3584, 3584], replicated
- w_key: bfloat16 [16, 3584, 512], replicated
- w_value: bfloat16 [16, 3584, 512], replicated
- w_out: bfloat16 [16, 3584, 3584], replicated
- k_prefix: bfloat16 [16, 1024, 4, 128], P(None, ('data', 'ctx')), parts along dimension 1
- v_prefix: bfloat16 [16, 1024, 4, 128], P(None, ('data', 'ctx')), parts along dimension 1
- k_suffix: bfloat16 [16, 256, 32, 4, 128], P(None, ('data', 'ctx')), parts along dimension 1
- v_suffix: bfloat16 [16, 256, 32, 4, 128], P(None, ('data', 'ctx')), parts along dimension 1
Outputs:
- output 1: bfloat16 [256, 3584], P(('data', 'ctx')), parts along dimension 0
- output 2: bfloat16 [16, 256, 32, 4, 128], P(None, ('data', 'ctx')), parts along dimension 1
- output 3: bfloat16 [16, 256, 32, 4, 128], P(None, ('data', 'ctx')), parts along dimension 1
There are 2 independent parts. The reference program is written for one: setup_inputs(seed, part) draws one part's arguments, and reference() takes and returns one part's arrays. A program takes and returns all parts, laid end to end along the dimension named above; an argument that names none is the same for every part.
All inputs are finite; a program needn't handle non-finite values.
Results may differ from the reference program's by a relative error of at most 0.02.
Values are sent between devices in bfloat16 or wider.
A program may use at most 4 GiB of HBM per device.

```python
import jax
import jax.numpy as jnp
from jax import lax

MODEL_DIM = 3584
NUM_HEADS = 28
KV_HEADS = 4
HEAD_DIM = 128
LAYERS = 16
SHARDS = 4
BATCH_SIZE = 128
PREFIX_LEN = 512
SUFFIX_LEN = 32
HOME_ROWS = 32


def setup_inputs(seed: int = 0, part: int = 0) -> dict:
    shared_keys = jax.random.split(jax.random.key(seed), 4)
    part_keys = jax.random.split(jax.random.fold_in(jax.random.key(seed + 1), part), 10)
    q_width = NUM_HEADS * HEAD_DIM
    kv_width = KV_HEADS * HEAD_DIM
    shard_rows = PREFIX_LEN // SHARDS
    w_query = jax.random.normal(shared_keys[0], (LAYERS, MODEL_DIM, q_width), jnp.float32) * MODEL_DIM ** -0.5
    w_key = jax.random.normal(shared_keys[1], (LAYERS, MODEL_DIM, kv_width), jnp.float32) * (2.5 * MODEL_DIM ** -0.5)
    w_value = jax.random.normal(shared_keys[2], (LAYERS, MODEL_DIM, kv_width), jnp.float32) * MODEL_DIM ** -0.5
    w_out = jax.random.normal(shared_keys[3], (LAYERS, q_width, MODEL_DIM), jnp.float32) * (q_width * LAYERS) ** -0.5
    hidden = jax.random.normal(part_keys[0], (BATCH_SIZE, MODEL_DIM), jnp.float32)
    centre_shape = (LAYERS, SHARDS, 1, KV_HEADS, HEAD_DIM)
    block_shape = (LAYERS, SHARDS, shard_rows, KV_HEADS, HEAD_DIM)
    prefix_shape = (LAYERS, PREFIX_LEN, KV_HEADS, HEAD_DIM)
    k_prefix = (1.5 * jax.random.normal(part_keys[1], centre_shape, jnp.float32) + jax.random.normal(part_keys[2], block_shape, jnp.float32)).reshape(prefix_shape)
    v_prefix = (jax.random.normal(part_keys[3], centre_shape, jnp.float32) + 0.5 * jax.random.normal(part_keys[4], block_shape, jnp.float32)).reshape(prefix_shape)
    seq_centre = (LAYERS, BATCH_SIZE, 1, KV_HEADS, HEAD_DIM)
    suffix_shape = (LAYERS, BATCH_SIZE, SUFFIX_LEN, KV_HEADS, HEAD_DIM)
    k_suffix = 2.5 * jax.random.normal(part_keys[5], seq_centre, jnp.float32) + jax.random.normal(part_keys[6], suffix_shape, jnp.float32)
    v_suffix = jax.random.normal(part_keys[7], seq_centre, jnp.float32) + 0.5 * jax.random.normal(part_keys[8], suffix_shape, jnp.float32)
    len_keys = jax.random.split(part_keys[9], 2)
    seq_lens = jax.random.randint(len_keys[0], (BATCH_SIZE,), 0, SUFFIX_LEN, dtype=jnp.int32)
    longest = jax.random.randint(len_keys[1], (), 0, BATCH_SIZE, dtype=jnp.int32)
    seq_lens = seq_lens.at[longest].set(SUFFIX_LEN - 1)
    seq_lens = seq_lens.at[(longest + BATCH_SIZE // 2) % BATCH_SIZE].set(0)
    return {'hidden': hidden.astype(jnp.bfloat16), 'seq_lens': seq_lens, 'w_query': w_query.astype(jnp.bfloat16), 'w_key': w_key.astype(jnp.bfloat16), 'w_value': w_value.astype(jnp.bfloat16), 'w_out': w_out.astype(jnp.bfloat16), 'k_prefix': k_prefix.astype(jnp.bfloat16), 'v_prefix': v_prefix.astype(jnp.bfloat16), 'k_suffix': k_suffix.astype(jnp.bfloat16), 'v_suffix': v_suffix.astype(jnp.bfloat16)}


def attend_block(queries, k_pre, v_pre, k_suf, v_suf, slot_live):
    score_scale = HEAD_DIM ** -0.5
    pre_scores = jnp.einsum('bkgd,pkd->bkgp', queries, k_pre) * score_scale
    suf_scores = jnp.einsum('bkgd,bskd->bkgs', queries, k_suf) * score_scale
    suf_scores = jnp.where(slot_live[:, None, None, :], suf_scores, -jnp.inf)
    row_max = jnp.maximum(pre_scores.max(axis=-1), suf_scores.max(axis=-1))
    pre_exp = jnp.exp(pre_scores - row_max[..., None])
    suf_exp = jnp.exp(suf_scores - row_max[..., None])
    mass_sum = pre_exp.sum(axis=-1) + suf_exp.sum(axis=-1)
    mixed_sum = jnp.einsum('bkgp,pkd->bkgd', pre_exp, v_pre) + jnp.einsum('bkgs,bskd->bkgd', suf_exp, v_suf)
    return mixed_sum / mass_sum[..., None]


def reference(hidden, seq_lens, w_query, w_key, w_value, w_out, k_prefix, v_prefix, k_suffix, v_suffix):
    group_size = NUM_HEADS // KV_HEADS
    blocks = BATCH_SIZE // HOME_ROWS
    slot_ids = jnp.arange(SUFFIX_LEN, dtype=jnp.int32)[None, :]
    slot_hit = (slot_ids == seq_lens[:, None])[:, :, None, None]
    slot_live = slot_ids <= seq_lens[:, None]
    live_blocks = slot_live.reshape(blocks, HOME_ROWS, SUFFIX_LEN)

    def layer_step(hidden_state, layer_args):
        q_weight, k_weight, v_weight, o_weight, k_pre, v_pre, k_suf, v_suf = layer_args
        queries = jnp.dot(hidden_state, q_weight, preferred_element_type=jnp.float32).astype(jnp.bfloat16)
        k_new = jnp.dot(hidden_state, k_weight, preferred_element_type=jnp.float32).astype(jnp.bfloat16).reshape(BATCH_SIZE, 1, KV_HEADS, HEAD_DIM)
        v_new = jnp.dot(hidden_state, v_weight, preferred_element_type=jnp.float32).astype(jnp.bfloat16).reshape(BATCH_SIZE, 1, KV_HEADS, HEAD_DIM)
        k_suf = jnp.where(slot_hit, k_new, k_suf)
        v_suf = jnp.where(slot_hit, v_new, v_suf)
        q_blocks = queries.astype(jnp.float32).reshape(blocks, HOME_ROWS, KV_HEADS, group_size, HEAD_DIM)
        k_full = k_pre.astype(jnp.float32)
        v_full = v_pre.astype(jnp.float32)
        k_blocks = k_suf.astype(jnp.float32).reshape(blocks, HOME_ROWS, SUFFIX_LEN, KV_HEADS, HEAD_DIM)
        v_blocks = v_suf.astype(jnp.float32).reshape(blocks, HOME_ROWS, SUFFIX_LEN, KV_HEADS, HEAD_DIM)
        attended = lax.map(lambda block_args: attend_block(block_args[0], k_full, v_full, block_args[1], block_args[2], block_args[3]), (q_blocks, k_blocks, v_blocks, live_blocks))
        attended = attended.astype(jnp.bfloat16).reshape(BATCH_SIZE, NUM_HEADS * HEAD_DIM)
        update = jnp.dot(attended, o_weight, preferred_element_type=jnp.float32).astype(jnp.bfloat16)
        hidden_state = (hidden_state.astype(jnp.float32) + update.astype(jnp.float32)).astype(jnp.bfloat16)
        return hidden_state, (k_suf, v_suf)

    hidden_out, cache_out = lax.scan(layer_step, hidden, (w_query, w_key, w_value, w_out, k_prefix, v_prefix, k_suffix, v_suffix))
    return hidden_out, cache_out[0], cache_out[1]
```

```python
import functools

import jax
import jax.numpy as jnp
from jax import lax
from jax.experimental import pallas as pl
from jax.experimental.pallas import tpu as pltpu
from jax.sharding import PartitionSpec as P

MESH = pl.DeviceIdType.MESH
BF16 = jnp.bfloat16
F32 = jnp.float32
TILE = 512
CHUNK = 16
PAD = 8


def decode_kernel(dims, hidden_ref, lens_ref, wq_ref, wk_ref, wv_ref, wo_ref, pre_ref, ksuf_ref, vsuf_ref,
                  out_ref, kv_out_ref,
                  wq_buf, wk_buf, wv_buf, wo_buf, pre_buf, suf_buf, x_buf, own_buf, recv_buf, acc_buf, q_buf, kn_buf, vn_buf,
                  o_buf, att_buf, lens_buf, kv_send_buf,
                  w_sem, suf_load_sem, suf_send_sem, suf_recv_sem, pre_local_sem, pre_send_sem, pre_recv_sem,
                  part_send_sem, part_recv_sem, lens_sem, kv_sem):
    layers, rows, group, head_dim, slots = dims
    tiles = x_buf.shape[0]
    q_width = wq_buf.shape[2]
    kv_width = wk_buf.shape[2]
    both = 2 * rows
    me = lax.axis_index("ctx")
    core = lax.rem(me, 2)
    chip = me // 2
    mate = chip * 2 + (1 - core)
    across = (1 - chip) * 2 + core
    diagonal = (1 - chip) * 2 + (1 - core)
    peers = ((mate, 1 - core), (across, core), (diagonal, 1 - core))
    mine = pl.multiple_of(core * rows, rows)
    other = pl.multiple_of((1 - core) * rows, rows)
    q_col = pl.multiple_of(core * q_width, 128)
    kv_col = pl.multiple_of(core * kv_width, 128)
    scale = head_dim ** -0.5

    def qkv_copies(layer, j):
        r = pl.ds(pl.multiple_of(j * TILE, TILE), TILE)
        return (
            pltpu.make_async_copy(wq_ref.at[layer, r, pl.ds(q_col, q_width)], wq_buf.at[j], w_sem.at[0, j]),
            pltpu.make_async_copy(wk_ref.at[layer, r, pl.ds(kv_col, kv_width)], wk_buf.at[j], w_sem.at[1, j]),
            pltpu.make_async_copy(wv_ref.at[layer, r, pl.ds(kv_col, kv_width)], wv_buf.at[j], w_sem.at[2, j]),
        )

    def wo_copy(layer, j):
        cols = pl.ds(pl.multiple_of(j * TILE, TILE), TILE)
        return pltpu.make_async_copy(wo_ref.at[layer, pl.ds(q_col, q_width), cols], wo_buf.at[j], w_sem.at[3, j])

    def suf_loads(layer):
        slot = lax.rem(layer, 3)
        return (
            pltpu.make_async_copy(ksuf_ref.at[layer], suf_buf.at[slot, 0], suf_load_sem.at[slot, 0]),
            pltpu.make_async_copy(vsuf_ref.at[layer], suf_buf.at[slot, 1], suf_load_sem.at[slot, 1]),
        )

    def suf_send(layer):
        return pltpu.make_async_remote_copy(
            src_ref=suf_buf.at[lax.rem(layer, 3)], dst_ref=suf_buf.at[3 + lax.rem(layer, 2)],
            send_sem=suf_send_sem.at[lax.rem(layer, 2)], recv_sem=suf_recv_sem.at[lax.rem(layer, 2)],
            device_id={"ctx": mate}, device_id_type=MESH)

    def pre_local(layer):
        return pltpu.make_async_copy(pre_ref.at[layer, core], pre_buf.at[layer, :, :, me], pre_local_sem.at[layer])

    def pre_remote(layer, k):
        device, half = peers[k]
        return pltpu.make_async_remote_copy(
            src_ref=pre_ref.at[layer, half], dst_ref=pre_buf.at[layer, :, :, me],
            send_sem=pre_send_sem.at[layer, k], recv_sem=pre_recv_sem.at[layer, k],
            device_id={"ctx": device}, device_id_type=MESH)

    def part_send(parity, j):
        return pltpu.make_async_remote_copy(
            src_ref=own_buf.at[j], dst_ref=recv_buf.at[parity, j],
            send_sem=part_send_sem.at[j], recv_sem=part_recv_sem.at[parity, j],
            device_id={"ctx": mate}, device_id_type=MESH)

    lens_send = pltpu.make_async_remote_copy(
        src_ref=lens_ref, dst_ref=lens_buf.at[pl.ds(mine, rows)], send_sem=lens_sem.at[0], recv_sem=lens_sem.at[1],
        device_id={"ctx": mate}, device_id_type=MESH)
    kv_send = pltpu.make_async_remote_copy(
        src_ref=kv_send_buf, dst_ref=kv_out_ref.at[:, core], send_sem=kv_sem.at[0], recv_sem=kv_sem.at[1],
        device_id={"ctx": mate}, device_id_type=MESH)

    def for_tiles(body):
        lax.fori_loop(0, tiles, lambda j, _: (body(j), 0)[1], 0)

    for layer in range(2):
        for copy in suf_loads(layer):
            copy.start()

    def first_qkv(j):
        for copy in qkv_copies(0, j):
            copy.start()

    for_tiles(first_qkv)
    pre_local(0).start()
    pre_local(1).start()
    for_tiles(lambda j: wo_copy(0, j).start())

    for j in range(tiles):
        x_buf[j] = jnp.zeros_like(x_buf[j])
        own_buf[j] = jnp.zeros_like(own_buf[j])
        own_buf[j, pl.ds(mine, rows), :] = hidden_ref[:, j * TILE:(j + 1) * TILE].astype(F32)
    lens_buf[pl.ds(mine, rows)] = lens_ref[...]
    q_buf[...] = jnp.zeros_like(q_buf)
    kn_buf[...] = jnp.zeros_like(kn_buf)
    vn_buf[...] = jnp.zeros_like(vn_buf)

    barrier = pltpu.get_barrier_semaphore()
    for device, _ in peers:
        pl.semaphore_signal(barrier, inc=1, device_id={"ctx": device}, device_id_type=MESH)
    pl.semaphore_wait(barrier, 3)

    for_tiles(lambda j: part_send(1, j).start())
    lens_send.start()
    for layer in range(2):
        for k in range(3):
            pre_remote(layer, k).start()
    for copy in suf_loads(0):
        copy.wait()
    suf_send(0).start()
    lens_send.wait()

    row_ids = lax.broadcasted_iota(jnp.int32, (2 * PAD, 128), 0)
    key_ids = lax.broadcasted_iota(jnp.int32, (2 * PAD, 128), 1)
    key_slot = jnp.where(lax.rem(key_ids, 4) == 2 * core + row_ids // PAD, key_ids // 4, slots)[None]

    def update_x(parity, j):
        copy = part_send(parity, j)
        copy.wait_recv()
        copy.wait_send()
        update = (own_buf[j] + recv_buf[parity, j]).astype(BF16)
        x_buf[j] = (x_buf[j].astype(F32) + update.astype(F32)).astype(BF16)

    def layer_body(layer, carry):
        parity_in = lax.rem(layer + 1, 2)
        parity_out = lax.rem(layer, 2)

        @pl.when(layer < layers - 2)
        def _():
            for copy in suf_loads(layer + 2):
                copy.start()
            pre_local(layer + 2).start()
            for k in range(3):
                pre_remote(layer + 2, k).start()

        acc_buf[...] = jnp.zeros_like(acc_buf)

        def qkv_tile(j):
            update_x(parity_in, j)
            for copy in qkv_copies(layer, j):
                copy.wait()
            x = x_buf[j]
            acc_buf[:, 0:q_width] += jnp.dot(x, wq_buf[j], preferred_element_type=F32)
            acc_buf[:, q_width:q_width + kv_width] += jnp.dot(x, wk_buf[j], preferred_element_type=F32)
            acc_buf[:, q_width + kv_width:q_width + 2 * kv_width] += jnp.dot(x, wv_buf[j], preferred_element_type=F32)

            @pl.when(layer < layers - 1)
            def _():
                for copy in qkv_copies(layer + 1, j):
                    copy.start()

        for_tiles(qkv_tile)

        @pl.when(layer < layers - 1)
        def _():
            for copy in suf_loads(layer + 1):
                copy.wait()
            suf_send(layer + 1).start()

        for h in range(2):
            for g in range(group):
                col = (h * group + g) * head_dim
                q_buf[pl.ds(h * PAD + g, both, stride=2 * PAD), :] = acc_buf[:, col:col + head_dim].astype(BF16).astype(F32)
            k_new = acc_buf[:, q_width + h * head_dim:q_width + (h + 1) * head_dim].astype(BF16).astype(F32)
            v_col = q_width + kv_width + h * head_dim
            v_new = acc_buf[:, v_col:v_col + head_dim].astype(BF16).astype(F32)
            for g in range(PAD):
                kn_buf[pl.ds(h * PAD + g, both, stride=2 * PAD), :] = k_new
                vn_buf[pl.ds(h * PAD + g, both, stride=2 * PAD), :] = v_new
        kv_out_ref[layer, core] = acc_buf[pl.ds(mine, rows), q_width:q_width + 2 * kv_width].astype(BF16)
        kv_send_buf[layer] = acc_buf[pl.ds(other, rows), q_width:q_width + 2 * kv_width].astype(BF16)

        pre_local(layer).wait()
        for k in range(3):
            pre_remote(layer, k).wait()
        suf_send(layer).wait()

        @pl.when(layer == layers - 1)
        def _():
            kv_send.start()

        per_core = rows // CHUNK

        def attend(i, carry):
            away = i // per_core
            part = pl.multiple_of(lax.rem(i, per_core) * CHUNK, CHUNK)
            first = pl.multiple_of(lax.rem(core + away, 2) * rows + part, CHUNK)
            slot = (1 - away) * lax.rem(layer, 3) + away * (3 + lax.rem(layer, 2))
            chunk_rows = pl.ds(pl.multiple_of(first * 2 * PAD, CHUNK * 2 * PAD), CHUNK * 2 * PAD)
            q = q_buf[chunk_rows, :]
            q3 = q.reshape(CHUNK, 2 * PAD, head_dim)
            k_suf = suf_buf[slot, 0, pl.ds(part, CHUNK)]
            v_suf = suf_buf[slot, 1, pl.ds(part, CHUNK)]
            suf_scores = lax.dot_general(q3.astype(BF16), k_suf, (((2,), (2,)), ((0,), (0,))), preferred_element_type=F32) * scale
            suf_scores = jnp.where(key_slot < lens_buf[pl.ds(first, CHUNK)], suf_scores, -jnp.inf)
            k_new = kn_buf[chunk_rows, :].reshape(CHUNK, 2 * PAD, head_dim)
            v_new = vn_buf[chunk_rows, :].reshape(CHUNK, 2 * PAD, head_dim)
            new_scores = jnp.sum(q3 * k_new, axis=-1, keepdims=True) * scale
            suf_weights, new_weights, masses, pre_vals = [], [], [], []
            for h in range(2):
                hs = slice(h * PAD, (h + 1) * PAD)
                q_h = q3[:, hs, :].reshape(CHUNK * PAD, head_dim).astype(BF16)
                k_pre = pre_buf[layer, 0, h].reshape(-1, head_dim)
                v_pre = pre_buf[layer, 1, h].reshape(-1, head_dim)
                scores = lax.dot_general(q_h, k_pre, (((1,), (1,)), ((), ())), preferred_element_type=F32) * scale
                suf_h = suf_scores[:, hs, :].reshape(CHUNK * PAD, 128)
                new_h = new_scores[:, hs, :].reshape(CHUNK * PAD, 1)
                peak = jnp.maximum(jnp.maximum(scores.max(axis=-1, keepdims=True), suf_h.max(axis=-1, keepdims=True)), new_h)
                pre_w = jnp.exp(scores - peak)
                suf_w = jnp.exp(suf_h - peak)
                new_w = jnp.exp(new_h - peak)
                masses.append(pre_w.sum(axis=-1, keepdims=True) + suf_w.sum(axis=-1, keepdims=True) + new_w)
                pre_vals.append(jnp.dot(pre_w.astype(BF16), v_pre, preferred_element_type=F32))
                suf_weights.append(suf_w.reshape(CHUNK, PAD, 128))
                new_weights.append(new_w)
            suf_w = jnp.concatenate(suf_weights, axis=1).astype(BF16)
            suf_vals = lax.dot_general(suf_w, v_suf, (((2,), (1,)), ((0,), (0,))), preferred_element_type=F32)
            outs = []
            for h in range(2):
                hs = slice(h * PAD, (h + 1) * PAD)
                mixed = pre_vals[h] + suf_vals[:, hs, :].reshape(CHUNK * PAD, head_dim)
                mixed = mixed + new_weights[h] * v_new[:, hs, :].reshape(CHUNK * PAD, head_dim)
                outs.append((mixed / masses[h]).reshape(CHUNK, PAD, head_dim))
            o_buf[chunk_rows, :] = jnp.concatenate(outs, axis=1).reshape(CHUNK * 2 * PAD, head_dim)
            return carry

        lax.fori_loop(0, 2 * per_core, attend, 0)

        for h in range(2):
            for g in range(group):
                col = (h * group + g) * head_dim
                att_buf[:, col:col + head_dim] = o_buf[pl.ds(h * PAD + g, both, stride=2 * PAD), :].astype(BF16)

        def out_tile(j):
            wo_copy(layer, j).wait()
            own_buf[j] = jnp.dot(att_buf[...], wo_buf[j], preferred_element_type=F32)

            @pl.when(layer < layers - 1)
            def _():
                wo_copy(layer + 1, j).start()

            @pl.when(j > 0)
            def _():
                part_send(parity_out, j - 1).start()

        for_tiles(out_tile)
        part_send(parity_out, tiles - 1).start()
        return carry

    lax.fori_loop(0, layers, layer_body, 0)
    for j in range(tiles):
        update_x((layers - 1) % 2, j)
        out_ref[:, j * TILE:(j + 1) * TILE] = x_buf[j, pl.ds(mine, rows), :]
    kv_send.wait()


def solution(mesh):
    home_axes = ('data', 'ctx')
    row_spec = P(home_axes, None)
    lens_spec = P(home_axes)
    whole_spec = P()
    prefix_spec = P(None, home_axes, None, None)
    cache_spec = P(None, home_axes, None, None, None)

    def local_step(hidden, seq_lens, w_query, w_key, w_value, w_out, k_prefix, v_prefix, k_suffix, v_suffix):
        layers, model_dim = w_query.shape[:2]
        positions, kv_heads, head_dim = k_prefix.shape[1:]
        rows = hidden.shape[0]
        slots = k_suffix.shape[2]
        group = w_query.shape[2] // head_dim // kv_heads
        half_heads = kv_heads // 2
        q_width = w_query.shape[2] // 2
        kv_width = w_key.shape[2] // 2
        tiles = model_dim // TILE
        keys = slots * kv_heads
        both = 2 * rows

        prefix = jnp.stack([k_prefix, v_prefix]).reshape(2, layers, positions, 2, half_heads, head_dim)
        prefix = prefix.transpose(1, 3, 0, 4, 2, 5)
        lens_rep = jnp.broadcast_to(seq_lens[:, None, None], (rows, 2 * PAD, 128))
        k_flat = k_suffix.reshape(layers, rows, keys, head_dim)
        v_flat = v_suffix.reshape(layers, rows, keys, head_dim)

        any_spec = pl.BlockSpec(memory_space=pl.ANY)
        vmem_spec = pl.BlockSpec(memory_space=pltpu.VMEM)
        dma = pltpu.SemaphoreType.DMA
        hidden_out, kv_new = pl.pallas_call(
            functools.partial(decode_kernel, (layers, rows, group, head_dim, slots)),
            out_shape=(jax.ShapeDtypeStruct((rows, model_dim), BF16),
                       jax.ShapeDtypeStruct((layers, 2, rows, 2 * kv_width), BF16)),
            in_specs=[vmem_spec, vmem_spec] + [any_spec] * 7,
            out_specs=(vmem_spec, vmem_spec),
            scratch_shapes=[
                pltpu.VMEM((tiles, TILE, q_width), BF16),
                pltpu.VMEM((tiles, TILE, kv_width), BF16),
                pltpu.VMEM((tiles, TILE, kv_width), BF16),
                pltpu.VMEM((tiles, q_width, TILE), BF16),
                pltpu.VMEM((layers, 2, half_heads, 4, positions, head_dim), BF16),
                pltpu.VMEM((5, 2, rows, keys, head_dim), BF16),
                pltpu.VMEM((tiles, both, TILE), BF16),
                pltpu.VMEM((tiles, both, TILE), F32),
                pltpu.VMEM((2, tiles, both, TILE), F32),
                pltpu.VMEM((both, q_width + 2 * kv_width), F32),
                pltpu.VMEM((both * 2 * PAD, head_dim), F32),
                pltpu.VMEM((both * 2 * PAD, head_dim), F32),
                pltpu.VMEM((both * 2 * PAD, head_dim), F32),
                pltpu.VMEM((both * 2 * PAD, head_dim), F32),
                pltpu.VMEM((both, q_width), BF16),
                pltpu.VMEM((both, 2 * PAD, 128), jnp.int32),
                pltpu.VMEM((layers, rows, 2 * kv_width), BF16),
                dma((4, tiles)), dma((3, 2)), dma((2,)), dma((2,)), dma((layers,)), dma((layers, 3)), dma((layers, 3)),
                dma((tiles,)), dma((2, tiles)), dma((2,)), dma((2,)),
            ],
            compiler_params=pltpu.CompilerParams(collective_id=0, has_side_effects=True, vmem_limit_bytes=66_000_000),
            name="decode_layers",
        )(hidden, lens_rep, w_query, w_key, w_value, w_out, prefix, k_flat, v_flat)

        kv_new = kv_new.reshape(layers, 2, rows, 2, half_heads, head_dim).transpose(3, 0, 2, 1, 4, 5)
        kv_new = kv_new.reshape(2, layers, rows, 1, kv_heads, head_dim)
        hit = (lax.broadcasted_iota(jnp.int32, (rows, slots), 1) == seq_lens[:, None])[None, :, :, None, None]
        k_out = jnp.where(hit, kv_new[0], k_suffix)
        v_out = jnp.where(hit, kv_new[1], v_suffix)
        return hidden_out, k_out, v_out

    return jax.shard_map(local_step, mesh=mesh, in_specs=(row_spec, lens_spec, whole_spec, whole_spec, whole_spec, whole_spec, prefix_spec, prefix_spec, cache_spec, cache_spec), out_specs=(row_spec, cache_spec, cache_spec), check_vma=False)
```

```python
import functools

import jax
import jax.numpy as jnp
from jax import lax
from jax.experimental import pallas as pl
from jax.experimental.pallas import tpu as pltpu
from jax.sharding import PartitionSpec as P

MESH = pl.DeviceIdType.MESH
BF16 = jnp.bfloat16
F32 = jnp.float32
TILE = 512
CHUNK = 16
PAD = 8
RING = 8


def decode_kernel(dims, lens_ref, hidden_ref, wq_ref, wk_ref, wv_ref, wo_ref, kpre_ref, vpre_ref, ksuf_ref, vsuf_ref,
                  out_ref, kv_out_ref,
                  wq_buf, wk_buf, wv_buf, wo_buf, pre_buf, raw_buf, wide_buf, split_buf, suf_buf, x_buf, own_buf, recv_buf, acc_buf,
                  q_buf, kvn_buf, o_buf, att_buf, lens_buf, kv_send_buf,
                  w_sem, suf_load_sem, suf_send_sem, suf_recv_sem, raw_sem, pre_send_sem, pre_recv_sem,
                  part_send_sem, part_recv_sem, lens_sem, kv_sem):
    layers, rows, group, head_dim, slots = dims
    half_heads = 2
    tiles = x_buf.shape[0]
    q_width = wq_buf.shape[2]
    kv_width = wk_buf.shape[2]
    both = 2 * rows
    me = lax.axis_index("ctx")
    core = lax.rem(me, 2)
    chip = me // 2
    mate = chip * 2 + (1 - core)
    across = (1 - chip) * 2 + core
    diagonal = (1 - chip) * 2 + (1 - core)
    peers = ((mate, 1 - core), (across, core), (diagonal, 1 - core))
    mine = pl.multiple_of(core * rows, rows)
    other = pl.multiple_of((1 - core) * rows, rows)
    q_col = pl.multiple_of(core * q_width, 128)
    kv_col = pl.multiple_of(core * kv_width, 128)
    scale = head_dim ** -0.5

    def qkv_copies(layer, j):
        r = pl.ds(pl.multiple_of(j * TILE, TILE), TILE)
        return (
            pltpu.make_async_copy(wq_ref.at[layer, r, pl.ds(q_col, q_width)], wq_buf.at[j], w_sem.at[0, j]),
            pltpu.make_async_copy(wk_ref.at[layer, r, pl.ds(kv_col, kv_width)], wk_buf.at[j], w_sem.at[1, j]),
            pltpu.make_async_copy(wv_ref.at[layer, r, pl.ds(kv_col, kv_width)], wv_buf.at[j], w_sem.at[2, j]),
        )

    def wo_copy(layer, j):
        cols = pl.ds(pl.multiple_of(j * TILE, TILE), TILE)
        return pltpu.make_async_copy(wo_ref.at[layer, pl.ds(q_col, q_width), cols], wo_buf.at[j], w_sem.at[3, j])

    def suf_loads(layer):
        slot = lax.rem(layer, 3)
        return (
            pltpu.make_async_copy(ksuf_ref.at[layer], suf_buf.at[slot, 0], suf_load_sem.at[slot, 0]),
            pltpu.make_async_copy(vsuf_ref.at[layer], suf_buf.at[slot, 1], suf_load_sem.at[slot, 1]),
        )

    def suf_send(layer):
        return pltpu.make_async_remote_copy(
            src_ref=suf_buf.at[lax.rem(layer, 3)], dst_ref=suf_buf.at[3 + lax.rem(layer, 2)],
            send_sem=suf_send_sem.at[lax.rem(layer, 2)], recv_sem=suf_recv_sem.at[lax.rem(layer, 2)],
            device_id={"ctx": mate}, device_id_type=MESH)

    def raw_loads(layer):
        slot = lax.rem(layer, 2)
        return (
            pltpu.make_async_copy(kpre_ref.at[layer], raw_buf.at[slot, 0], raw_sem.at[slot, 0]),
            pltpu.make_async_copy(vpre_ref.at[layer], raw_buf.at[slot, 1], raw_sem.at[slot, 1]),
        )

    def split_prefix(layer):
        slot = lax.rem(layer, 2)
        heads = 2 * half_heads
        positions = pre_buf.shape[4]
        for copy in raw_loads(layer):
            copy.wait()
        for kv in range(2):
            wide_buf[kv] = raw_buf[slot, kv].astype(F32)
            for h in range(half_heads):
                for half in range(2):
                    split_buf[slot, half, kv, h] = wide_buf[kv, pl.ds(half * half_heads + h, positions, stride=heads), :].astype(BF16)
                pre_buf[layer, kv, h, me] = split_buf[slot, core, kv, h]

    def pre_remote(layer, k):
        device, half = peers[k]
        return pltpu.make_async_remote_copy(
            src_ref=split_buf.at[lax.rem(layer, 2), half], dst_ref=pre_buf.at[layer, :, :, me],
            send_sem=pre_send_sem.at[layer, k], recv_sem=pre_recv_sem.at[layer, k],
            device_id={"ctx": device}, device_id_type=MESH)

    def part_send(parity, j):
        return pltpu.make_async_remote_copy(
            src_ref=own_buf.at[j], dst_ref=recv_buf.at[parity, j],
            send_sem=part_send_sem.at[j], recv_sem=part_recv_sem.at[parity, j],
            device_id={"ctx": mate}, device_id_type=MESH)

    lens_send = pltpu.make_async_remote_copy(
        src_ref=lens_buf.at[pl.ds(mine, rows)], dst_ref=lens_buf.at[pl.ds(mine, rows)], send_sem=lens_sem.at[0], recv_sem=lens_sem.at[1],
        device_id={"ctx": mate}, device_id_type=MESH)
    kv_send = pltpu.make_async_remote_copy(
        src_ref=kv_send_buf, dst_ref=kv_out_ref.at[:, :, pl.ds(core * half_heads, half_heads)], send_sem=kv_sem.at[0], recv_sem=kv_sem.at[1],
        device_id={"ctx": mate}, device_id_type=MESH)

    def for_tiles(body):
        lax.fori_loop(0, tiles, lambda j, _: (body(j), 0)[1], 0)

    for layer in range(2):
        for copy in raw_loads(layer):
            copy.start()
    for copy in suf_loads(0):
        copy.start()

    def first_qkv(j):
        for copy in qkv_copies(0, j):
            copy.start()

    for_tiles(first_qkv)
    for_tiles(lambda j: wo_copy(0, j).start())
    for copy in suf_loads(1):
        copy.start()

    for j in range(tiles):
        x_buf[j] = jnp.zeros_like(x_buf[j])
        own_buf[j] = jnp.zeros_like(own_buf[j])
        own_buf[j, pl.ds(mine, rows), :] = hidden_ref[:, j * TILE:(j + 1) * TILE].astype(F32)
    diagonal_hit = lax.broadcasted_iota(jnp.int32, (rows, rows), 0) == lax.broadcasted_iota(jnp.int32, (rows, rows), 1)
    lens_wide = jnp.broadcast_to(lens_ref[...].astype(F32), (rows, rows))
    lens_wide = jnp.where(diagonal_hit, lens_wide, 0.0).sum(axis=1, keepdims=True)
    lens_wide = jnp.broadcast_to(lens_wide, (rows, 128)).astype(jnp.int32)
    for b in range(rows):
        lens_buf[mine + b] = jnp.broadcast_to(lens_wide[b:b + 1, :], (2 * PAD, 128))
    q_buf[...] = jnp.zeros_like(q_buf)
    split_prefix(0)
    for copy in raw_loads(2):
        copy.start()
    split_prefix(1)

    barrier = pltpu.get_barrier_semaphore()
    for device, _ in peers:
        pl.semaphore_signal(barrier, inc=1, device_id={"ctx": device}, device_id_type=MESH)
    pl.semaphore_wait(barrier, 3)

    for_tiles(lambda j: part_send(1, j).start())
    lens_send.start()
    for layer in range(2):
        for k in range(3):
            pre_remote(layer, k).start()
    for copy in suf_loads(0):
        copy.wait()
    suf_send(0).start()
    lens_send.wait()

    row_ids = lax.broadcasted_iota(jnp.int32, (2 * PAD, 128), 0)
    key_ids = lax.broadcasted_iota(jnp.int32, (2 * PAD, 128), 1)
    key_slot = jnp.where(lax.rem(key_ids, 4) == 2 * core + row_ids // PAD, key_ids // 4, slots)[None]

    def update_x(parity, j):
        copy = part_send(parity, j)
        copy.wait_recv()
        copy.wait_send()
        update = (own_buf[j] + recv_buf[parity, j]).astype(BF16)
        x_buf[j] = (x_buf[j].astype(F32) + update.astype(F32)).astype(BF16)

    def layer_body(layer, carry):
        parity_in = lax.rem(layer + 1, 2)
        parity_out = lax.rem(layer, 2)

        @pl.when(layer < layers - 3)
        def _():
            for copy in raw_loads(layer + 3):
                copy.start()

        for k in range(3):
            pre_remote(layer, k).wait_send()

        @pl.when(layer < layers - 2)
        def _():
            for copy in suf_loads(layer + 2):
                copy.start()
            split_prefix(layer + 2)

        acc_buf[...] = jnp.zeros_like(acc_buf)

        def qkv_tile(j):
            update_x(parity_in, j)
            for copy in qkv_copies(layer, j):
                copy.wait()
            x = x_buf[j]
            acc_buf[:, 0:q_width] += jnp.dot(x, wq_buf[j], preferred_element_type=F32)
            acc_buf[:, q_width:q_width + kv_width] += jnp.dot(x, wk_buf[j], preferred_element_type=F32)
            acc_buf[:, q_width + kv_width:q_width + 2 * kv_width] += jnp.dot(x, wv_buf[j], preferred_element_type=F32)

            @pl.when(layer < layers - 1)
            def _():
                for copy in qkv_copies(layer + 1, j):
                    copy.start()

            @pl.when(j == 1)
            def _():
                @pl.when(layer < layers - 1)
                def _():
                    for copy in suf_loads(layer + 1):
                        copy.wait()
                    suf_send(layer + 1).start()

                @pl.when(layer < layers - 2)
                def _():
                    for k in range(3):
                        pre_remote(layer + 2, k).start()

        for_tiles(qkv_tile)

        for h in range(2):
            for g in range(group):
                col = (h * group + g) * head_dim
                q_buf[pl.ds(h * PAD + g, both, stride=2 * PAD), :] = acc_buf[:, col:col + head_dim].astype(BF16).astype(F32)
            for kv in range(2):
                col = q_width + kv * kv_width + h * head_dim
                fresh = acc_buf[:, col:col + head_dim].astype(BF16).astype(F32)
                kvn_buf[kv, h] = fresh
        for h in range(2):
            for kv in range(2):
                kv_out_ref[layer, kv, core * half_heads + h] = kvn_buf[kv, h, pl.ds(mine, rows), :]
                kv_send_buf[layer, kv, h] = kvn_buf[kv, h, pl.ds(other, rows), :]

        for k in range(3):
            pre_remote(layer, k).wait_recv()
        suf_send(layer).wait()

        @pl.when(layer == layers - 1)
        def _():
            kv_send.start()

        per_core = rows // CHUNK

        def attend(i, carry):
            away = i // per_core
            part = pl.multiple_of(lax.rem(i, per_core) * CHUNK, CHUNK)
            first = pl.multiple_of(lax.rem(core + away, 2) * rows + part, CHUNK)
            slot = (1 - away) * lax.rem(layer, 3) + away * (3 + lax.rem(layer, 2))
            chunk_rows = pl.ds(pl.multiple_of(first * 2 * PAD, CHUNK * 2 * PAD), CHUNK * 2 * PAD)
            q = q_buf[chunk_rows, :]
            q3 = q.reshape(CHUNK, 2 * PAD, head_dim)
            k_suf = suf_buf[slot, 0, pl.ds(part, CHUNK)]
            v_suf = suf_buf[slot, 1, pl.ds(part, CHUNK)]
            suf_scores = lax.dot_general(q3.astype(BF16), k_suf, (((2,), (2,)), ((0,), (0,))), preferred_element_type=F32) * scale
            suf_scores = jnp.where(key_slot < lens_buf[pl.ds(first, CHUNK)], suf_scores, -jnp.inf)
            def spread(kv):
                picked = [jnp.broadcast_to(kvn_buf[kv, h, pl.ds(first + b, 1), :], (PAD, head_dim)) for b in range(CHUNK) for h in range(2)]
                return jnp.concatenate(picked, axis=0).reshape(CHUNK, 2 * PAD, head_dim)

            k_new = spread(0)
            v_new = spread(1)
            new_scores = jnp.sum(q3 * k_new, axis=-1, keepdims=True) * scale
            suf_weights, new_weights, masses, pre_vals = [], [], [], []
            for h in range(2):
                hs = slice(h * PAD, (h + 1) * PAD)
                q_h = q3[:, hs, :].reshape(CHUNK * PAD, head_dim).astype(BF16)
                k_pre = pre_buf[layer, 0, h].reshape(-1, head_dim)
                v_pre = pre_buf[layer, 1, h].reshape(-1, head_dim)
                scores = lax.dot_general(q_h, k_pre, (((1,), (1,)), ((), ())), preferred_element_type=F32) * scale
                suf_h = suf_scores[:, hs, :].reshape(CHUNK * PAD, 128)
                new_h = new_scores[:, hs, :].reshape(CHUNK * PAD, 1)
                peak = jnp.maximum(jnp.maximum(scores.max(axis=-1, keepdims=True), suf_h.max(axis=-1, keepdims=True)), new_h)
                pre_w = jnp.exp(scores - peak)
                suf_w = jnp.exp(suf_h - peak)
                new_w = jnp.exp(new_h - peak)
                masses.append(pre_w.sum(axis=-1, keepdims=True) + suf_w.sum(axis=-1, keepdims=True) + new_w)
                pre_vals.append(jnp.dot(pre_w.astype(BF16), v_pre, preferred_element_type=F32))
                suf_weights.append(suf_w.reshape(CHUNK, PAD, 128))
                new_weights.append(new_w)
            suf_w = jnp.concatenate(suf_weights, axis=1).astype(BF16)
            suf_vals = lax.dot_general(suf_w, v_suf, (((2,), (1,)), ((0,), (0,))), preferred_element_type=F32)
            outs = []
            for h in range(2):
                hs = slice(h * PAD, (h + 1) * PAD)
                mixed = pre_vals[h] + suf_vals[:, hs, :].reshape(CHUNK * PAD, head_dim)
                mixed = mixed + new_weights[h] * v_new[:, hs, :].reshape(CHUNK * PAD, head_dim)
                outs.append((mixed / masses[h]).reshape(CHUNK, PAD, head_dim))
            o_buf[chunk_rows, :] = jnp.concatenate(outs, axis=1).reshape(CHUNK * 2 * PAD, head_dim)
            return carry

        lax.fori_loop(0, 2 * per_core, attend, 0)

        for h in range(2):
            for g in range(group):
                col = (h * group + g) * head_dim
                att_buf[:, col:col + head_dim] = o_buf[pl.ds(h * PAD + g, both, stride=2 * PAD), :].astype(BF16)

        def out_tile(j):
            wo_copy(layer, j).wait()
            own_buf[j] = jnp.dot(att_buf[...], wo_buf[j], preferred_element_type=F32)

            @pl.when(layer < layers - 1)
            def _():
                wo_copy(layer + 1, j).start()

            @pl.when(j > 0)
            def _():
                part_send(parity_out, j - 1).start()

        for_tiles(out_tile)
        part_send(parity_out, tiles - 1).start()
        return carry

    lax.fori_loop(0, layers, layer_body, 0)
    for j in range(tiles):
        update_x((layers - 1) % 2, j)
        out_ref[:, j * TILE:(j + 1) * TILE] = x_buf[j, pl.ds(mine, rows), :]
    kv_send.wait()


def cache_kernel(lens_ref, new_ref, k_ref, v_ref, k_out_ref, v_out_ref, buf, new_buf, in_sem, out_sem, new_sem):
    layers, rows, _, heads, _ = k_ref.shape
    ahead = RING // 2

    def loads(layer):
        slot = lax.rem(layer, RING)
        return (
            pltpu.make_async_copy(k_ref.at[layer], buf.at[slot, 0], in_sem.at[slot, 0]),
            pltpu.make_async_copy(v_ref.at[layer], buf.at[slot, 1], in_sem.at[slot, 1]),
            pltpu.make_async_copy(new_ref.at[layer], new_buf.at[slot], new_sem.at[slot]),
        )

    def stores(layer):
        slot = lax.rem(layer, RING)
        return (
            pltpu.make_async_copy(buf.at[slot, 0], k_out_ref.at[layer], out_sem.at[slot, 0]),
            pltpu.make_async_copy(buf.at[slot, 1], v_out_ref.at[layer], out_sem.at[slot, 1]),
        )

    for layer in range(ahead):
        for copy in loads(layer):
            copy.start()

    def step(layer, carry):
        slot = lax.rem(layer, RING)

        @pl.when(layer >= ahead)
        def _():
            for copy in stores(layer - ahead):
                copy.wait()

        @pl.when(layer < layers - ahead)
        def _():
            for copy in loads(layer + ahead):
                copy.start()

        for copy in loads(layer):
            copy.wait()
        for b in range(rows):
            for kv in range(2):
                buf[slot, kv, b, lens_ref[b]] = new_buf[slot, kv, pl.ds(b, heads, stride=rows), :].astype(BF16)
        for copy in stores(layer):
            copy.start()
        return carry

    lax.fori_loop(0, layers, step, 0)
    for layer in range(layers - ahead, layers):
        for copy in stores(layer):
            copy.wait()


def solution(mesh):
    home_axes = ('data', 'ctx')
    row_spec = P(home_axes, None)
    lens_spec = P(home_axes)
    whole_spec = P()
    prefix_spec = P(None, home_axes, None, None)
    cache_spec = P(None, home_axes, None, None, None)

    def local_step(hidden, seq_lens, w_query, w_key, w_value, w_out, k_prefix, v_prefix, k_suffix, v_suffix):
        layers, model_dim = w_query.shape[:2]
        positions, kv_heads, head_dim = k_prefix.shape[1:]
        rows = hidden.shape[0]
        slots = k_suffix.shape[2]
        group = w_query.shape[2] // head_dim // kv_heads
        half_heads = kv_heads // 2
        q_width = w_query.shape[2] // 2
        kv_width = w_key.shape[2] // 2
        tiles = model_dim // TILE
        keys = slots * kv_heads
        both = 2 * rows

        k_flat = k_suffix.reshape(layers, rows, keys, head_dim)
        v_flat = v_suffix.reshape(layers, rows, keys, head_dim)
        k_pre = k_prefix.reshape(layers, positions * kv_heads, head_dim)
        v_pre = v_prefix.reshape(layers, positions * kv_heads, head_dim)

        any_spec = pl.BlockSpec(memory_space=pl.ANY)
        smem_spec = pl.BlockSpec(memory_space=pltpu.SMEM)
        vmem_spec = pl.BlockSpec(memory_space=pltpu.VMEM)
        dma = pltpu.SemaphoreType.DMA
        hidden_out, kv_new = pl.pallas_call(
            functools.partial(decode_kernel, (layers, rows, group, head_dim, slots)),
            out_shape=(jax.ShapeDtypeStruct((rows, model_dim), BF16),
                       jax.ShapeDtypeStruct((layers, 2, kv_heads, rows, head_dim), F32)),
            in_specs=[vmem_spec, vmem_spec] + [any_spec] * 8,
            out_specs=(vmem_spec, vmem_spec),
            scratch_shapes=[
                pltpu.VMEM((tiles, TILE, q_width), BF16),
                pltpu.VMEM((tiles, TILE, kv_width), BF16),
                pltpu.VMEM((tiles, TILE, kv_width), BF16),
                pltpu.VMEM((tiles, q_width, TILE), BF16),
                pltpu.VMEM((layers, 2, half_heads, 4, positions, head_dim), BF16),
                pltpu.VMEM((2, 2, positions * kv_heads, head_dim), BF16),
                pltpu.VMEM((2, positions * kv_heads, head_dim), F32),
                pltpu.VMEM((2, 2, 2, half_heads, positions, head_dim), BF16),
                pltpu.VMEM((5, 2, rows, keys, head_dim), BF16),
                pltpu.VMEM((tiles, both, TILE), BF16),
                pltpu.VMEM((tiles, both, TILE), F32),
                pltpu.VMEM((2, tiles, both, TILE), F32),
                pltpu.VMEM((both, q_width + 2 * kv_width), F32),
                pltpu.VMEM((both * 2 * PAD, head_dim), F32),
                pltpu.VMEM((2, half_heads, both, head_dim), F32),
                pltpu.VMEM((both * 2 * PAD, head_dim), F32),
                pltpu.VMEM((both, q_width), BF16),
                pltpu.VMEM((both, 2 * PAD, 128), jnp.int32),
                pltpu.VMEM((layers, 2, half_heads, rows, head_dim), F32),
                dma((4, tiles)), dma((3, 2)), dma((2,)), dma((2,)), dma((2, 2)), dma((layers, 3)), dma((layers, 3)),
                dma((tiles,)), dma((2, tiles)), dma((2,)), dma((2,)),
            ],
            compiler_params=pltpu.CompilerParams(collective_id=0, has_side_effects=True, vmem_limit_bytes=66_000_000),
            name="decode_layers",
        )(seq_lens.reshape(1, rows), hidden, w_query, w_key, w_value, w_out, k_pre, v_pre, k_flat, v_flat)

        k_out, v_out = pl.pallas_call(
            cache_kernel,
            out_shape=(jax.ShapeDtypeStruct(k_suffix.shape, BF16), jax.ShapeDtypeStruct(v_suffix.shape, BF16)),
            in_specs=[smem_spec] + [any_spec] * 3,
            out_specs=(any_spec, any_spec),
            scratch_shapes=[
                pltpu.VMEM((RING, 2) + k_suffix.shape[1:], BF16),
                pltpu.VMEM((RING, 2, kv_heads * rows, head_dim), F32),
                dma((RING, 2)), dma((RING, 2)), dma((RING,)),
            ],
            compiler_params=pltpu.CompilerParams(vmem_limit_bytes=60_000_000),
            name="write_caches",
        )(seq_lens, kv_new.reshape(layers, 2, kv_heads * rows, head_dim), k_suffix, v_suffix)
        return hidden_out, k_out, v_out

    return jax.shard_map(local_step, mesh=mesh, in_specs=(row_spec, lens_spec, whole_spec, whole_spec, whole_spec, whole_spec, prefix_spec, prefix_spec, cache_spec, cache_spec), out_specs=(row_spec, cache_spec, cache_spec), check_vma=False)
```

```python
import functools

import jax
import jax.numpy as jnp
from jax import lax
from jax.experimental import pallas as pl
from jax.experimental.pallas import tpu as pltpu
from jax.sharding import PartitionSpec as P

MESH = pl.DeviceIdType.MESH
BF16 = jnp.bfloat16
F32 = jnp.float32
TILE = 512
CHUNK = 16
PAD = 8
RING = 8
BLOCK = 2
CHUNKS_PER_TRIP = 2


def decode_kernel(dims, lens_ref, hidden_ref, wq_ref, wk_ref, wv_ref, wo_ref, kpre_ref, vpre_ref, ksuf_ref, vsuf_ref,
                  out_ref, kv_out_ref,
                  wq_buf, wk_buf, wv_buf, wo_buf, pre_buf, raw_buf, wide_buf, split_buf, suf_buf, x_buf, own_buf, recv_buf, acc_buf,
                  q_buf, kvn_buf, o_buf, att_buf, lens_buf, kv_send_buf,
                  w_sem, suf_load_sem, suf_send_sem, suf_recv_sem, raw_sem, pre_send_sem, pre_recv_sem,
                  part_send_sem, part_recv_sem, lens_sem, kv_sem):
    layers, rows, group, head_dim, slots = dims
    half_heads = 2
    tiles = own_buf.shape[0]
    q_width = wq_buf.shape[1]
    kv_width = wk_buf.shape[1]
    blocks = [(a, min(a + BLOCK, tiles)) for a in range(0, tiles, BLOCK)]
    both = 2 * rows
    me = lax.axis_index("ctx")
    core = lax.rem(me, 2)
    chip = me // 2
    mate = chip * 2 + (1 - core)
    across = (1 - chip) * 2 + core
    diagonal = (1 - chip) * 2 + (1 - core)
    peers = ((mate, 1 - core), (across, core), (diagonal, 1 - core))
    mine = pl.multiple_of(core * rows, rows)
    other = pl.multiple_of((1 - core) * rows, rows)
    q_col = pl.multiple_of(core * q_width, 128)
    kv_col = pl.multiple_of(core * kv_width, 128)
    scale = head_dim ** -0.5

    def qkv_copies(layer, i):
        a, b = blocks[i]
        r = pl.ds(a * TILE, (b - a) * TILE)
        return (
            pltpu.make_async_copy(wq_ref.at[layer, r, pl.ds(q_col, q_width)], wq_buf.at[r], w_sem.at[0, i]),
            pltpu.make_async_copy(wk_ref.at[layer, r, pl.ds(kv_col, kv_width)], wk_buf.at[r], w_sem.at[1, i]),
            pltpu.make_async_copy(wv_ref.at[layer, r, pl.ds(kv_col, kv_width)], wv_buf.at[r], w_sem.at[2, i]),
        )

    def wo_copy(layer, i):
        a, b = blocks[i]
        cols = pl.ds(a * TILE, (b - a) * TILE)
        return pltpu.make_async_copy(wo_ref.at[layer, pl.ds(q_col, q_width), cols], wo_buf.at[:, cols], w_sem.at[3, i])

    def suf_loads(layer):
        slot = lax.rem(layer, 3)
        return (
            pltpu.make_async_copy(ksuf_ref.at[layer], suf_buf.at[slot, 0], suf_load_sem.at[slot, 0]),
            pltpu.make_async_copy(vsuf_ref.at[layer], suf_buf.at[slot, 1], suf_load_sem.at[slot, 1]),
        )

    def suf_send(layer):
        return pltpu.make_async_remote_copy(
            src_ref=suf_buf.at[lax.rem(layer, 3)], dst_ref=suf_buf.at[3 + lax.rem(layer, 2)],
            send_sem=suf_send_sem.at[lax.rem(layer, 2)], recv_sem=suf_recv_sem.at[lax.rem(layer, 2)],
            device_id={"ctx": mate}, device_id_type=MESH)

    def raw_loads(layer):
        slot = lax.rem(layer, 2)
        return (
            pltpu.make_async_copy(kpre_ref.at[layer], raw_buf.at[slot, 0], raw_sem.at[slot, 0]),
            pltpu.make_async_copy(vpre_ref.at[layer], raw_buf.at[slot, 1], raw_sem.at[slot, 1]),
        )

    def split_prefix(layer):
        slot = lax.rem(layer, 2)
        heads = 2 * half_heads
        positions = pre_buf.shape[4]
        for copy in raw_loads(layer):
            copy.wait()
        for kv in range(2):
            wide_buf[kv] = raw_buf[slot, kv].astype(F32)
            for h in range(half_heads):
                for half in range(2):
                    split_buf[slot, half, kv, h] = wide_buf[kv, pl.ds(half * half_heads + h, positions, stride=heads), :].astype(BF16)
                pre_buf[layer, kv, h, me] = split_buf[slot, core, kv, h]

    def pre_remote(layer, k):
        device, half = peers[k]
        return pltpu.make_async_remote_copy(
            src_ref=split_buf.at[lax.rem(layer, 2), half], dst_ref=pre_buf.at[layer, :, :, me],
            send_sem=pre_send_sem.at[layer, k], recv_sem=pre_recv_sem.at[layer, k],
            device_id={"ctx": device}, device_id_type=MESH)

    def part_send(parity, j):
        return pltpu.make_async_remote_copy(
            src_ref=own_buf.at[j], dst_ref=recv_buf.at[parity, j],
            send_sem=part_send_sem.at[j], recv_sem=part_recv_sem.at[parity, j],
            device_id={"ctx": mate}, device_id_type=MESH)

    lens_send = pltpu.make_async_remote_copy(
        src_ref=lens_buf.at[pl.ds(mine, rows)], dst_ref=lens_buf.at[pl.ds(mine, rows)], send_sem=lens_sem.at[0], recv_sem=lens_sem.at[1],
        device_id={"ctx": mate}, device_id_type=MESH)
    kv_send = pltpu.make_async_remote_copy(
        src_ref=kv_send_buf, dst_ref=kv_out_ref.at[:, :, pl.ds(core * half_heads, half_heads)], send_sem=kv_sem.at[0], recv_sem=kv_sem.at[1],
        device_id={"ctx": mate}, device_id_type=MESH)

    for layer in range(2):
        for copy in raw_loads(layer):
            copy.start()
    for copy in suf_loads(0):
        copy.start()

    for i in range(len(blocks)):
        for copy in qkv_copies(0, i):
            copy.start()
    for i in range(len(blocks)):
        wo_copy(0, i).start()
    for copy in suf_loads(1):
        copy.start()

    x_buf[...] = jnp.zeros_like(x_buf)
    for j in range(tiles):
        own_buf[j] = jnp.zeros_like(own_buf[j])
        own_buf[j, pl.ds(mine, rows), :] = hidden_ref[:, j * TILE:(j + 1) * TILE].astype(F32)
    diagonal_hit = lax.broadcasted_iota(jnp.int32, (rows, rows), 0) == lax.broadcasted_iota(jnp.int32, (rows, rows), 1)
    lens_wide = jnp.broadcast_to(lens_ref[...].astype(F32), (rows, rows))
    lens_wide = jnp.where(diagonal_hit, lens_wide, 0.0).sum(axis=1, keepdims=True)
    lens_wide = jnp.broadcast_to(lens_wide, (rows, 128)).astype(jnp.int32)
    for b in range(rows):
        lens_buf[mine + b] = jnp.broadcast_to(lens_wide[b:b + 1, :], (2 * PAD, 128))
    q_buf[...] = jnp.zeros_like(q_buf)
    split_prefix(0)
    for copy in raw_loads(2):
        copy.start()
    split_prefix(1)

    barrier = pltpu.get_barrier_semaphore()
    for device, _ in peers:
        pl.semaphore_signal(barrier, inc=1, device_id={"ctx": device}, device_id_type=MESH)
    pl.semaphore_wait(barrier, 3)

    for j in range(tiles):
        part_send(1, j).start()
    lens_send.start()
    for layer in range(2):
        for k in range(3):
            pre_remote(layer, k).start()
    for copy in suf_loads(0):
        copy.wait()
    suf_send(0).start()
    lens_send.wait()

    row_ids = lax.broadcasted_iota(jnp.int32, (2 * PAD, 128), 0)
    key_ids = lax.broadcasted_iota(jnp.int32, (2 * PAD, 128), 1)
    key_slot = jnp.where(lax.rem(key_ids, 4) == 2 * core + row_ids // PAD, key_ids // 4, slots)[None]

    def update_x(parity, j):
        copy = part_send(parity, j)
        copy.wait_recv()
        copy.wait_send()
        update = (own_buf[j] + recv_buf[parity, j]).astype(BF16)
        cols = slice(j * TILE, (j + 1) * TILE)
        x_buf[:, cols] = (x_buf[:, cols].astype(F32) + update.astype(F32)).astype(BF16)

    def layer_body(layer, carry):
        parity_in = lax.rem(layer + 1, 2)
        parity_out = lax.rem(layer, 2)

        @pl.when(layer < layers - 3)
        def _():
            for copy in raw_loads(layer + 3):
                copy.start()

        for k in range(3):
            pre_remote(layer, k).wait_send()

        @pl.when(layer < layers - 2)
        def _():
            for copy in suf_loads(layer + 2):
                copy.start()
            split_prefix(layer + 2)

        for i, (a, b) in enumerate(blocks):
            if i == 0:
                for copy in qkv_copies(layer, 0):
                    copy.wait()
            if i + 1 < len(blocks):
                for copy in qkv_copies(layer, i + 1):
                    copy.wait()
            for j in range(a, b):
                update_x(parity_in, j)
            r = slice(a * TILE, b * TILE)
            x = x_buf[:, r]
            parts = ((slice(0, q_width), wq_buf), (slice(q_width, q_width + kv_width), wk_buf),
                     (slice(q_width + kv_width, q_width + 2 * kv_width), wv_buf))
            for cols, w_buf in parts:
                product = jnp.dot(x, w_buf[r, :], preferred_element_type=F32)
                acc_buf[:, cols] = product if i == 0 else acc_buf[:, cols] + product

            @pl.when(layer < layers - 1)
            def _():
                for copy in qkv_copies(layer + 1, i):
                    copy.start()
                if i == 0:
                    for copy in suf_loads(layer + 1):
                        copy.wait()
                    suf_send(layer + 1).start()

            if i == 0:
                @pl.when(layer < layers - 2)
                def _():
                    for k in range(3):
                        pre_remote(layer + 2, k).start()

        for h in range(2):
            for g in range(group):
                col = (h * group + g) * head_dim
                q_buf[pl.ds(h * PAD + g, both, stride=2 * PAD), :] = acc_buf[:, col:col + head_dim].astype(BF16).astype(F32)
            for kv in range(2):
                col = q_width + kv * kv_width + h * head_dim
                fresh = acc_buf[:, col:col + head_dim].astype(BF16).astype(F32)
                kvn_buf[kv, h] = fresh
        for h in range(2):
            for kv in range(2):
                kv_out_ref[layer, kv, core * half_heads + h] = kvn_buf[kv, h, pl.ds(mine, rows), :]
                kv_send_buf[layer, kv, h] = kvn_buf[kv, h, pl.ds(other, rows), :]

        for k in range(3):
            pre_remote(layer, k).wait_recv()
        suf_send(layer).wait()

        @pl.when(layer == layers - 1)
        def _():
            kv_send.start()

        per_core = rows // CHUNK

        def unpair(both_seqs):
            first_seq = both_seqs[:, None, 0:2 * PAD, 0:128]
            second_seq = both_seqs[:, None, 2 * PAD:4 * PAD, 128:256]
            return jnp.concatenate([first_seq, second_seq], axis=1).reshape(CHUNK, 2 * PAD, 128)

        def attend(i):
            away = i // per_core
            part = pl.multiple_of(lax.rem(i, per_core) * CHUNK, CHUNK)
            first = pl.multiple_of(lax.rem(core + away, 2) * rows + part, CHUNK)
            slot = (1 - away) * lax.rem(layer, 3) + away * (3 + lax.rem(layer, 2))
            chunk_rows = pl.ds(pl.multiple_of(first * 2 * PAD, CHUNK * 2 * PAD), CHUNK * 2 * PAD)
            q = q_buf[chunk_rows, :]
            q3 = q.reshape(CHUNK, 2 * PAD, head_dim)
            k_suf = suf_buf[slot, 0, pl.ds(part, CHUNK)]
            v_suf = suf_buf[slot, 1, pl.ds(part, CHUNK)]
            q_pairs = q3.astype(BF16).reshape(CHUNK // 2, 4 * PAD, head_dim)
            k_pairs = k_suf.reshape(CHUNK // 2, 256, head_dim)
            suf_scores = unpair(lax.dot_general(q_pairs, k_pairs, (((2,), (2,)), ((0,), (0,))), preferred_element_type=F32)) * scale
            suf_scores = jnp.where(key_slot < lens_buf[pl.ds(first, CHUNK)], suf_scores, -jnp.inf)
            def spread(kv):
                picked = [jnp.broadcast_to(kvn_buf[kv, h, pl.ds(first + b, 1), :], (PAD, head_dim)) for b in range(CHUNK) for h in range(2)]
                return jnp.concatenate(picked, axis=0).reshape(CHUNK, 2 * PAD, head_dim)

            k_new = spread(0)
            v_new = spread(1)
            new_scores = jnp.sum(q3 * k_new, axis=-1, keepdims=True) * scale
            suf_weights, new_weights, masses, pre_vals = [], [], [], []
            for h in range(2):
                hs = slice(h * PAD, (h + 1) * PAD)
                q_h = q3[:, hs, :].reshape(CHUNK * PAD, head_dim).astype(BF16)
                k_pre = pre_buf[layer, 0, h].reshape(-1, head_dim)
                v_pre = pre_buf[layer, 1, h].reshape(-1, head_dim)
                scores = lax.dot_general(q_h, k_pre, (((1,), (1,)), ((), ())), preferred_element_type=F32) * scale
                suf_h = suf_scores[:, hs, :].reshape(CHUNK * PAD, 128)
                new_h = new_scores[:, hs, :].reshape(CHUNK * PAD, 1)
                peak = jnp.maximum(jnp.maximum(scores.max(axis=-1, keepdims=True), suf_h.max(axis=-1, keepdims=True)), new_h)
                pre_w = jnp.exp(scores - peak)
                suf_w = jnp.exp(suf_h - peak)
                new_w = jnp.exp(new_h - peak)
                masses.append(pre_w.sum(axis=-1, keepdims=True) + suf_w.sum(axis=-1, keepdims=True) + new_w)
                pre_vals.append(jnp.dot(pre_w.astype(BF16), v_pre, preferred_element_type=F32))
                suf_weights.append(suf_w.reshape(CHUNK, PAD, 128))
                new_weights.append(new_w)
            suf_w = jnp.concatenate(suf_weights, axis=1).astype(BF16)
            v_suf = v_suf.reshape(CHUNK // 2, 2, 128, head_dim)
            v_pairs = jnp.concatenate([v_suf[:, 0], v_suf[:, 1]], axis=-1)
            suf_w = suf_w.reshape(CHUNK // 2, 4 * PAD, 128)
            suf_vals = unpair(lax.dot_general(suf_w, v_pairs, (((2,), (1,)), ((0,), (0,))), preferred_element_type=F32))
            outs = []
            for h in range(2):
                hs = slice(h * PAD, (h + 1) * PAD)
                mixed = pre_vals[h] + suf_vals[:, hs, :].reshape(CHUNK * PAD, head_dim)
                mixed = mixed + new_weights[h] * v_new[:, hs, :].reshape(CHUNK * PAD, head_dim)
                outs.append((mixed / masses[h]).reshape(CHUNK, PAD, head_dim))
            o_buf[chunk_rows, :] = jnp.concatenate(outs, axis=1).reshape(CHUNK * 2 * PAD, head_dim)

        def attend_trip(trip, carry):
            for i in range(CHUNKS_PER_TRIP):
                attend(trip * CHUNKS_PER_TRIP + i)
            return carry

        lax.fori_loop(0, 2 * per_core // CHUNKS_PER_TRIP, attend_trip, 0)
        wo_copy(layer, 0).wait()

        for h in range(2):
            for g in range(group):
                col = (h * group + g) * head_dim
                att_buf[:, col:col + head_dim] = o_buf[pl.ds(h * PAD + g, both, stride=2 * PAD), :].astype(BF16)

        for i, (a, b) in enumerate(blocks):
            if i + 1 < len(blocks):
                wo_copy(layer, i + 1).wait()
            product = jnp.dot(att_buf[...], wo_buf[:, a * TILE:b * TILE], preferred_element_type=F32)
            for j in range(a, b):
                own_buf[j] = product[:, (j - a) * TILE:(j - a + 1) * TILE]

            @pl.when(layer < layers - 1)
            def _():
                wo_copy(layer + 1, i).start()

            for j in range(a, b):
                part_send(parity_out, j).start()

        return carry

    lax.fori_loop(0, layers, layer_body, 0)
    for j in range(tiles):
        update_x((layers - 1) % 2, j)
        out_ref[:, j * TILE:(j + 1) * TILE] = x_buf[pl.ds(mine, rows), j * TILE:(j + 1) * TILE]
    kv_send.wait()


def cache_kernel(lens_ref, new_ref, k_ref, v_ref, k_out_ref, v_out_ref, buf, new_buf, in_sem, out_sem, new_sem):
    layers, rows, _, heads, _ = k_ref.shape
    ahead = RING // 2

    def loads(layer):
        slot = lax.rem(layer, RING)
        return (
            pltpu.make_async_copy(k_ref.at[layer], buf.at[slot, 0], in_sem.at[slot, 0]),
            pltpu.make_async_copy(v_ref.at[layer], buf.at[slot, 1], in_sem.at[slot, 1]),
            pltpu.make_async_copy(new_ref.at[layer], new_buf.at[slot], new_sem.at[slot]),
        )

    def stores(layer):
        slot = lax.rem(layer, RING)
        return (
            pltpu.make_async_copy(buf.at[slot, 0], k_out_ref.at[layer], out_sem.at[slot, 0]),
            pltpu.make_async_copy(buf.at[slot, 1], v_out_ref.at[layer], out_sem.at[slot, 1]),
        )

    for layer in range(ahead):
        for copy in loads(layer):
            copy.start()

    def step(layer, carry):
        slot = lax.rem(layer, RING)

        @pl.when(layer >= ahead)
        def _():
            for copy in stores(layer - ahead):
                copy.wait()

        @pl.when(layer < layers - ahead)
        def _():
            for copy in loads(layer + ahead):
                copy.start()

        for copy in loads(layer):
            copy.wait()
        for b in range(rows):
            for kv in range(2):
                buf[slot, kv, b, lens_ref[b]] = new_buf[slot, kv, pl.ds(b, heads, stride=rows), :].astype(BF16)
        for copy in stores(layer):
            copy.start()
        return carry

    lax.fori_loop(0, layers, step, 0)
    for layer in range(layers - ahead, layers):
        for copy in stores(layer):
            copy.wait()


def solution(mesh):
    home_axes = ('data', 'ctx')
    row_spec = P(home_axes, None)
    lens_spec = P(home_axes)
    whole_spec = P()
    prefix_spec = P(None, home_axes, None, None)
    cache_spec = P(None, home_axes, None, None, None)

    def local_step(hidden, seq_lens, w_query, w_key, w_value, w_out, k_prefix, v_prefix, k_suffix, v_suffix):
        layers, model_dim = w_query.shape[:2]
        positions, kv_heads, head_dim = k_prefix.shape[1:]
        rows = hidden.shape[0]
        slots = k_suffix.shape[2]
        group = w_query.shape[2] // head_dim // kv_heads
        half_heads = kv_heads // 2
        q_width = w_query.shape[2] // 2
        kv_width = w_key.shape[2] // 2
        tiles = model_dim // TILE
        keys = slots * kv_heads
        both = 2 * rows

        k_flat = k_suffix.reshape(layers, rows, keys, head_dim)
        v_flat = v_suffix.reshape(layers, rows, keys, head_dim)
        k_pre = k_prefix.reshape(layers, positions * kv_heads, head_dim)
        v_pre = v_prefix.reshape(layers, positions * kv_heads, head_dim)

        any_spec = pl.BlockSpec(memory_space=pl.ANY)
        smem_spec = pl.BlockSpec(memory_space=pltpu.SMEM)
        vmem_spec = pl.BlockSpec(memory_space=pltpu.VMEM)
        dma = pltpu.SemaphoreType.DMA
        hidden_out, kv_new = pl.pallas_call(
            functools.partial(decode_kernel, (layers, rows, group, head_dim, slots)),
            out_shape=(jax.ShapeDtypeStruct((rows, model_dim), BF16),
                       jax.ShapeDtypeStruct((layers, 2, kv_heads, rows, head_dim), F32)),
            in_specs=[vmem_spec, vmem_spec] + [any_spec] * 8,
            out_specs=(vmem_spec, vmem_spec),
            scratch_shapes=[
                pltpu.VMEM((model_dim, q_width), BF16),
                pltpu.VMEM((model_dim, kv_width), BF16),
                pltpu.VMEM((model_dim, kv_width), BF16),
                pltpu.VMEM((q_width, model_dim), BF16),
                pltpu.VMEM((layers, 2, half_heads, 4, positions, head_dim), BF16),
                pltpu.VMEM((2, 2, positions * kv_heads, head_dim), BF16),
                pltpu.VMEM((2, positions * kv_heads, head_dim), F32),
                pltpu.VMEM((2, 2, 2, half_heads, positions, head_dim), BF16),
                pltpu.VMEM((5, 2, rows, keys, head_dim), BF16),
                pltpu.VMEM((both, model_dim), BF16),
                pltpu.VMEM((tiles, both, TILE), F32),
                pltpu.VMEM((2, tiles, both, TILE), F32),
                pltpu.VMEM((both, q_width + 2 * kv_width), F32),
                pltpu.VMEM((both * 2 * PAD, head_dim), F32),
                pltpu.VMEM((2, half_heads, both, head_dim), F32),
                pltpu.VMEM((both * 2 * PAD, head_dim), F32),
                pltpu.VMEM((both, q_width), BF16),
                pltpu.VMEM((both, 2 * PAD, 128), jnp.int32),
                pltpu.VMEM((layers, 2, half_heads, rows, head_dim), F32),
                dma((4, -(-tiles // BLOCK))), dma((3, 2)), dma((2,)), dma((2,)), dma((2, 2)), dma((layers, 3)), dma((layers, 3)),
                dma((tiles,)), dma((2, tiles)), dma((2,)), dma((2,)),
            ],
            compiler_params=pltpu.CompilerParams(collective_id=0, has_side_effects=True, vmem_limit_bytes=66_000_000),
            name="decode_layers",
        )(seq_lens.reshape(1, rows), hidden, w_query, w_key, w_value, w_out, k_pre, v_pre, k_flat, v_flat)

        k_out, v_out = pl.pallas_call(
            cache_kernel,
            out_shape=(jax.ShapeDtypeStruct(k_suffix.shape, BF16), jax.ShapeDtypeStruct(v_suffix.shape, BF16)),
            in_specs=[smem_spec] + [any_spec] * 3,
            out_specs=(any_spec, any_spec),
            scratch_shapes=[
                pltpu.VMEM((RING, 2) + k_suffix.shape[1:], BF16),
                pltpu.VMEM((RING, 2, kv_heads * rows, head_dim), F32),
                dma((RING, 2)), dma((RING, 2)), dma((RING,)),
            ],
            compiler_params=pltpu.CompilerParams(vmem_limit_bytes=60_000_000),
            name="write_caches",
        )(seq_lens, kv_new.reshape(layers, 2, kv_heads * rows, head_dim), k_suffix, v_suffix)
        return hidden_out, k_out, v_out

    return jax.shard_map(local_step, mesh=mesh, in_specs=(row_spec, lens_spec, whole_spec, whole_spec, whole_spec, whole_spec, prefix_spec, prefix_spec, cache_spec, cache_spec), out_specs=(row_spec, cache_spec, cache_spec), check_vma=False)
```

```python
import functools

import jax
import jax.numpy as jnp
from jax import lax
from jax.experimental import pallas as pl
from jax.experimental.pallas import tpu as pltpu
from jax.sharding import PartitionSpec as P

MESH = pl.DeviceIdType.MESH
BF16 = jnp.bfloat16
F32 = jnp.float32
TILE = 512
CHUNK = 32
PAD = 8
RING = 8
BLOCK = 2
LOG2E = 1.4426950408889634
CHUNKS_PER_TRIP = 1


def decode_kernel(dims, lens_ref, hidden_ref, wq_ref, wk_ref, wv_ref, wo_ref, kpre_ref, vpre_ref, ksuf_ref, vsuf_ref,
                  out_ref, kv_out_ref,
                  wq_buf, wk_buf, wv_buf, wo_buf, pre_buf, raw_buf, wide_buf, split_buf, suf_buf, x_buf, own_buf, recv_buf, acc_buf,
                  q_buf, kvn_buf, o_buf, att_buf, lens_buf, kv_mine_buf, kv_send_buf,
                  w_sem, suf_load_sem, suf_send_sem, suf_recv_sem, raw_sem, pre_send_sem, pre_recv_sem,
                  part_send_sem, part_recv_sem, lens_sem, kv_sem):
    layers, rows, group, head_dim, slots = dims
    half_heads = 2
    tiles = own_buf.shape[0]
    q_width = wq_buf.shape[1]
    kv_width = wk_buf.shape[1]
    blocks = [(a, min(a + BLOCK, tiles)) for a in range(0, tiles, BLOCK)]
    both = 2 * rows
    me = lax.axis_index("ctx")
    core = lax.rem(me, 2)
    chip = me // 2
    mate = chip * 2 + (1 - core)
    across = (1 - chip) * 2 + core
    diagonal = (1 - chip) * 2 + (1 - core)
    peers = ((mate, 1 - core), (across, core), (diagonal, 1 - core))
    mine = pl.multiple_of(core * rows, rows)
    other = pl.multiple_of((1 - core) * rows, rows)
    q_col = pl.multiple_of(core * q_width, 128)
    kv_col = pl.multiple_of(core * kv_width, 128)
    scale = head_dim ** -0.5

    def qkv_copies(layer, i):
        a, b = blocks[i]
        r = pl.ds(a * TILE, (b - a) * TILE)
        return (
            pltpu.make_async_copy(wq_ref.at[layer, r, pl.ds(q_col, q_width)], wq_buf.at[r], w_sem.at[0, i]),
            pltpu.make_async_copy(wk_ref.at[layer, r, pl.ds(kv_col, kv_width)], wk_buf.at[r], w_sem.at[1, i]),
            pltpu.make_async_copy(wv_ref.at[layer, r, pl.ds(kv_col, kv_width)], wv_buf.at[r], w_sem.at[2, i]),
        )

    def wo_copy(layer, i):
        a, b = blocks[i]
        cols = pl.ds(a * TILE, (b - a) * TILE)
        return pltpu.make_async_copy(wo_ref.at[layer, pl.ds(q_col, q_width), cols], wo_buf.at[:, cols], w_sem.at[3, i])

    def suf_loads(layer):
        slot = lax.rem(layer, 3)
        return (
            pltpu.make_async_copy(ksuf_ref.at[layer], suf_buf.at[slot, 0], suf_load_sem.at[slot, 0]),
            pltpu.make_async_copy(vsuf_ref.at[layer], suf_buf.at[slot, 1], suf_load_sem.at[slot, 1]),
        )

    def suf_send(layer):
        return pltpu.make_async_remote_copy(
            src_ref=suf_buf.at[lax.rem(layer, 3)], dst_ref=suf_buf.at[3 + lax.rem(layer, 2)],
            send_sem=suf_send_sem.at[lax.rem(layer, 2)], recv_sem=suf_recv_sem.at[lax.rem(layer, 2)],
            device_id={"ctx": mate}, device_id_type=MESH)

    def raw_loads(layer):
        slot = lax.rem(layer, 2)
        return (
            pltpu.make_async_copy(kpre_ref.at[layer], raw_buf.at[slot, 0], raw_sem.at[slot, 0]),
            pltpu.make_async_copy(vpre_ref.at[layer], raw_buf.at[slot, 1], raw_sem.at[slot, 1]),
        )

    def split_prefix(layer):
        slot = lax.rem(layer, 2)
        heads = 2 * half_heads
        positions = pre_buf.shape[4]
        for copy in raw_loads(layer):
            copy.wait()
        for kv in range(2):
            wide_buf[kv] = raw_buf[slot, kv].astype(F32)
            for h in range(half_heads):
                for half in range(2):
                    split_buf[slot, half, kv, h] = wide_buf[kv, pl.ds(half * half_heads + h, positions, stride=heads), :].astype(BF16)
                pre_buf[layer, kv, h, me] = split_buf[slot, core, kv, h]

    def pre_remote(layer, k):
        device, half = peers[k]
        return pltpu.make_async_remote_copy(
            src_ref=split_buf.at[lax.rem(layer, 2), half], dst_ref=pre_buf.at[layer, :, :, me],
            send_sem=pre_send_sem.at[layer, k], recv_sem=pre_recv_sem.at[layer, k],
            device_id={"ctx": device}, device_id_type=MESH)

    def part_send(parity, j):
        return pltpu.make_async_remote_copy(
            src_ref=own_buf.at[j], dst_ref=recv_buf.at[parity, j],
            send_sem=part_send_sem.at[j], recv_sem=part_recv_sem.at[parity, j],
            device_id={"ctx": mate}, device_id_type=MESH)

    lens_send = pltpu.make_async_remote_copy(
        src_ref=lens_buf.at[pl.ds(mine, rows)], dst_ref=lens_buf.at[pl.ds(mine, rows)], send_sem=lens_sem.at[0], recv_sem=lens_sem.at[1],
        device_id={"ctx": mate}, device_id_type=MESH)
    kv_slice = kv_out_ref.at[:, :, pl.ds(core * half_heads, half_heads)]
    kv_store = pltpu.make_async_copy(kv_mine_buf, kv_slice, kv_sem.at[2])
    kv_send = pltpu.make_async_remote_copy(
        src_ref=kv_send_buf, dst_ref=kv_slice, send_sem=kv_sem.at[0], recv_sem=kv_sem.at[1],
        device_id={"ctx": mate}, device_id_type=MESH)

    for layer in range(2):
        for copy in raw_loads(layer):
            copy.start()
    for i in range(len(blocks)):
        for copy in qkv_copies(0, i):
            copy.start()
        if i == 0:
            for copy in suf_loads(0):
                copy.start()
    for i in range(len(blocks)):
        wo_copy(0, i).start()
    for copy in suf_loads(1):
        copy.start()

    x_buf[...] = jnp.zeros_like(x_buf)
    for j in range(tiles):
        own_buf[j] = jnp.zeros_like(own_buf[j])
        own_buf[j, pl.ds(mine, rows), :] = hidden_ref[:, j * TILE:(j + 1) * TILE].astype(F32)
    diagonal_hit = lax.broadcasted_iota(jnp.int32, (rows, rows), 0) == lax.broadcasted_iota(jnp.int32, (rows, rows), 1)
    lens_wide = jnp.broadcast_to(lens_ref[...].astype(F32), (rows, rows))
    lens_wide = jnp.where(diagonal_hit, lens_wide, 0.0).sum(axis=1, keepdims=True)
    lens_wide = jnp.broadcast_to(lens_wide, (rows, 128)).astype(jnp.int32)
    for b in range(rows):
        lens_buf[mine + b] = jnp.broadcast_to(lens_wide[b:b + 1, :], (2 * PAD, 128))
    q_buf[...] = jnp.zeros_like(q_buf)
    split_prefix(0)
    for copy in raw_loads(2):
        copy.start()
    split_prefix(1)

    barrier = pltpu.get_barrier_semaphore()
    for device, _ in peers:
        pl.semaphore_signal(barrier, inc=1, device_id={"ctx": device}, device_id_type=MESH)
    pl.semaphore_wait(barrier, 3)

    for j in range(tiles):
        part_send(1, j).start()
    lens_send.start()
    for layer in range(2):
        for k in range(3):
            pre_remote(layer, k).start()
    for copy in suf_loads(0):
        copy.wait()
    suf_send(0).start()
    lens_send.wait()

    row_ids = lax.broadcasted_iota(jnp.int32, (2 * PAD, 128), 0)
    key_ids = lax.broadcasted_iota(jnp.int32, (2 * PAD, 128), 1)
    key_slot = jnp.where(lax.rem(key_ids, 4) == 2 * core + row_ids // PAD, key_ids // 4, slots)[None]

    def await_part(parity, j):
        copy = part_send(parity, j)
        copy.wait_recv()
        copy.wait_send()

    def update_x(parity, j):
        update = (own_buf[j] + recv_buf[parity, j]).astype(BF16)
        cols = slice(j * TILE, (j + 1) * TILE)
        x_buf[:, cols] = (x_buf[:, cols].astype(F32) + update.astype(F32)).astype(BF16)

    def layer_body(layer, carry):
        parity_in = lax.rem(layer + 1, 2)
        parity_out = lax.rem(layer, 2)

        @pl.when(layer < layers - 3)
        def _():
            for copy in raw_loads(layer + 3):
                copy.start()

        for k in range(3):
            pre_remote(layer, k).wait_send()

        @pl.when(layer < layers - 2)
        def _():
            for copy in suf_loads(layer + 2):
                copy.start()
            split_prefix(layer + 2)

        for i, (a, b) in enumerate(blocks):
            if i == 0:
                for copy in qkv_copies(layer, 0):
                    copy.wait()
            if i + 1 < len(blocks):
                for copy in qkv_copies(layer, i + 1):
                    copy.wait()
            for j in range(a, b):
                await_part(parity_in, j)
            for j in range(a, b):
                update_x(parity_in, j)
            r = slice(a * TILE, b * TILE)
            x = x_buf[:, r]
            parts = ((slice(0, q_width), wq_buf), (slice(q_width, q_width + kv_width), wk_buf),
                     (slice(q_width + kv_width, q_width + 2 * kv_width), wv_buf))
            for cols, w_buf in parts:
                product = jnp.dot(x, w_buf[r, :], preferred_element_type=F32)
                acc_buf[:, cols] = product if i == 0 else acc_buf[:, cols] + product

            @pl.when(layer < layers - 1)
            def _():
                for copy in qkv_copies(layer + 1, i):
                    copy.start()
                if i == 0:
                    for copy in suf_loads(layer + 1):
                        copy.wait()
                    suf_send(layer + 1).start()

            if i == 0:
                @pl.when(layer < layers - 2)
                def _():
                    for k in range(3):
                        pre_remote(layer + 2, k).start()

        for h in range(2):
            for g in range(group):
                col = (h * group + g) * head_dim
                q_buf[pl.ds(h * PAD + g, both, stride=2 * PAD), :] = acc_buf[:, col:col + head_dim].astype(BF16).astype(F32)
            for kv in range(2):
                col = q_width + kv * kv_width + h * head_dim
                fresh = acc_buf[:, col:col + head_dim].astype(BF16).astype(F32)
                kvn_buf[kv, h] = fresh
        for h in range(2):
            for kv in range(2):
                kv_mine_buf[layer, kv, h] = kvn_buf[kv, h, pl.ds(mine, rows), :]
                kv_send_buf[layer, kv, h] = kvn_buf[kv, h, pl.ds(other, rows), :]

        for k in range(3):
            pre_remote(layer, k).wait_recv()
        suf_send(layer).wait()

        per_core = rows // CHUNK

        def unpair(both_seqs):
            first_seq = both_seqs[:, None, 0:2 * PAD, 0:128]
            second_seq = both_seqs[:, None, 2 * PAD:4 * PAD, 128:256]
            return jnp.concatenate([first_seq, second_seq], axis=1).reshape(CHUNK, 2 * PAD, 128)

        def attend(i):
            away = i // per_core
            part = pl.multiple_of(lax.rem(i, per_core) * CHUNK, CHUNK)
            first = pl.multiple_of(lax.rem(core + away, 2) * rows + part, CHUNK)
            slot = (1 - away) * lax.rem(layer, 3) + away * (3 + lax.rem(layer, 2))
            chunk_rows = pl.ds(pl.multiple_of(first * 2 * PAD, CHUNK * 2 * PAD), CHUNK * 2 * PAD)
            q = q_buf[chunk_rows, :]
            q3 = q.reshape(CHUNK, 2 * PAD, head_dim)
            k_suf = suf_buf[slot, 0, pl.ds(part, CHUNK)]
            v_suf = suf_buf[slot, 1, pl.ds(part, CHUNK)]
            q_pairs = q3.astype(BF16).reshape(CHUNK // 2, 4 * PAD, head_dim)
            k_pairs = k_suf.reshape(CHUNK // 2, 256, head_dim)
            suf_scores = unpair(lax.dot_general(q_pairs, k_pairs, (((2,), (2,)), ((0,), (0,))), preferred_element_type=F32))
            suf_scores = jnp.where(key_slot < lens_buf[pl.ds(first, CHUNK)], suf_scores, -jnp.inf)
            def spread(kv):
                picked = [jnp.broadcast_to(kvn_buf[kv, h, pl.ds(first + b, 1), :], (PAD, head_dim)) for b in range(CHUNK) for h in range(2)]
                return jnp.concatenate(picked, axis=0).reshape(CHUNK, 2 * PAD, head_dim)

            k_new = spread(0)
            v_new = spread(1)
            new_scores = jnp.sum(q3 * k_new, axis=-1, keepdims=True)
            suf_weights, new_weights, masses, pre_vals = [], [], [], []
            for h in range(2):
                hs = slice(h * PAD, (h + 1) * PAD)
                q_h = q3[:, hs, :].reshape(CHUNK * PAD, head_dim).astype(BF16)
                k_pre = pre_buf[layer, 0, h].reshape(-1, head_dim)
                v_pre = pre_buf[layer, 1, h].reshape(-1, head_dim)
                scores = lax.dot_general(q_h, k_pre, (((1,), (1,)), ((), ())), preferred_element_type=F32)
                suf_h = suf_scores[:, hs, :].reshape(CHUNK * PAD, 128)
                new_h = new_scores[:, hs, :].reshape(CHUNK * PAD, 1)
                peak = jnp.maximum(jnp.maximum(scores.max(axis=-1, keepdims=True), suf_h.max(axis=-1, keepdims=True)), new_h)
                pre_w = jnp.exp2((scores - peak) * (scale * LOG2E))
                suf_w = jnp.exp2((suf_h - peak) * (scale * LOG2E))
                new_w = jnp.exp2((new_h - peak) * (scale * LOG2E))
                masses.append(pre_w.sum(axis=-1, keepdims=True) + suf_w.sum(axis=-1, keepdims=True) + new_w)
                pre_vals.append(jnp.dot(pre_w.astype(BF16), v_pre, preferred_element_type=F32))
                suf_weights.append(suf_w.reshape(CHUNK, PAD, 128))
                new_weights.append(new_w)
            suf_w = jnp.concatenate(suf_weights, axis=1).astype(BF16)
            v_suf = v_suf.reshape(CHUNK // 2, 2, 128, head_dim)
            v_pairs = jnp.concatenate([v_suf[:, 0], v_suf[:, 1]], axis=-1)
            suf_w = suf_w.reshape(CHUNK // 2, 4 * PAD, 128)
            suf_vals = unpair(lax.dot_general(suf_w, v_pairs, (((2,), (1,)), ((0,), (0,))), preferred_element_type=F32))
            outs = []
            for h in range(2):
                hs = slice(h * PAD, (h + 1) * PAD)
                mixed = pre_vals[h] + suf_vals[:, hs, :].reshape(CHUNK * PAD, head_dim)
                mixed = mixed + new_weights[h] * v_new[:, hs, :].reshape(CHUNK * PAD, head_dim)
                outs.append((mixed / masses[h]).reshape(CHUNK, PAD, head_dim))
            o_buf[chunk_rows, :] = jnp.concatenate(outs, axis=1).reshape(CHUNK * 2 * PAD, head_dim)

        def attend_trip(trip, carry):
            for i in range(CHUNKS_PER_TRIP):
                attend(trip * CHUNKS_PER_TRIP + i)
            return carry

        lax.fori_loop(0, 2 * per_core // CHUNKS_PER_TRIP, attend_trip, 0)

        @pl.when(layer == layers - 1)
        def _():
            kv_store.start()
            kv_send.start()

        wo_copy(layer, 0).wait()
        wo_copy(layer, 1).wait()

        for h in range(2):
            for g in range(group):
                col = (h * group + g) * head_dim
                att_buf[:, col:col + head_dim] = o_buf[pl.ds(h * PAD + g, both, stride=2 * PAD), :].astype(BF16)

        for i, (a, b) in enumerate(blocks):
            if 0 < i < len(blocks) - 1:
                wo_copy(layer, i + 1).wait()
            product = jnp.dot(att_buf[...], wo_buf[:, a * TILE:b * TILE], preferred_element_type=F32)
            for j in range(a, b):
                own_buf[j] = product[:, (j - a) * TILE:(j - a + 1) * TILE]

            @pl.when(layer < layers - 1)
            def _():
                wo_copy(layer + 1, i).start()

            for j in range(a, b):
                part_send(parity_out, j).start()

        return carry

    lax.fori_loop(0, layers, layer_body, 0)
    for j in range(tiles):
        await_part((layers - 1) % 2, j)
    for j in range(tiles):
        update_x((layers - 1) % 2, j)
        out_ref[:, j * TILE:(j + 1) * TILE] = x_buf[pl.ds(mine, rows), j * TILE:(j + 1) * TILE]
    kv_store.wait()
    kv_send.wait()


def cache_kernel(lens_ref, new_ref, hidden_ref, k_ref, v_ref, hidden_out_ref, k_out_ref, v_out_ref,
                 buf, new_buf, hidden_buf, in_sem, out_sem, new_sem, hidden_sem):
    layers, rows, _, heads, _ = k_ref.shape
    ahead = RING // 2

    def loads(layer):
        slot = lax.rem(layer, RING)
        return (
            pltpu.make_async_copy(new_ref.at[layer], new_buf.at[slot], new_sem.at[slot]),
            pltpu.make_async_copy(k_ref.at[layer], buf.at[slot, 0], in_sem.at[slot, 0]),
            pltpu.make_async_copy(v_ref.at[layer], buf.at[slot, 1], in_sem.at[slot, 1]),
        )

    def stores(layer):
        slot = lax.rem(layer, RING)
        return (
            pltpu.make_async_copy(buf.at[slot, 0], k_out_ref.at[layer], out_sem.at[slot, 0]),
            pltpu.make_async_copy(buf.at[slot, 1], v_out_ref.at[layer], out_sem.at[slot, 1]),
        )

    for layer in range(ahead):
        for copy in loads(layer):
            copy.start()
    hidden_load = pltpu.make_async_copy(hidden_ref, hidden_buf, hidden_sem.at[0])
    hidden_store = pltpu.make_async_copy(hidden_buf, hidden_out_ref, hidden_sem.at[1])
    hidden_load.start()

    def step(layer, carry):
        slot = lax.rem(layer, RING)

        @pl.when(layer >= ahead)
        def _():
            for copy in stores(layer - ahead):
                copy.wait()

        @pl.when(layer < layers - ahead)
        def _():
            for copy in loads(layer + ahead):
                copy.start()

        arrivals = loads(layer)
        arrivals[0].wait()
        for kv in range(2):
            arrivals[1 + kv].wait()
            for b in range(rows):
                buf[slot, kv, b, lens_ref[b]] = new_buf[slot, kv, pl.ds(b, heads, stride=rows), :].astype(BF16)
            stores(layer)[kv].start()
        return carry

    lax.fori_loop(0, layers, step, 0)
    hidden_load.wait()
    hidden_store.start()
    for layer in range(layers - ahead, layers):
        for copy in stores(layer):
            copy.wait()
    hidden_store.wait()


def solution(mesh):
    home_axes = ('data', 'ctx')
    row_spec = P(home_axes, None)
    lens_spec = P(home_axes)
    whole_spec = P()
    prefix_spec = P(None, home_axes, None, None)
    cache_spec = P(None, home_axes, None, None, None)

    def local_step(hidden, seq_lens, w_query, w_key, w_value, w_out, k_prefix, v_prefix, k_suffix, v_suffix):
        layers, model_dim = w_query.shape[:2]
        positions, kv_heads, head_dim = k_prefix.shape[1:]
        rows = hidden.shape[0]
        slots = k_suffix.shape[2]
        group = w_query.shape[2] // head_dim // kv_heads
        half_heads = kv_heads // 2
        q_width = w_query.shape[2] // 2
        kv_width = w_key.shape[2] // 2
        tiles = model_dim // TILE
        keys = slots * kv_heads
        both = 2 * rows

        k_flat = k_suffix.reshape(layers, rows, keys, head_dim)
        v_flat = v_suffix.reshape(layers, rows, keys, head_dim)
        k_pre = k_prefix.reshape(layers, positions * kv_heads, head_dim)
        v_pre = v_prefix.reshape(layers, positions * kv_heads, head_dim)

        any_spec = pl.BlockSpec(memory_space=pl.ANY)
        smem_spec = pl.BlockSpec(memory_space=pltpu.SMEM)
        vmem_spec = pl.BlockSpec(memory_space=pltpu.VMEM)
        dma = pltpu.SemaphoreType.DMA
        hidden_out, kv_new = pl.pallas_call(
            functools.partial(decode_kernel, (layers, rows, group, head_dim, slots)),
            out_shape=(jax.ShapeDtypeStruct((rows, model_dim), BF16),
                       jax.ShapeDtypeStruct((layers, 2, kv_heads, rows, head_dim), F32)),
            in_specs=[vmem_spec, vmem_spec] + [any_spec] * 8,
            out_specs=(vmem_spec, any_spec),
            scratch_shapes=[
                pltpu.VMEM((model_dim, q_width), BF16),
                pltpu.VMEM((model_dim, kv_width), BF16),
                pltpu.VMEM((model_dim, kv_width), BF16),
                pltpu.VMEM((q_width, model_dim), BF16),
                pltpu.VMEM((layers, 2, half_heads, 4, positions, head_dim), BF16),
                pltpu.VMEM((2, 2, positions * kv_heads, head_dim), BF16),
                pltpu.VMEM((2, positions * kv_heads, head_dim), F32),
                pltpu.VMEM((2, 2, 2, half_heads, positions, head_dim), BF16),
                pltpu.VMEM((5, 2, rows, keys, head_dim), BF16),
                pltpu.VMEM((both, model_dim), BF16),
                pltpu.VMEM((tiles, both, TILE), F32),
                pltpu.VMEM((2, tiles, both, TILE), F32),
                pltpu.VMEM((both, q_width + 2 * kv_width), F32),
                pltpu.VMEM((both * 2 * PAD, head_dim), F32),
                pltpu.VMEM((2, half_heads, both, head_dim), F32),
                pltpu.VMEM((both * 2 * PAD, head_dim), F32),
                pltpu.VMEM((both, q_width), BF16),
                pltpu.VMEM((both, 2 * PAD, 128), jnp.int32),
                pltpu.VMEM((layers, 2, half_heads, rows, head_dim), F32),
                pltpu.VMEM((layers, 2, half_heads, rows, head_dim), F32),
                dma((4, -(-tiles // BLOCK))), dma((3, 2)), dma((2,)), dma((2,)), dma((2, 2)), dma((layers, 3)), dma((layers, 3)),
                dma((tiles,)), dma((2, tiles)), dma((2,)), dma((3,)),
            ],
            compiler_params=pltpu.CompilerParams(collective_id=0, has_side_effects=True, vmem_limit_bytes=66_000_000),
            name="decode_layers",
        )(seq_lens.reshape(1, rows), hidden, w_query, w_key, w_value, w_out, k_pre, v_pre, k_flat, v_flat)

        hidden_out, k_out, v_out = pl.pallas_call(
            cache_kernel,
            out_shape=(jax.ShapeDtypeStruct(hidden.shape, BF16), jax.ShapeDtypeStruct(k_suffix.shape, BF16), jax.ShapeDtypeStruct(v_suffix.shape, BF16)),
            in_specs=[smem_spec] + [any_spec] * 4,
            out_specs=(any_spec, any_spec, any_spec),
            scratch_shapes=[
                pltpu.VMEM((RING, 2) + k_suffix.shape[1:], BF16),
                pltpu.VMEM((RING, 2, kv_heads * rows, head_dim), F32),
                pltpu.VMEM(hidden.shape, BF16),
                dma((RING, 2)), dma((RING, 2)), dma((RING,)), dma((2,)),
            ],
            compiler_params=pltpu.CompilerParams(vmem_limit_bytes=60_000_000),
            name="write_caches",
        )(seq_lens, kv_new.reshape(layers, 2, kv_heads * rows, head_dim), hidden_out, k_suffix, v_suffix)
        return hidden_out, k_out, v_out

    return jax.shard_map(local_step, mesh=mesh, in_specs=(row_spec, lens_spec, whole_spec, whole_spec, whole_spec, whole_spec, prefix_spec, prefix_spec, cache_spec, cache_spec), out_specs=(row_spec, cache_spec, cache_spec), check_vma=False)
```

```python
import functools

import jax
import jax.numpy as jnp
from jax import lax
from jax.experimental import pallas as pl
from jax.experimental.pallas import tpu as pltpu
from jax.sharding import PartitionSpec as P

MESH = pl.DeviceIdType.MESH
BF16 = jnp.bfloat16
F32 = jnp.float32
TILE = 512
CHUNK = 32
PAD = 8
RING = 8
BLOCK = 2
LOG2E = 1.4426950408889634
CHUNKS_PER_TRIP = 1


def decode_kernel(dims, lens_ref, hidden_ref, wq_ref, wk_ref, wv_ref, wo_ref, kpre_ref, vpre_ref, ksuf_ref, vsuf_ref,
                  out_ref, kv_out_ref,
                  wq_buf, wk_buf, wv_buf, wo_buf, pre_buf, raw_buf, wide_buf, split_buf, suf_buf, x_buf, own_buf, recv_buf, acc_buf,
                  q_buf, kvn_buf, o_buf, att_buf, lens_buf, kv_mine_buf, kv_send_buf,
                  w_sem, suf_load_sem, suf_send_sem, suf_recv_sem, raw_sem, pre_send_sem, pre_recv_sem,
                  part_send_sem, part_recv_sem, lens_sem, kv_sem):
    layers, rows, group, head_dim, slots = dims
    half_heads = 2
    tiles = own_buf.shape[0]
    q_width = wq_buf.shape[1]
    kv_width = wk_buf.shape[1]
    blocks = [(i * BLOCK, (i + 1) * BLOCK if i < tiles // BLOCK - 1 else tiles) for i in range(tiles // BLOCK)]
    both = 2 * rows
    me = lax.axis_index("ctx")
    core = lax.rem(me, 2)
    chip = me // 2
    mate = chip * 2 + (1 - core)
    across = (1 - chip) * 2 + core
    diagonal = (1 - chip) * 2 + (1 - core)
    peers = ((mate, 1 - core), (across, core), (diagonal, 1 - core))
    mine = pl.multiple_of(core * rows, rows)
    other = pl.multiple_of((1 - core) * rows, rows)
    q_col = pl.multiple_of(core * q_width, 128)
    kv_col = pl.multiple_of(core * kv_width, 128)
    scale = head_dim ** -0.5

    def qkv_copies(layer, i):
        a, b = blocks[i]
        r = pl.ds(a * TILE, (b - a) * TILE)
        return (
            pltpu.make_async_copy(wq_ref.at[layer, r, pl.ds(q_col, q_width)], wq_buf.at[r], w_sem.at[0, i]),
            pltpu.make_async_copy(wk_ref.at[layer, r, pl.ds(kv_col, kv_width)], wk_buf.at[r], w_sem.at[1, i]),
            pltpu.make_async_copy(wv_ref.at[layer, r, pl.ds(kv_col, kv_width)], wv_buf.at[r], w_sem.at[2, i]),
        )

    def wo_copy(layer, i):
        a, b = blocks[i]
        cols = pl.ds(a * TILE, (b - a) * TILE)
        return pltpu.make_async_copy(wo_ref.at[layer, pl.ds(q_col, q_width), cols], wo_buf.at[:, cols], w_sem.at[3, i])

    def suf_loads(layer):
        slot = lax.rem(layer, 3)
        return (
            pltpu.make_async_copy(ksuf_ref.at[layer], suf_buf.at[slot, 0], suf_load_sem.at[slot, 0]),
            pltpu.make_async_copy(vsuf_ref.at[layer], suf_buf.at[slot, 1], suf_load_sem.at[slot, 1]),
        )

    def suf_send(layer):
        return pltpu.make_async_remote_copy(
            src_ref=suf_buf.at[lax.rem(layer, 3)], dst_ref=suf_buf.at[3 + lax.rem(layer, 2)],
            send_sem=suf_send_sem.at[lax.rem(layer, 2)], recv_sem=suf_recv_sem.at[lax.rem(layer, 2)],
            device_id={"ctx": mate}, device_id_type=MESH)

    def raw_loads(layer):
        slot = lax.rem(layer, 2)
        return (
            pltpu.make_async_copy(kpre_ref.at[layer], raw_buf.at[slot, 0], raw_sem.at[slot, 0]),
            pltpu.make_async_copy(vpre_ref.at[layer], raw_buf.at[slot, 1], raw_sem.at[slot, 1]),
        )

    def split_prefix(layer):
        slot = lax.rem(layer, 2)
        heads = 2 * half_heads
        positions = pre_buf.shape[4]
        for copy in raw_loads(layer):
            copy.wait()
        for kv in range(2):
            wide_buf[kv] = raw_buf[slot, kv].astype(F32)
            for h in range(half_heads):
                for half in range(2):
                    split_buf[slot, half, kv, h] = wide_buf[kv, pl.ds(half * half_heads + h, positions, stride=heads), :].astype(BF16)
                pre_buf[layer, kv, h, me] = split_buf[slot, core, kv, h]

    def pre_remote(layer, k):
        device, half = peers[k]
        return pltpu.make_async_remote_copy(
            src_ref=split_buf.at[lax.rem(layer, 2), half], dst_ref=pre_buf.at[layer, :, :, me],
            send_sem=pre_send_sem.at[layer, k], recv_sem=pre_recv_sem.at[layer, k],
            device_id={"ctx": device}, device_id_type=MESH)

    def part_send(parity, j):
        return pltpu.make_async_remote_copy(
            src_ref=own_buf.at[j], dst_ref=recv_buf.at[parity, j],
            send_sem=part_send_sem.at[j], recv_sem=part_recv_sem.at[parity, j],
            device_id={"ctx": mate}, device_id_type=MESH)

    lens_send = pltpu.make_async_remote_copy(
        src_ref=lens_buf.at[pl.ds(mine, rows)], dst_ref=lens_buf.at[pl.ds(mine, rows)], send_sem=lens_sem.at[0], recv_sem=lens_sem.at[1],
        device_id={"ctx": mate}, device_id_type=MESH)
    kv_slice = kv_out_ref.at[:, :, pl.ds(core * half_heads, half_heads)]
    kv_store = pltpu.make_async_copy(kv_mine_buf, kv_slice, kv_sem.at[2])
    kv_send = pltpu.make_async_remote_copy(
        src_ref=kv_send_buf, dst_ref=kv_slice, send_sem=kv_sem.at[0], recv_sem=kv_sem.at[1],
        device_id={"ctx": mate}, device_id_type=MESH)

    for layer in range(2):
        for copy in raw_loads(layer):
            copy.start()
    for i in range(len(blocks)):
        for copy in qkv_copies(0, i):
            copy.start()
        if i == 0:
            for copy in suf_loads(0):
                copy.start()
    for i in range(len(blocks)):
        wo_copy(0, i).start()
    for copy in suf_loads(1):
        copy.start()

    x_buf[...] = jnp.zeros_like(x_buf)
    for j in range(tiles):
        own_buf[j] = jnp.zeros_like(own_buf[j])
        own_buf[j, pl.ds(mine, rows), :] = hidden_ref[:, j * TILE:(j + 1) * TILE].astype(F32)
    diagonal_hit = lax.broadcasted_iota(jnp.int32, (rows, rows), 0) == lax.broadcasted_iota(jnp.int32, (rows, rows), 1)
    lens_wide = jnp.broadcast_to(lens_ref[...].astype(F32), (rows, rows))
    lens_wide = jnp.where(diagonal_hit, lens_wide, 0.0).sum(axis=1, keepdims=True)
    lens_wide = jnp.broadcast_to(lens_wide, (rows, 128)).astype(jnp.int32)
    for b in range(rows):
        lens_buf[mine + b] = jnp.broadcast_to(lens_wide[b:b + 1, :], (2 * PAD, 128))
    q_buf[...] = jnp.zeros_like(q_buf)
    split_prefix(0)
    for copy in raw_loads(2):
        copy.start()
    split_prefix(1)

    barrier = pltpu.get_barrier_semaphore()
    for device, _ in peers:
        pl.semaphore_signal(barrier, inc=1, device_id={"ctx": device}, device_id_type=MESH)
    pl.semaphore_wait(barrier, 3)

    for j in range(tiles):
        part_send(1, j).start()
    lens_send.start()
    for layer in range(2):
        for k in range(3):
            pre_remote(layer, k).start()
    for copy in suf_loads(0):
        copy.wait()
    suf_send(0).start()
    lens_send.wait()

    row_ids = lax.broadcasted_iota(jnp.int32, (2 * PAD, 128), 0)
    key_ids = lax.broadcasted_iota(jnp.int32, (2 * PAD, 128), 1)
    key_slot = jnp.where(lax.rem(key_ids, 4) == 2 * core + row_ids // PAD, key_ids // 4, slots)[None]

    def await_part(parity, j):
        copy = part_send(parity, j)
        copy.wait_recv()
        copy.wait_send()

    def update_x(parity, j):
        update = (own_buf[j] + recv_buf[parity, j]).astype(BF16)
        cols = slice(j * TILE, (j + 1) * TILE)
        x_buf[:, cols] = (x_buf[:, cols].astype(F32) + update.astype(F32)).astype(BF16)

    def layer_body(layer, carry):
        parity_in = lax.rem(layer + 1, 2)
        parity_out = lax.rem(layer, 2)

        @pl.when(layer < layers - 3)
        def _():
            for copy in raw_loads(layer + 3):
                copy.start()

        for k in range(3):
            pre_remote(layer, k).wait_send()

        @pl.when(layer < layers - 2)
        def _():
            for copy in suf_loads(layer + 2):
                copy.start()
            split_prefix(layer + 2)

        for i, (a, b) in enumerate(blocks):
            if i == 0:
                for copy in qkv_copies(layer, 0):
                    copy.wait()
            if i + 1 < len(blocks):
                for copy in qkv_copies(layer, i + 1):
                    copy.wait()
            for j in range(a, b):
                await_part(parity_in, j)
            for j in range(a, b):
                update_x(parity_in, j)
            r = slice(a * TILE, b * TILE)
            x = x_buf[:, r]
            parts = ((slice(0, q_width), wq_buf), (slice(q_width, q_width + kv_width), wk_buf),
                     (slice(q_width + kv_width, q_width + 2 * kv_width), wv_buf))
            for cols, w_buf in parts:
                product = jnp.dot(x, w_buf[r, :], preferred_element_type=F32)
                acc_buf[:, cols] = product if i == 0 else acc_buf[:, cols] + product

            @pl.when(layer < layers - 1)
            def _():
                for copy in qkv_copies(layer + 1, i):
                    copy.start()
                if i == 0:
                    for copy in suf_loads(layer + 1):
                        copy.wait()
                    suf_send(layer + 1).start()

            if i == 0:
                @pl.when(layer < layers - 2)
                def _():
                    for k in range(3):
                        pre_remote(layer + 2, k).start()

        for h in range(2):
            for g in range(group):
                col = (h * group + g) * head_dim
                q_buf[h, pl.ds(g, both, stride=PAD), :] = acc_buf[:, col:col + head_dim].astype(BF16).astype(F32)
            for kv in range(2):
                col = q_width + kv * kv_width + h * head_dim
                fresh = acc_buf[:, col:col + head_dim].astype(BF16).astype(F32)
                kvn_buf[kv, h] = fresh
        for h in range(2):
            for kv in range(2):
                kv_mine_buf[layer, kv, h] = kvn_buf[kv, h, pl.ds(mine, rows), :]
                kv_send_buf[layer, kv, h] = kvn_buf[kv, h, pl.ds(other, rows), :]

        for k in range(3):
            pre_remote(layer, k).wait_recv()
        suf_send(layer).wait()

        per_core = rows // CHUNK

        def unpair(both_seqs):
            first_seq = both_seqs[:, None, 0:2 * PAD, 0:128]
            second_seq = both_seqs[:, None, 2 * PAD:4 * PAD, 128:256]
            return jnp.concatenate([first_seq, second_seq], axis=1).reshape(CHUNK, 2 * PAD, 128)

        def attend(i):
            away = i // per_core
            part = pl.multiple_of(lax.rem(i, per_core) * CHUNK, CHUNK)
            first = pl.multiple_of(lax.rem(core + away, 2) * rows + part, CHUNK)
            slot = (1 - away) * lax.rem(layer, 3) + away * (3 + lax.rem(layer, 2))
            chunk_rows = pl.ds(pl.multiple_of(first * PAD, CHUNK * PAD), CHUNK * PAD)
            q_heads = [q_buf[h, chunk_rows, :] for h in range(2)]
            q3 = jnp.concatenate([q.reshape(CHUNK, PAD, head_dim) for q in q_heads], axis=1)
            k_suf = suf_buf[slot, 0, pl.ds(part, CHUNK)]
            v_suf = suf_buf[slot, 1, pl.ds(part, CHUNK)]
            q_pairs = q3.astype(BF16).reshape(CHUNK // 2, 4 * PAD, head_dim)
            k_pairs = k_suf.reshape(CHUNK // 2, 256, head_dim)
            suf_scores = unpair(lax.dot_general(q_pairs, k_pairs, (((2,), (2,)), ((0,), (0,))), preferred_element_type=F32))
            suf_scores = jnp.where(key_slot < lens_buf[pl.ds(first, CHUNK)], suf_scores, -jnp.inf)
            def spread(kv):
                picked = [jnp.broadcast_to(kvn_buf[kv, h, pl.ds(first + b, 1), :], (PAD, head_dim)) for b in range(CHUNK) for h in range(2)]
                return jnp.concatenate(picked, axis=0).reshape(CHUNK, 2 * PAD, head_dim)

            k_new = spread(0)
            v_new = spread(1)
            new_scores = jnp.sum(q3 * k_new, axis=-1, keepdims=True)
            suf_weights, new_weights, masses, pre_vals = [], [], [], []
            for h in range(2):
                hs = slice(h * PAD, (h + 1) * PAD)
                q_h = q_heads[h].astype(BF16)
                k_pre = pre_buf[layer, 0, h].reshape(-1, head_dim)
                v_pre = pre_buf[layer, 1, h].reshape(-1, head_dim)
                scores = lax.dot_general(q_h, k_pre, (((1,), (1,)), ((), ())), preferred_element_type=F32)
                suf_h = suf_scores[:, hs, :].reshape(CHUNK * PAD, 128)
                new_h = new_scores[:, hs, :].reshape(CHUNK * PAD, 1)
                peak = jnp.maximum(jnp.maximum(scores.max(axis=-1, keepdims=True), suf_h.max(axis=-1, keepdims=True)), new_h)
                pre_w = jnp.exp2((scores - peak) * (scale * LOG2E))
                suf_w = jnp.exp2((suf_h - peak) * (scale * LOG2E))
                new_w = jnp.exp2((new_h - peak) * (scale * LOG2E))
                masses.append(pre_w.sum(axis=-1, keepdims=True) + suf_w.sum(axis=-1, keepdims=True) + new_w)
                pre_vals.append(jnp.dot(pre_w.astype(BF16), v_pre, preferred_element_type=F32))
                suf_weights.append(suf_w.reshape(CHUNK, PAD, 128))
                new_weights.append(new_w)
            suf_w = jnp.concatenate(suf_weights, axis=1).astype(BF16)
            v_suf = v_suf.reshape(CHUNK // 2, 2, 128, head_dim)
            v_pairs = jnp.concatenate([v_suf[:, 0], v_suf[:, 1]], axis=-1)
            suf_w = suf_w.reshape(CHUNK // 2, 4 * PAD, 128)
            suf_vals = unpair(lax.dot_general(suf_w, v_pairs, (((2,), (1,)), ((0,), (0,))), preferred_element_type=F32))
            for h in range(2):
                hs = slice(h * PAD, (h + 1) * PAD)
                mixed = pre_vals[h] + suf_vals[:, hs, :].reshape(CHUNK * PAD, head_dim)
                mixed = mixed + new_weights[h] * v_new[:, hs, :].reshape(CHUNK * PAD, head_dim)
                o_buf[h, chunk_rows, :] = mixed / masses[h]

        def attend_trip(trip, carry):
            for i in range(CHUNKS_PER_TRIP):
                attend(trip * CHUNKS_PER_TRIP + i)
            return carry

        lax.fori_loop(0, 2 * per_core // CHUNKS_PER_TRIP, attend_trip, 0)

        @pl.when(layer == layers - 1)
        def _():
            kv_store.start()
            kv_send.start()

        wo_copy(layer, 0).wait()
        wo_copy(layer, 1).wait()

        for h in range(2):
            for g in range(group):
                col = (h * group + g) * head_dim
                att_buf[:, col:col + head_dim] = o_buf[h, pl.ds(g, both, stride=PAD), :].astype(BF16)

        for i, (a, b) in enumerate(blocks):
            if 0 < i < len(blocks) - 1:
                wo_copy(layer, i + 1).wait()
            product = jnp.dot(att_buf[...], wo_buf[:, a * TILE:b * TILE], preferred_element_type=F32)
            for j in range(a, b):
                own_buf[j] = product[:, (j - a) * TILE:(j - a + 1) * TILE]

            @pl.when(layer < layers - 1)
            def _():
                wo_copy(layer + 1, i).start()

            for j in range(a, b):
                part_send(parity_out, j).start()

        return carry

    lax.fori_loop(0, layers, layer_body, 0)
    for j in range(tiles):
        await_part((layers - 1) % 2, j)
    for j in range(tiles):
        update_x((layers - 1) % 2, j)
        out_ref[:, j * TILE:(j + 1) * TILE] = x_buf[pl.ds(mine, rows), j * TILE:(j + 1) * TILE]
    kv_store.wait()
    kv_send.wait()


def cache_kernel(lens_ref, new_ref, hidden_ref, k_ref, v_ref, hidden_out_ref, k_out_ref, v_out_ref,
                 buf, new_buf, hidden_buf, in_sem, out_sem, new_sem, hidden_sem):
    layers, rows, _, heads, _ = k_ref.shape
    ahead = RING // 2

    def loads(layer):
        slot = lax.rem(layer, RING)
        return (
            pltpu.make_async_copy(new_ref.at[layer], new_buf.at[slot], new_sem.at[slot]),
            pltpu.make_async_copy(k_ref.at[layer], buf.at[slot, 0], in_sem.at[slot, 0]),
            pltpu.make_async_copy(v_ref.at[layer], buf.at[slot, 1], in_sem.at[slot, 1]),
        )

    def stores(layer):
        slot = lax.rem(layer, RING)
        return (
            pltpu.make_async_copy(buf.at[slot, 0], k_out_ref.at[layer], out_sem.at[slot, 0]),
            pltpu.make_async_copy(buf.at[slot, 1], v_out_ref.at[layer], out_sem.at[slot, 1]),
        )

    for layer in range(ahead):
        for copy in loads(layer):
            copy.start()
    hidden_load = pltpu.make_async_copy(hidden_ref, hidden_buf, hidden_sem.at[0])
    hidden_store = pltpu.make_async_copy(hidden_buf, hidden_out_ref, hidden_sem.at[1])
    hidden_load.start()

    def step(layer, carry):
        slot = lax.rem(layer, RING)

        @pl.when(layer >= ahead)
        def _():
            for copy in stores(layer - ahead):
                copy.wait()

        @pl.when(layer < layers - ahead)
        def _():
            for copy in loads(layer + ahead):
                copy.start()

        arrivals = loads(layer)
        arrivals[0].wait()
        for kv in range(2):
            arrivals[1 + kv].wait()
            for b in range(rows):
                buf[slot, kv, b, lens_ref[b]] = new_buf[slot, kv, pl.ds(b, heads, stride=rows), :].astype(BF16)
            stores(layer)[kv].start()
        return carry

    lax.fori_loop(0, layers, step, 0)
    hidden_load.wait()
    hidden_store.start()
    for layer in range(layers - ahead, layers):
        for copy in stores(layer):
            copy.wait()
    hidden_store.wait()


def solution(mesh):
    home_axes = ('data', 'ctx')
    row_spec = P(home_axes, None)
    lens_spec = P(home_axes)
    whole_spec = P()
    prefix_spec = P(None, home_axes, None, None)
    cache_spec = P(None, home_axes, None, None, None)

    def local_step(hidden, seq_lens, w_query, w_key, w_value, w_out, k_prefix, v_prefix, k_suffix, v_suffix):
        layers, model_dim = w_query.shape[:2]
        positions, kv_heads, head_dim = k_prefix.shape[1:]
        rows = hidden.shape[0]
        slots = k_suffix.shape[2]
        group = w_query.shape[2] // head_dim // kv_heads
        half_heads = kv_heads // 2
        q_width = w_query.shape[2] // 2
        kv_width = w_key.shape[2] // 2
        tiles = model_dim // TILE
        keys = slots * kv_heads
        both = 2 * rows

        k_flat = k_suffix.reshape(layers, rows, keys, head_dim)
        v_flat = v_suffix.reshape(layers, rows, keys, head_dim)
        k_pre = k_prefix.reshape(layers, positions * kv_heads, head_dim)
        v_pre = v_prefix.reshape(layers, positions * kv_heads, head_dim)

        any_spec = pl.BlockSpec(memory_space=pl.ANY)
        smem_spec = pl.BlockSpec(memory_space=pltpu.SMEM)
        vmem_spec = pl.BlockSpec(memory_space=pltpu.VMEM)
        dma = pltpu.SemaphoreType.DMA
        hidden_out, kv_new = pl.pallas_call(
            functools.partial(decode_kernel, (layers, rows, group, head_dim, slots)),
            out_shape=(jax.ShapeDtypeStruct((rows, model_dim), BF16),
                       jax.ShapeDtypeStruct((layers, 2, kv_heads, rows, head_dim), F32)),
            in_specs=[vmem_spec, vmem_spec] + [any_spec] * 8,
            out_specs=(vmem_spec, any_spec),
            scratch_shapes=[
                pltpu.VMEM((model_dim, q_width), BF16),
                pltpu.VMEM((model_dim, kv_width), BF16),
                pltpu.VMEM((model_dim, kv_width), BF16),
                pltpu.VMEM((q_width, model_dim), BF16),
                pltpu.VMEM((layers, 2, half_heads, 4, positions, head_dim), BF16),
                pltpu.VMEM((2, 2, positions * kv_heads, head_dim), BF16),
                pltpu.VMEM((2, positions * kv_heads, head_dim), F32),
                pltpu.VMEM((2, 2, 2, half_heads, positions, head_dim), BF16),
                pltpu.VMEM((5, 2, rows, keys, head_dim), BF16),
                pltpu.VMEM((both, model_dim), BF16),
                pltpu.VMEM((tiles, both, TILE), F32),
                pltpu.VMEM((2, tiles, both, TILE), F32),
                pltpu.VMEM((both, q_width + 2 * kv_width), F32),
                pltpu.VMEM((half_heads, both * PAD, head_dim), F32),
                pltpu.VMEM((2, half_heads, both, head_dim), F32),
                pltpu.VMEM((half_heads, both * PAD, head_dim), F32),
                pltpu.VMEM((both, q_width), BF16),
                pltpu.VMEM((both, 2 * PAD, 128), jnp.int32),
                pltpu.VMEM((layers, 2, half_heads, rows, head_dim), F32),
                pltpu.VMEM((layers, 2, half_heads, rows, head_dim), F32),
                dma((4, tiles // BLOCK)), dma((3, 2)), dma((2,)), dma((2,)), dma((2, 2)), dma((layers, 3)), dma((layers, 3)),
                dma((tiles,)), dma((2, tiles)), dma((2,)), dma((3,)),
            ],
            compiler_params=pltpu.CompilerParams(collective_id=0, has_side_effects=True, vmem_limit_bytes=66_000_000),
            name="decode_layers",
        )(seq_lens.reshape(1, rows), hidden, w_query, w_key, w_value, w_out, k_pre, v_pre, k_flat, v_flat)

        hidden_out, k_out, v_out = pl.pallas_call(
            cache_kernel,
            out_shape=(jax.ShapeDtypeStruct(hidden.shape, BF16), jax.ShapeDtypeStruct(k_suffix.shape, BF16), jax.ShapeDtypeStruct(v_suffix.shape, BF16)),
            in_specs=[smem_spec] + [any_spec] * 4,
            out_specs=(any_spec, any_spec, any_spec),
            scratch_shapes=[
                pltpu.VMEM((RING, 2) + k_suffix.shape[1:], BF16),
                pltpu.VMEM((RING, 2, kv_heads * rows, head_dim), F32),
                pltpu.VMEM(hidden.shape, BF16),
                dma((RING, 2)), dma((RING, 2)), dma((RING,)), dma((2,)),
            ],
            compiler_params=pltpu.CompilerParams(vmem_limit_bytes=60_000_000),
            name="write_caches",
        )(seq_lens, kv_new.reshape(layers, 2, kv_heads * rows, head_dim), hidden_out, k_suffix, v_suffix)
        return hidden_out, k_out, v_out

    return jax.shard_map(local_step, mesh=mesh, in_specs=(row_spec, lens_spec, whole_spec, whole_spec, whole_spec, whole_spec, prefix_spec, prefix_spec, cache_spec, cache_spec), out_specs=(row_spec, cache_spec, cache_spec), check_vma=False)
```

```python
import functools

import jax
import jax.numpy as jnp
from jax import lax
from jax.experimental import pallas as pl
from jax.experimental.pallas import tpu as pltpu
from jax.sharding import PartitionSpec as P

MESH = pl.DeviceIdType.MESH
BF16 = jnp.bfloat16
F32 = jnp.float32
TILE = 512
CHUNK = 32
PAD = 8
RING = 8
BLOCK = 2
LOG2E = 1.4426950408889634
CHUNKS_PER_TRIP = 1


def decode_kernel(dims, lens_ref, hidden_ref, wq_ref, wk_ref, wv_ref, wo_ref, kpre_ref, vpre_ref, ksuf_ref, vsuf_ref,
                  out_ref, kv_out_ref,
                  wq_buf, wk_buf, wv_buf, wo_first_buf, wo_buf, pre_buf, raw_buf, wide_buf, split_buf, suf_buf, x_buf, own_buf, recv_buf, acc_buf,
                  q_buf, kvn_buf, o_buf, att_buf, lens_buf, kv_mine_buf, kv_send_buf,
                  w_sem, wo_first_sem, suf_load_sem, suf_send_sem, suf_recv_sem, raw_sem, pre_send_sem, pre_recv_sem,
                  part_send_sem, part_recv_sem, lens_sem, kv_sem):
    layers, rows, group, head_dim, slots = dims
    half_heads = 2
    tiles = own_buf.shape[0]
    q_width = wq_buf.shape[1]
    kv_width = wk_buf.shape[1]
    blocks = [(i * BLOCK, (i + 1) * BLOCK if i < tiles // BLOCK - 1 else tiles) for i in range(tiles // BLOCK)]
    both = 2 * rows
    me = lax.axis_index("ctx")
    core = lax.rem(me, 2)
    chip = me // 2
    mate = chip * 2 + (1 - core)
    across = (1 - chip) * 2 + core
    diagonal = (1 - chip) * 2 + (1 - core)
    peers = ((mate, 1 - core), (across, core), (diagonal, 1 - core))
    mine = pl.multiple_of(core * rows, rows)
    other = pl.multiple_of((1 - core) * rows, rows)
    q_col = pl.multiple_of(core * q_width, 128)
    kv_col = pl.multiple_of(core * kv_width, 128)
    scale = head_dim ** -0.5

    def qkv_copies(layer, i):
        a, b = blocks[i]
        r = pl.ds(a * TILE, (b - a) * TILE)
        return (
            pltpu.make_async_copy(wq_ref.at[layer, r, pl.ds(q_col, q_width)], wq_buf.at[r], w_sem.at[0, i]),
            pltpu.make_async_copy(wk_ref.at[layer, r, pl.ds(kv_col, kv_width)], wk_buf.at[r], w_sem.at[1, i]),
            pltpu.make_async_copy(wv_ref.at[layer, r, pl.ds(kv_col, kv_width)], wv_buf.at[r], w_sem.at[2, i]),
        )

    def wo_copy(layer, i):
        a, b = blocks[i]
        src = wo_ref.at[layer, pl.ds(q_col, q_width), pl.ds(a * TILE, (b - a) * TILE)]
        if i == 0:
            return pltpu.make_async_copy(src, wo_first_buf.at[lax.rem(layer, 2)], wo_first_sem.at[lax.rem(layer, 2)])
        return pltpu.make_async_copy(src, wo_buf.at[:, pl.ds((a - BLOCK) * TILE, (b - a) * TILE)], w_sem.at[3, i])

    def suf_loads(layer):
        slot = lax.rem(layer, 3)
        return (
            pltpu.make_async_copy(ksuf_ref.at[layer], suf_buf.at[slot, 0], suf_load_sem.at[slot, 0]),
            pltpu.make_async_copy(vsuf_ref.at[layer], suf_buf.at[slot, 1], suf_load_sem.at[slot, 1]),
        )

    def suf_send(layer):
        return pltpu.make_async_remote_copy(
            src_ref=suf_buf.at[lax.rem(layer, 3)], dst_ref=suf_buf.at[3 + lax.rem(layer, 2)],
            send_sem=suf_send_sem.at[lax.rem(layer, 2)], recv_sem=suf_recv_sem.at[lax.rem(layer, 2)],
            device_id={"ctx": mate}, device_id_type=MESH)

    def raw_loads(layer):
        slot = lax.rem(layer, 2)
        return (
            pltpu.make_async_copy(kpre_ref.at[layer], raw_buf.at[slot, 0], raw_sem.at[slot, 0]),
            pltpu.make_async_copy(vpre_ref.at[layer], raw_buf.at[slot, 1], raw_sem.at[slot, 1]),
        )

    def split_prefix(layer):
        slot = lax.rem(layer, 2)
        heads = 2 * half_heads
        positions = pre_buf.shape[4]
        for copy in raw_loads(layer):
            copy.wait()
        for kv in range(2):
            wide_buf[kv] = raw_buf[slot, kv].astype(F32)
            for h in range(half_heads):
                for half in range(2):
                    split_buf[slot, half, kv, h] = wide_buf[kv, pl.ds(half * half_heads + h, positions, stride=heads), :].astype(BF16)
                pre_buf[layer, kv, h, me] = split_buf[slot, core, kv, h]

    def pre_remote(layer, k):
        device, half = peers[k]
        return pltpu.make_async_remote_copy(
            src_ref=split_buf.at[lax.rem(layer, 2), half], dst_ref=pre_buf.at[layer, :, :, me],
            send_sem=pre_send_sem.at[layer, k], recv_sem=pre_recv_sem.at[layer, k],
            device_id={"ctx": device}, device_id_type=MESH)

    def part_send(parity, j):
        return pltpu.make_async_remote_copy(
            src_ref=own_buf.at[j], dst_ref=recv_buf.at[parity, j],
            send_sem=part_send_sem.at[j], recv_sem=part_recv_sem.at[parity, j],
            device_id={"ctx": mate}, device_id_type=MESH)

    lens_send = pltpu.make_async_remote_copy(
        src_ref=lens_buf.at[pl.ds(mine, rows)], dst_ref=lens_buf.at[pl.ds(mine, rows)], send_sem=lens_sem.at[0], recv_sem=lens_sem.at[1],
        device_id={"ctx": mate}, device_id_type=MESH)
    kv_slice = kv_out_ref.at[:, :, pl.ds(core * half_heads, half_heads)]
    kv_store = pltpu.make_async_copy(kv_mine_buf, kv_slice, kv_sem.at[2])
    kv_send = pltpu.make_async_remote_copy(
        src_ref=kv_send_buf, dst_ref=kv_slice, send_sem=kv_sem.at[0], recv_sem=kv_sem.at[1],
        device_id={"ctx": mate}, device_id_type=MESH)

    for layer in range(2):
        for copy in raw_loads(layer):
            copy.start()
    for i in range(len(blocks)):
        for copy in qkv_copies(0, i):
            copy.start()
        if i == 0:
            for copy in suf_loads(0):
                copy.start()
    for i in range(len(blocks)):
        wo_copy(0, i).start()
    for copy in suf_loads(1):
        copy.start()

    x_buf[...] = jnp.zeros_like(x_buf)
    for j in range(tiles):
        own_buf[j] = jnp.zeros_like(own_buf[j])
        own_buf[j, pl.ds(mine, rows), :] = hidden_ref[:, j * TILE:(j + 1) * TILE].astype(F32)
    diagonal_hit = lax.broadcasted_iota(jnp.int32, (rows, rows), 0) == lax.broadcasted_iota(jnp.int32, (rows, rows), 1)
    lens_wide = jnp.broadcast_to(lens_ref[...].astype(F32), (rows, rows))
    lens_wide = jnp.where(diagonal_hit, lens_wide, 0.0).sum(axis=1, keepdims=True)
    lens_wide = jnp.broadcast_to(lens_wide, (rows, 128)).astype(jnp.int32)
    for b in range(rows):
        lens_buf[mine + b] = jnp.broadcast_to(lens_wide[b:b + 1, :], (2 * PAD, 128))
    q_buf[...] = jnp.zeros_like(q_buf)
    split_prefix(0)
    for copy in raw_loads(2):
        copy.start()
    split_prefix(1)

    barrier = pltpu.get_barrier_semaphore()
    for device, _ in peers:
        pl.semaphore_signal(barrier, inc=1, device_id={"ctx": device}, device_id_type=MESH)
    pl.semaphore_wait(barrier, 3)

    for j in range(tiles):
        part_send(1, j).start()
    lens_send.start()
    for layer in range(2):
        for k in range(3):
            pre_remote(layer, k).start()
    for copy in suf_loads(0):
        copy.wait()
    suf_send(0).start()
    lens_send.wait()

    row_ids = lax.broadcasted_iota(jnp.int32, (2 * PAD, 128), 0)
    key_ids = lax.broadcasted_iota(jnp.int32, (2 * PAD, 128), 1)
    key_slot = jnp.where(lax.rem(key_ids, 4) == 2 * core + row_ids // PAD, key_ids // 4, slots)[None]

    def await_part(parity, j):
        copy = part_send(parity, j)
        copy.wait_recv()
        copy.wait_send()

    def update_x(parity, j):
        update = (own_buf[j] + recv_buf[parity, j]).astype(BF16)
        cols = slice(j * TILE, (j + 1) * TILE)
        x_buf[:, cols] = (x_buf[:, cols].astype(F32) + update.astype(F32)).astype(BF16)

    def layer_body(layer, carry):
        parity_in = lax.rem(layer + 1, 2)
        parity_out = lax.rem(layer, 2)

        @pl.when(layer < layers - 3)
        def _():
            for copy in raw_loads(layer + 3):
                copy.start()

        for k in range(3):
            pre_remote(layer, k).wait_send()

        @pl.when(layer < layers - 2)
        def _():
            for copy in suf_loads(layer + 2):
                copy.start()
            split_prefix(layer + 2)

        for i, (a, b) in enumerate(blocks):
            if i == 0:
                for copy in qkv_copies(layer, 0):
                    copy.wait()
            if i + 1 < len(blocks):
                for copy in qkv_copies(layer, i + 1):
                    copy.wait()
            for j in range(a, b):
                await_part(parity_in, j)
            for j in range(a, b):
                update_x(parity_in, j)
            r = slice(a * TILE, b * TILE)
            x = x_buf[:, r]
            parts = ((slice(0, q_width), wq_buf), (slice(q_width, q_width + kv_width), wk_buf),
                     (slice(q_width + kv_width, q_width + 2 * kv_width), wv_buf))
            for cols, w_buf in parts:
                product = jnp.dot(x, w_buf[r, :], preferred_element_type=F32)
                acc_buf[:, cols] = product if i == 0 else acc_buf[:, cols] + product

            @pl.when(layer < layers - 1)
            def _():
                for copy in qkv_copies(layer + 1, i):
                    copy.start()
                if i == 0:
                    for copy in suf_loads(layer + 1):
                        copy.wait()
                    suf_send(layer + 1).start()

            if i == 0:
                @pl.when(layer < layers - 2)
                def _():
                    for k in range(3):
                        pre_remote(layer + 2, k).start()

        @pl.when(layer < layers - 1)
        def _():
            wo_copy(layer + 1, 0).start()

        for h in range(2):
            for g in range(group):
                col = (h * group + g) * head_dim
                q_buf[h, pl.ds(g, both, stride=PAD), :] = acc_buf[:, col:col + head_dim].astype(BF16).astype(F32)
            for kv in range(2):
                col = q_width + kv * kv_width + h * head_dim
                fresh = acc_buf[:, col:col + head_dim].astype(BF16).astype(F32)
                kvn_buf[kv, h] = fresh
        for h in range(2):
            for kv in range(2):
                kv_mine_buf[layer, kv, h] = kvn_buf[kv, h, pl.ds(mine, rows), :]
                kv_send_buf[layer, kv, h] = kvn_buf[kv, h, pl.ds(other, rows), :]

        for k in range(3):
            pre_remote(layer, k).wait_recv()
        suf_send(layer).wait()

        per_core = rows // CHUNK

        def unpair(both_seqs):
            first_seq = both_seqs[:, None, 0:2 * PAD, 0:128]
            second_seq = both_seqs[:, None, 2 * PAD:4 * PAD, 128:256]
            return jnp.concatenate([first_seq, second_seq], axis=1).reshape(CHUNK, 2 * PAD, 128)

        def attend(i):
            away = i // per_core
            part = pl.multiple_of(lax.rem(i, per_core) * CHUNK, CHUNK)
            first = pl.multiple_of(lax.rem(core + away, 2) * rows + part, CHUNK)
            slot = (1 - away) * lax.rem(layer, 3) + away * (3 + lax.rem(layer, 2))
            chunk_rows = pl.ds(pl.multiple_of(first * PAD, CHUNK * PAD), CHUNK * PAD)
            q_heads = [q_buf[h, chunk_rows, :] for h in range(2)]
            q3 = jnp.concatenate([q.reshape(CHUNK, PAD, head_dim) for q in q_heads], axis=1)
            k_suf = suf_buf[slot, 0, pl.ds(part, CHUNK)]
            v_suf = suf_buf[slot, 1, pl.ds(part, CHUNK)]
            q_pairs = q3.astype(BF16).reshape(CHUNK // 2, 4 * PAD, head_dim)
            k_pairs = k_suf.reshape(CHUNK // 2, 256, head_dim)
            suf_scores = unpair(lax.dot_general(q_pairs, k_pairs, (((2,), (2,)), ((0,), (0,))), preferred_element_type=F32))
            suf_scores = jnp.where(key_slot < lens_buf[pl.ds(first, CHUNK)], suf_scores, -jnp.inf)
            def spread(kv):
                picked = [jnp.broadcast_to(kvn_buf[kv, h, pl.ds(first + b, 1), :], (PAD, head_dim)) for b in range(CHUNK) for h in range(2)]
                return jnp.concatenate(picked, axis=0).reshape(CHUNK, 2 * PAD, head_dim)

            k_new = spread(0)
            v_new = spread(1)
            new_scores = jnp.sum(q3 * k_new, axis=-1, keepdims=True)
            suf_weights, new_weights, masses, pre_vals = [], [], [], []
            for h in range(2):
                hs = slice(h * PAD, (h + 1) * PAD)
                q_h = q_heads[h].astype(BF16)
                k_pre = pre_buf[layer, 0, h].reshape(-1, head_dim)
                v_pre = pre_buf[layer, 1, h].reshape(-1, head_dim)
                scores = lax.dot_general(q_h, k_pre, (((1,), (1,)), ((), ())), preferred_element_type=F32)
                suf_h = suf_scores[:, hs, :].reshape(CHUNK * PAD, 128)
                new_h = new_scores[:, hs, :].reshape(CHUNK * PAD, 1)
                peak = jnp.maximum(jnp.maximum(scores.max(axis=-1, keepdims=True), suf_h.max(axis=-1, keepdims=True)), new_h)
                pre_w = jnp.exp2((scores - peak) * (scale * LOG2E))
                suf_w = jnp.exp2((suf_h - peak) * (scale * LOG2E))
                new_w = jnp.exp2((new_h - peak) * (scale * LOG2E))
                masses.append(pre_w.sum(axis=-1, keepdims=True) + suf_w.sum(axis=-1, keepdims=True) + new_w)
                pre_vals.append(jnp.dot(pre_w.astype(BF16), v_pre, preferred_element_type=F32))
                suf_weights.append(suf_w.reshape(CHUNK, PAD, 128))
                new_weights.append(new_w)
            suf_w = jnp.concatenate(suf_weights, axis=1).astype(BF16)
            v_suf = v_suf.reshape(CHUNK // 2, 2, 128, head_dim)
            v_pairs = jnp.concatenate([v_suf[:, 0], v_suf[:, 1]], axis=-1)
            suf_w = suf_w.reshape(CHUNK // 2, 4 * PAD, 128)
            suf_vals = unpair(lax.dot_general(suf_w, v_pairs, (((2,), (1,)), ((0,), (0,))), preferred_element_type=F32))
            for h in range(2):
                hs = slice(h * PAD, (h + 1) * PAD)
                mixed = pre_vals[h] + suf_vals[:, hs, :].reshape(CHUNK * PAD, head_dim)
                mixed = mixed + new_weights[h] * v_new[:, hs, :].reshape(CHUNK * PAD, head_dim)
                o_buf[h, chunk_rows, :] = mixed / masses[h]

        def attend_trip(trip, carry):
            for i in range(CHUNKS_PER_TRIP):
                attend(trip * CHUNKS_PER_TRIP + i)
            return carry

        lax.fori_loop(0, 2 * per_core // CHUNKS_PER_TRIP, attend_trip, 0)

        @pl.when(layer == layers - 1)
        def _():
            kv_store.start()
            kv_send.start()

        wo_copy(layer, 0).wait()
        wo_copy(layer, 1).wait()

        for h in range(2):
            for g in range(group):
                col = (h * group + g) * head_dim
                att_buf[:, col:col + head_dim] = o_buf[h, pl.ds(g, both, stride=PAD), :].astype(BF16)

        for i, (a, b) in enumerate(blocks):
            if 0 < i < len(blocks) - 1:
                wo_copy(layer, i + 1).wait()
            weights = wo_first_buf[lax.rem(layer, 2)] if i == 0 else wo_buf[:, (a - BLOCK) * TILE:(b - BLOCK) * TILE]
            product = jnp.dot(att_buf[...], weights, preferred_element_type=F32)
            for j in range(a, b):
                own_buf[j] = product[:, (j - a) * TILE:(j - a + 1) * TILE]

            if i > 0:
                @pl.when(layer < layers - 1)
                def _():
                    wo_copy(layer + 1, i).start()

            for j in range(a, b):
                part_send(parity_out, j).start()

        return carry

    lax.fori_loop(0, layers, layer_body, 0)
    for j in range(tiles):
        await_part((layers - 1) % 2, j)
    for j in range(tiles):
        update_x((layers - 1) % 2, j)
        out_ref[:, j * TILE:(j + 1) * TILE] = x_buf[pl.ds(mine, rows), j * TILE:(j + 1) * TILE]
    kv_store.wait()
    kv_send.wait()


def cache_kernel(lens_ref, new_ref, hidden_ref, k_ref, v_ref, hidden_out_ref, k_out_ref, v_out_ref,
                 buf, new_buf, hidden_buf, in_sem, out_sem, new_sem, hidden_sem):
    layers, rows, _, heads, _ = k_ref.shape
    ahead = RING // 2

    def loads(layer):
        slot = lax.rem(layer, RING)
        return (
            pltpu.make_async_copy(new_ref.at[layer], new_buf.at[slot], new_sem.at[slot]),
            pltpu.make_async_copy(k_ref.at[layer], buf.at[slot, 0], in_sem.at[slot, 0]),
            pltpu.make_async_copy(v_ref.at[layer], buf.at[slot, 1], in_sem.at[slot, 1]),
        )

    def stores(layer):
        slot = lax.rem(layer, RING)
        return (
            pltpu.make_async_copy(buf.at[slot, 0], k_out_ref.at[layer], out_sem.at[slot, 0]),
            pltpu.make_async_copy(buf.at[slot, 1], v_out_ref.at[layer], out_sem.at[slot, 1]),
        )

    for layer in range(ahead):
        for copy in loads(layer):
            copy.start()
    hidden_load = pltpu.make_async_copy(hidden_ref, hidden_buf, hidden_sem.at[0])
    hidden_store = pltpu.make_async_copy(hidden_buf, hidden_out_ref, hidden_sem.at[1])
    hidden_load.start()

    def step(layer, carry):
        slot = lax.rem(layer, RING)

        @pl.when(layer >= ahead)
        def _():
            for copy in stores(layer - ahead):
                copy.wait()

        @pl.when(layer < layers - ahead)
        def _():
            for copy in loads(layer + ahead):
                copy.start()

        arrivals = loads(layer)
        arrivals[0].wait()
        for kv in range(2):
            arrivals[1 + kv].wait()
            for b in range(rows):
                buf[slot, kv, b, lens_ref[b]] = new_buf[slot, kv, pl.ds(b, heads, stride=rows), :].astype(BF16)
            stores(layer)[kv].start()
        return carry

    lax.fori_loop(0, layers, step, 0)
    hidden_load.wait()
    hidden_store.start()
    for layer in range(layers - ahead, layers):
        for copy in stores(layer):
            copy.wait()
    hidden_store.wait()


def solution(mesh):
    home_axes = ('data', 'ctx')
    row_spec = P(home_axes, None)
    lens_spec = P(home_axes)
    whole_spec = P()
    prefix_spec = P(None, home_axes, None, None)
    cache_spec = P(None, home_axes, None, None, None)

    def local_step(hidden, seq_lens, w_query, w_key, w_value, w_out, k_prefix, v_prefix, k_suffix, v_suffix):
        layers, model_dim = w_query.shape[:2]
        positions, kv_heads, head_dim = k_prefix.shape[1:]
        rows = hidden.shape[0]
        slots = k_suffix.shape[2]
        group = w_query.shape[2] // head_dim // kv_heads
        half_heads = kv_heads // 2
        q_width = w_query.shape[2] // 2
        kv_width = w_key.shape[2] // 2
        tiles = model_dim // TILE
        keys = slots * kv_heads
        both = 2 * rows

        k_flat = k_suffix.reshape(layers, rows, keys, head_dim)
        v_flat = v_suffix.reshape(layers, rows, keys, head_dim)
        k_pre = k_prefix.reshape(layers, positions * kv_heads, head_dim)
        v_pre = v_prefix.reshape(layers, positions * kv_heads, head_dim)

        any_spec = pl.BlockSpec(memory_space=pl.ANY)
        smem_spec = pl.BlockSpec(memory_space=pltpu.SMEM)
        vmem_spec = pl.BlockSpec(memory_space=pltpu.VMEM)
        dma = pltpu.SemaphoreType.DMA
        hidden_out, kv_new = pl.pallas_call(
            functools.partial(decode_kernel, (layers, rows, group, head_dim, slots)),
            out_shape=(jax.ShapeDtypeStruct((rows, model_dim), BF16),
                       jax.ShapeDtypeStruct((layers, 2, kv_heads, rows, head_dim), F32)),
            in_specs=[vmem_spec, vmem_spec] + [any_spec] * 8,
            out_specs=(vmem_spec, any_spec),
            scratch_shapes=[
                pltpu.VMEM((model_dim, q_width), BF16),
                pltpu.VMEM((model_dim, kv_width), BF16),
                pltpu.VMEM((model_dim, kv_width), BF16),
                pltpu.VMEM((2, q_width, BLOCK * TILE), BF16),
                pltpu.VMEM((q_width, model_dim - BLOCK * TILE), BF16),
                pltpu.VMEM((layers, 2, half_heads, 4, positions, head_dim), BF16),
                pltpu.VMEM((2, 2, positions * kv_heads, head_dim), BF16),
                pltpu.VMEM((2, positions * kv_heads, head_dim), F32),
                pltpu.VMEM((2, 2, 2, half_heads, positions, head_dim), BF16),
                pltpu.VMEM((5, 2, rows, keys, head_dim), BF16),
                pltpu.VMEM((both, model_dim), BF16),
                pltpu.VMEM((tiles, both, TILE), F32),
                pltpu.VMEM((2, tiles, both, TILE), F32),
                pltpu.VMEM((both, q_width + 2 * kv_width), F32),
                pltpu.VMEM((half_heads, both * PAD, head_dim), F32),
                pltpu.VMEM((2, half_heads, both, head_dim), F32),
                pltpu.VMEM((half_heads, both * PAD, head_dim), F32),
                pltpu.VMEM((both, q_width), BF16),
                pltpu.VMEM((both, 2 * PAD, 128), jnp.int32),
                pltpu.VMEM((layers, 2, half_heads, rows, head_dim), F32),
                pltpu.VMEM((layers, 2, half_heads, rows, head_dim), F32),
                dma((4, tiles // BLOCK)), dma((2,)), dma((3, 2)), dma((2,)), dma((2,)), dma((2, 2)), dma((layers, 3)), dma((layers, 3)),
                dma((tiles,)), dma((2, tiles)), dma((2,)), dma((3,)),
            ],
            compiler_params=pltpu.CompilerParams(collective_id=0, has_side_effects=True, vmem_limit_bytes=66_000_000),
            name="decode_layers",
        )(seq_lens.reshape(1, rows), hidden, w_query, w_key, w_value, w_out, k_pre, v_pre, k_flat, v_flat)

        hidden_out, k_out, v_out = pl.pallas_call(
            cache_kernel,
            out_shape=(jax.ShapeDtypeStruct(hidden.shape, BF16), jax.ShapeDtypeStruct(k_suffix.shape, BF16), jax.ShapeDtypeStruct(v_suffix.shape, BF16)),
            in_specs=[smem_spec] + [any_spec] * 4,
            out_specs=(any_spec, any_spec, any_spec),
            scratch_shapes=[
                pltpu.VMEM((RING, 2) + k_suffix.shape[1:], BF16),
                pltpu.VMEM((RING, 2, kv_heads * rows, head_dim), F32),
                pltpu.VMEM(hidden.shape, BF16),
                dma((RING, 2)), dma((RING, 2)), dma((RING,)), dma((2,)),
            ],
            compiler_params=pltpu.CompilerParams(vmem_limit_bytes=60_000_000),
            name="write_caches",
        )(seq_lens, kv_new.reshape(layers, 2, kv_heads * rows, head_dim), hidden_out, k_suffix, v_suffix)
        return hidden_out, k_out, v_out

    return jax.shard_map(local_step, mesh=mesh, in_specs=(row_spec, lens_spec, whole_spec, whole_spec, whole_spec, whole_spec, prefix_spec, prefix_spec, cache_spec, cache_spec), out_specs=(row_spec, cache_spec, cache_spec), check_vma=False)
```

```python
import functools

import jax
import jax.numpy as jnp
from jax import lax
from jax.experimental import pallas as pl
from jax.experimental.pallas import tpu as pltpu
from jax.sharding import PartitionSpec as P

MESH = pl.DeviceIdType.MESH
BF16 = jnp.bfloat16
F32 = jnp.float32
TILE = 512
CHUNK = 32
PAD = 8
WRITE_LAG = 15
BLOCK = 2
LOG2E = 1.4426950408889634
CHUNKS_PER_TRIP = 1


def decode_kernel(dims, lens_ref, hidden_ref, wq_ref, wk_ref, wv_ref, wo_ref, kpre_ref, vpre_ref, ksuf_ref, vsuf_ref,
                  out_ref, kv_out_ref,
                  wq_buf, wk_buf, wv_buf, wo_first_buf, wo_buf, pre_buf, raw_buf, wide_buf, split_buf, suf_buf, x_buf, own_buf, recv_buf, acc_buf,
                  q_buf, kvn_buf, o_buf, att_buf, lens_buf, kv_mine_buf, kv_send_buf,
                  w_sem, wo_first_sem, suf_load_sem, suf_send_sem, suf_recv_sem, raw_sem, pre_send_sem, pre_recv_sem,
                  part_send_sem, part_recv_sem, lens_sem, kv_sem):
    layers, rows, group, head_dim, slots = dims
    half_heads = 2
    tiles = own_buf.shape[0]
    q_width = wq_buf.shape[1]
    kv_width = wk_buf.shape[1]
    blocks = [(i * BLOCK, (i + 1) * BLOCK if i < tiles // BLOCK - 1 else tiles) for i in range(tiles // BLOCK)]
    both = 2 * rows
    me = lax.axis_index("ctx")
    core = lax.rem(me, 2)
    chip = me // 2
    mate = chip * 2 + (1 - core)
    across = (1 - chip) * 2 + core
    diagonal = (1 - chip) * 2 + (1 - core)
    peers = ((mate, 1 - core), (across, core), (diagonal, 1 - core))
    mine = pl.multiple_of(core * rows, rows)
    other = pl.multiple_of((1 - core) * rows, rows)
    q_col = pl.multiple_of(core * q_width, 128)
    kv_col = pl.multiple_of(core * kv_width, 128)
    scale = head_dim ** -0.5

    def qkv_copies(layer, i):
        a, b = blocks[i]
        r = pl.ds(a * TILE, (b - a) * TILE)
        return (
            pltpu.make_async_copy(wq_ref.at[layer, r, pl.ds(q_col, q_width)], wq_buf.at[r], w_sem.at[0, i]),
            pltpu.make_async_copy(wk_ref.at[layer, r, pl.ds(kv_col, kv_width)], wk_buf.at[r], w_sem.at[1, i]),
            pltpu.make_async_copy(wv_ref.at[layer, r, pl.ds(kv_col, kv_width)], wv_buf.at[r], w_sem.at[2, i]),
        )

    def wo_copy(layer, i):
        a, b = blocks[i]
        src = wo_ref.at[layer, pl.ds(q_col, q_width), pl.ds(a * TILE, (b - a) * TILE)]
        if i == 0:
            return pltpu.make_async_copy(src, wo_first_buf.at[lax.rem(layer, 2)], wo_first_sem.at[lax.rem(layer, 2)])
        return pltpu.make_async_copy(src, wo_buf.at[:, pl.ds((a - BLOCK) * TILE, (b - a) * TILE)], w_sem.at[3, i])

    def suf_loads(layer):
        slot = lax.rem(layer, 3)
        return (
            pltpu.make_async_copy(ksuf_ref.at[layer], suf_buf.at[slot, 0], suf_load_sem.at[slot, 0]),
            pltpu.make_async_copy(vsuf_ref.at[layer], suf_buf.at[slot, 1], suf_load_sem.at[slot, 1]),
        )

    def suf_send(layer):
        return pltpu.make_async_remote_copy(
            src_ref=suf_buf.at[lax.rem(layer, 3)], dst_ref=suf_buf.at[3 + lax.rem(layer, 2)],
            send_sem=suf_send_sem.at[lax.rem(layer, 2)], recv_sem=suf_recv_sem.at[lax.rem(layer, 2)],
            device_id={"ctx": mate}, device_id_type=MESH)

    def raw_loads(layer):
        slot = lax.rem(layer, 2)
        return (
            pltpu.make_async_copy(kpre_ref.at[layer], raw_buf.at[slot, 0], raw_sem.at[slot, 0]),
            pltpu.make_async_copy(vpre_ref.at[layer], raw_buf.at[slot, 1], raw_sem.at[slot, 1]),
        )

    def split_prefix(layer):
        slot = lax.rem(layer, 2)
        heads = 2 * half_heads
        positions = pre_buf.shape[4]
        for copy in raw_loads(layer):
            copy.wait()
        for kv in range(2):
            wide_buf[kv] = raw_buf[slot, kv].astype(F32)
            for h in range(half_heads):
                for half in range(2):
                    split_buf[slot, half, kv, h] = wide_buf[kv, pl.ds(half * half_heads + h, positions, stride=heads), :].astype(BF16)
                pre_buf[layer, kv, h, me] = split_buf[slot, core, kv, h]

    def pre_remote(layer, k):
        device, half = peers[k]
        return pltpu.make_async_remote_copy(
            src_ref=split_buf.at[lax.rem(layer, 2), half], dst_ref=pre_buf.at[layer, :, :, me],
            send_sem=pre_send_sem.at[layer, k], recv_sem=pre_recv_sem.at[layer, k],
            device_id={"ctx": device}, device_id_type=MESH)

    def part_send(parity, j):
        return pltpu.make_async_remote_copy(
            src_ref=own_buf.at[j], dst_ref=recv_buf.at[parity, j],
            send_sem=part_send_sem.at[j], recv_sem=part_recv_sem.at[parity, j],
            device_id={"ctx": mate}, device_id_type=MESH)

    lens_send = pltpu.make_async_remote_copy(
        src_ref=lens_buf.at[pl.ds(mine, rows)], dst_ref=lens_buf.at[pl.ds(mine, rows)], send_sem=lens_sem.at[0], recv_sem=lens_sem.at[1],
        device_id={"ctx": mate}, device_id_type=MESH)
    kv_slice = kv_out_ref.at[:, :, pl.ds(core * half_heads, half_heads)]
    kv_store = pltpu.make_async_copy(kv_mine_buf, kv_slice, kv_sem.at[2])
    kv_send = pltpu.make_async_remote_copy(
        src_ref=kv_send_buf, dst_ref=kv_slice, send_sem=kv_sem.at[0], recv_sem=kv_sem.at[1],
        device_id={"ctx": mate}, device_id_type=MESH)

    for layer in range(2):
        for copy in raw_loads(layer):
            copy.start()
    for i in range(len(blocks)):
        for copy in qkv_copies(0, i):
            copy.start()
        if i == 0:
            for copy in suf_loads(0):
                copy.start()
    for i in range(len(blocks)):
        wo_copy(0, i).start()
    for copy in suf_loads(1):
        copy.start()

    x_buf[...] = jnp.zeros_like(x_buf)
    for j in range(tiles):
        own_buf[j] = jnp.zeros_like(own_buf[j])
        own_buf[j, pl.ds(mine, rows), :] = hidden_ref[:, j * TILE:(j + 1) * TILE].astype(F32)
    diagonal_hit = lax.broadcasted_iota(jnp.int32, (rows, rows), 0) == lax.broadcasted_iota(jnp.int32, (rows, rows), 1)
    lens_wide = jnp.broadcast_to(lens_ref[...].astype(F32), (rows, rows))
    lens_wide = jnp.where(diagonal_hit, lens_wide, 0.0).sum(axis=1, keepdims=True)
    lens_wide = jnp.broadcast_to(lens_wide, (rows, 128)).astype(jnp.int32)
    for b in range(rows):
        lens_buf[mine + b] = jnp.broadcast_to(lens_wide[b:b + 1, :], (2 * PAD, 128))
    q_buf[...] = jnp.zeros_like(q_buf)
    split_prefix(0)
    for copy in raw_loads(2):
        copy.start()
    split_prefix(1)

    barrier = pltpu.get_barrier_semaphore()
    for device, _ in peers:
        pl.semaphore_signal(barrier, inc=1, device_id={"ctx": device}, device_id_type=MESH)
    pl.semaphore_wait(barrier, 3)

    for j in range(tiles):
        part_send(1, j).start()
    lens_send.start()
    for layer in range(2):
        for k in range(3):
            pre_remote(layer, k).start()
    for copy in suf_loads(0):
        copy.wait()
    suf_send(0).start()
    lens_send.wait()

    row_ids = lax.broadcasted_iota(jnp.int32, (2 * PAD, 128), 0)
    key_ids = lax.broadcasted_iota(jnp.int32, (2 * PAD, 128), 1)
    key_slot = jnp.where(lax.rem(key_ids, 4) == 2 * core + row_ids // PAD, key_ids // 4, slots)[None]

    def await_part(parity, j):
        copy = part_send(parity, j)
        copy.wait_recv()
        copy.wait_send()

    def update_x(parity, j):
        update = (own_buf[j] + recv_buf[parity, j]).astype(BF16)
        cols = slice(j * TILE, (j + 1) * TILE)
        x_buf[:, cols] = (x_buf[:, cols].astype(F32) + update.astype(F32)).astype(BF16)

    def layer_body(layer, carry):
        parity_in = lax.rem(layer + 1, 2)
        parity_out = lax.rem(layer, 2)

        @pl.when(layer < layers - 3)
        def _():
            for copy in raw_loads(layer + 3):
                copy.start()

        for k in range(3):
            pre_remote(layer, k).wait_send()

        @pl.when(layer < layers - 2)
        def _():
            for copy in suf_loads(layer + 2):
                copy.start()
            split_prefix(layer + 2)

        for i, (a, b) in enumerate(blocks):
            if i == 0:
                for copy in qkv_copies(layer, 0):
                    copy.wait()
            if i + 1 < len(blocks):
                for copy in qkv_copies(layer, i + 1):
                    copy.wait()
            for j in range(a, b):
                await_part(parity_in, j)
            for j in range(a, b):
                update_x(parity_in, j)
            r = slice(a * TILE, b * TILE)
            x = x_buf[:, r]
            parts = ((slice(0, q_width), wq_buf), (slice(q_width, q_width + kv_width), wk_buf),
                     (slice(q_width + kv_width, q_width + 2 * kv_width), wv_buf))
            for cols, w_buf in parts:
                product = jnp.dot(x, w_buf[r, :], preferred_element_type=F32)
                acc_buf[:, cols] = product if i == 0 else acc_buf[:, cols] + product

            @pl.when(layer < layers - 1)
            def _():
                for copy in qkv_copies(layer + 1, i):
                    copy.start()
                if i == 0:
                    for copy in suf_loads(layer + 1):
                        copy.wait()
                    suf_send(layer + 1).start()

            if i == 0:
                @pl.when(layer < layers - 2)
                def _():
                    for k in range(3):
                        pre_remote(layer + 2, k).start()

        @pl.when(layer < layers - 1)
        def _():
            wo_copy(layer + 1, 0).start()

        for h in range(2):
            for g in range(group):
                col = (h * group + g) * head_dim
                q_buf[h, pl.ds(g, both, stride=PAD), :] = acc_buf[:, col:col + head_dim].astype(BF16).astype(F32)
            for kv in range(2):
                col = q_width + kv * kv_width + h * head_dim
                fresh = acc_buf[:, col:col + head_dim].astype(BF16).astype(F32)
                kvn_buf[kv, h] = fresh
        for h in range(2):
            for kv in range(2):
                kv_mine_buf[layer, kv, h] = kvn_buf[kv, h, pl.ds(mine, rows), :]
                kv_send_buf[layer, kv, h] = kvn_buf[kv, h, pl.ds(other, rows), :]

        for k in range(3):
            pre_remote(layer, k).wait_recv()
        suf_send(layer).wait()

        per_core = rows // CHUNK

        def unpair(both_seqs):
            first_seq = both_seqs[:, None, 0:2 * PAD, 0:128]
            second_seq = both_seqs[:, None, 2 * PAD:4 * PAD, 128:256]
            return jnp.concatenate([first_seq, second_seq], axis=1).reshape(CHUNK, 2 * PAD, 128)

        def attend(i):
            away = i // per_core
            part = pl.multiple_of(lax.rem(i, per_core) * CHUNK, CHUNK)
            first = pl.multiple_of(lax.rem(core + away, 2) * rows + part, CHUNK)
            slot = (1 - away) * lax.rem(layer, 3) + away * (3 + lax.rem(layer, 2))
            chunk_rows = pl.ds(pl.multiple_of(first * PAD, CHUNK * PAD), CHUNK * PAD)
            q_heads = [q_buf[h, chunk_rows, :] for h in range(2)]
            q3 = jnp.concatenate([q.reshape(CHUNK, PAD, head_dim) for q in q_heads], axis=1)
            k_suf = suf_buf[slot, 0, pl.ds(part, CHUNK)]
            v_suf = suf_buf[slot, 1, pl.ds(part, CHUNK)]
            q_pairs = q3.astype(BF16).reshape(CHUNK // 2, 4 * PAD, head_dim)
            k_pairs = k_suf.reshape(CHUNK // 2, 256, head_dim)
            suf_scores = unpair(lax.dot_general(q_pairs, k_pairs, (((2,), (2,)), ((0,), (0,))), preferred_element_type=F32))
            suf_scores = jnp.where(key_slot < lens_buf[pl.ds(first, CHUNK)], suf_scores, -jnp.inf)
            def spread(kv):
                picked = [jnp.broadcast_to(kvn_buf[kv, h, pl.ds(first + b, 1), :], (PAD, head_dim)) for b in range(CHUNK) for h in range(2)]
                return jnp.concatenate(picked, axis=0).reshape(CHUNK, 2 * PAD, head_dim)

            k_new = spread(0)
            v_new = spread(1)
            new_scores = jnp.sum(q3 * k_new, axis=-1, keepdims=True)
            suf_weights, new_weights, masses, pre_vals = [], [], [], []
            for h in range(2):
                hs = slice(h * PAD, (h + 1) * PAD)
                q_h = q_heads[h].astype(BF16)
                k_pre = pre_buf[layer, 0, h].reshape(-1, head_dim)
                v_pre = pre_buf[layer, 1, h].reshape(-1, head_dim)
                scores = lax.dot_general(q_h, k_pre, (((1,), (1,)), ((), ())), preferred_element_type=F32)
                suf_h = suf_scores[:, hs, :].reshape(CHUNK * PAD, 128)
                new_h = new_scores[:, hs, :].reshape(CHUNK * PAD, 1)
                peak = jnp.maximum(jnp.maximum(scores.max(axis=-1, keepdims=True), suf_h.max(axis=-1, keepdims=True)), new_h)
                pre_w = jnp.exp2((scores - peak) * (scale * LOG2E))
                suf_w = jnp.exp2((suf_h - peak) * (scale * LOG2E))
                new_w = jnp.exp2((new_h - peak) * (scale * LOG2E))
                masses.append(pre_w.sum(axis=-1, keepdims=True) + suf_w.sum(axis=-1, keepdims=True) + new_w)
                pre_vals.append(jnp.dot(pre_w.astype(BF16), v_pre, preferred_element_type=F32))
                suf_weights.append(suf_w.reshape(CHUNK, PAD, 128))
                new_weights.append(new_w)
            suf_w = jnp.concatenate(suf_weights, axis=1).astype(BF16)
            v_suf = v_suf.reshape(CHUNK // 2, 2, 128, head_dim)
            v_pairs = jnp.concatenate([v_suf[:, 0], v_suf[:, 1]], axis=-1)
            suf_w = suf_w.reshape(CHUNK // 2, 4 * PAD, 128)
            suf_vals = unpair(lax.dot_general(suf_w, v_pairs, (((2,), (1,)), ((0,), (0,))), preferred_element_type=F32))
            for h in range(2):
                hs = slice(h * PAD, (h + 1) * PAD)
                mixed = pre_vals[h] + suf_vals[:, hs, :].reshape(CHUNK * PAD, head_dim)
                mixed = mixed + new_weights[h] * v_new[:, hs, :].reshape(CHUNK * PAD, head_dim)
                o_buf[h, chunk_rows, :] = mixed / masses[h]

        def attend_trip(trip, carry):
            for i in range(CHUNKS_PER_TRIP):
                attend(trip * CHUNKS_PER_TRIP + i)
            return carry

        lax.fori_loop(0, 2 * per_core // CHUNKS_PER_TRIP, attend_trip, 0)

        @pl.when(layer == layers - 1)
        def _():
            kv_store.start()
            kv_send.start()

        wo_copy(layer, 0).wait()
        wo_copy(layer, 1).wait()

        for h in range(2):
            for g in range(group):
                col = (h * group + g) * head_dim
                att_buf[:, col:col + head_dim] = o_buf[h, pl.ds(g, both, stride=PAD), :].astype(BF16)

        for i, (a, b) in enumerate(blocks):
            if 0 < i < len(blocks) - 1:
                wo_copy(layer, i + 1).wait()
            weights = wo_first_buf[lax.rem(layer, 2)] if i == 0 else wo_buf[:, (a - BLOCK) * TILE:(b - BLOCK) * TILE]
            product = jnp.dot(att_buf[...], weights, preferred_element_type=F32)
            for j in range(a, b):
                own_buf[j] = product[:, (j - a) * TILE:(j - a + 1) * TILE]

            if i > 0:
                @pl.when(layer < layers - 1)
                def _():
                    wo_copy(layer + 1, i).start()

            for j in range(a, b):
                part_send(parity_out, j).start()

        return carry

    lax.fori_loop(0, layers, layer_body, 0)
    for j in range(tiles):
        await_part((layers - 1) % 2, j)
    for j in range(tiles):
        update_x((layers - 1) % 2, j)
        out_ref[:, j * TILE:(j + 1) * TILE] = x_buf[pl.ds(mine, rows), j * TILE:(j + 1) * TILE]
    kv_store.wait()
    kv_send.wait()


def cache_kernel(lens_ref, new_ref, hidden_ref, k_ref, v_ref, hidden_out_ref, k_out_ref, v_out_ref,
                 buf, new_buf, hidden_buf, in_sem, out_sem, new_sem, hidden_sem):
    layers, rows, _, heads, _ = k_ref.shape

    def loads(layer):
        return (
            pltpu.make_async_copy(new_ref.at[layer], new_buf.at[layer], new_sem.at[layer]),
            pltpu.make_async_copy(k_ref.at[layer], buf.at[layer, 0], in_sem.at[layer, 0]),
            pltpu.make_async_copy(v_ref.at[layer], buf.at[layer, 1], in_sem.at[layer, 1]),
        )

    def stores(layer):
        return (
            pltpu.make_async_copy(buf.at[layer, 0], k_out_ref.at[layer], out_sem.at[layer, 0]),
            pltpu.make_async_copy(buf.at[layer, 1], v_out_ref.at[layer], out_sem.at[layer, 1]),
        )

    hidden_load = pltpu.make_async_copy(hidden_ref, hidden_buf, hidden_sem.at[0])
    hidden_store = pltpu.make_async_copy(hidden_buf, hidden_out_ref, hidden_sem.at[1])
    hidden_load.start()
    for layer in range(layers):
        for copy in loads(layer):
            copy.start()

    def patch(layer, carry):
        for copy in loads(layer):
            copy.wait()
        for kv in range(2):
            for b in range(rows):
                buf[layer, kv, b, lens_ref[b]] = new_buf[layer, kv, pl.ds(b, heads, stride=rows), :].astype(BF16)

        @pl.when(layer >= WRITE_LAG)
        def _():
            for copy in stores(layer - WRITE_LAG):
                copy.start()

        return carry

    lax.fori_loop(0, layers, patch, 0)
    for layer in range(layers - WRITE_LAG, layers):
        for copy in stores(layer):
            copy.start()
    hidden_load.wait()
    hidden_store.start()
    for layer in range(layers):
        for copy in stores(layer):
            copy.wait()
    hidden_store.wait()


def solution(mesh):
    home_axes = ('data', 'ctx')
    row_spec = P(home_axes, None)
    lens_spec = P(home_axes)
    whole_spec = P()
    prefix_spec = P(None, home_axes, None, None)
    cache_spec = P(None, home_axes, None, None, None)

    def local_step(hidden, seq_lens, w_query, w_key, w_value, w_out, k_prefix, v_prefix, k_suffix, v_suffix):
        layers, model_dim = w_query.shape[:2]
        positions, kv_heads, head_dim = k_prefix.shape[1:]
        rows = hidden.shape[0]
        slots = k_suffix.shape[2]
        group = w_query.shape[2] // head_dim // kv_heads
        half_heads = kv_heads // 2
        q_width = w_query.shape[2] // 2
        kv_width = w_key.shape[2] // 2
        tiles = model_dim // TILE
        keys = slots * kv_heads
        both = 2 * rows

        k_flat = k_suffix.reshape(layers, rows, keys, head_dim)
        v_flat = v_suffix.reshape(layers, rows, keys, head_dim)
        k_pre = k_prefix.reshape(layers, positions * kv_heads, head_dim)
        v_pre = v_prefix.reshape(layers, positions * kv_heads, head_dim)

        any_spec = pl.BlockSpec(memory_space=pl.ANY)
        smem_spec = pl.BlockSpec(memory_space=pltpu.SMEM)
        vmem_spec = pl.BlockSpec(memory_space=pltpu.VMEM)
        dma = pltpu.SemaphoreType.DMA
        hidden_out, kv_new = pl.pallas_call(
            functools.partial(decode_kernel, (layers, rows, group, head_dim, slots)),
            out_shape=(jax.ShapeDtypeStruct((rows, model_dim), BF16),
                       jax.ShapeDtypeStruct((layers, 2, kv_heads, rows, head_dim), F32)),
            in_specs=[vmem_spec, vmem_spec] + [any_spec] * 8,
            out_specs=(vmem_spec, any_spec),
            scratch_shapes=[
                pltpu.VMEM((model_dim, q_width), BF16),
                pltpu.VMEM((model_dim, kv_width), BF16),
                pltpu.VMEM((model_dim, kv_width), BF16),
                pltpu.VMEM((2, q_width, BLOCK * TILE), BF16),
                pltpu.VMEM((q_width, model_dim - BLOCK * TILE), BF16),
                pltpu.VMEM((layers, 2, half_heads, 4, positions, head_dim), BF16),
                pltpu.VMEM((2, 2, positions * kv_heads, head_dim), BF16),
                pltpu.VMEM((2, positions * kv_heads, head_dim), F32),
                pltpu.VMEM((2, 2, 2, half_heads, positions, head_dim), BF16),
                pltpu.VMEM((5, 2, rows, keys, head_dim), BF16),
                pltpu.VMEM((both, model_dim), BF16),
                pltpu.VMEM((tiles, both, TILE), F32),
                pltpu.VMEM((2, tiles, both, TILE), F32),
                pltpu.VMEM((both, q_width + 2 * kv_width), F32),
                pltpu.VMEM((half_heads, both * PAD, head_dim), F32),
                pltpu.VMEM((2, half_heads, both, head_dim), F32),
                pltpu.VMEM((half_heads, both * PAD, head_dim), F32),
                pltpu.VMEM((both, q_width), BF16),
                pltpu.VMEM((both, 2 * PAD, 128), jnp.int32),
                pltpu.VMEM((layers, 2, half_heads, rows, head_dim), F32),
                pltpu.VMEM((layers, 2, half_heads, rows, head_dim), F32),
                dma((4, tiles // BLOCK)), dma((2,)), dma((3, 2)), dma((2,)), dma((2,)), dma((2, 2)), dma((layers, 3)), dma((layers, 3)),
                dma((tiles,)), dma((2, tiles)), dma((2,)), dma((3,)),
            ],
            compiler_params=pltpu.CompilerParams(collective_id=0, has_side_effects=True, vmem_limit_bytes=66_000_000),
            name="decode_layers",
        )(seq_lens.reshape(1, rows), hidden, w_query, w_key, w_value, w_out, k_pre, v_pre, k_flat, v_flat)

        hidden_out, k_out, v_out = pl.pallas_call(
            cache_kernel,
            out_shape=(jax.ShapeDtypeStruct(hidden.shape, BF16), jax.ShapeDtypeStruct(k_suffix.shape, BF16), jax.ShapeDtypeStruct(v_suffix.shape, BF16)),
            in_specs=[smem_spec] + [any_spec] * 4,
            out_specs=(any_spec, any_spec, any_spec),
            scratch_shapes=[
                pltpu.VMEM((layers, 2) + k_suffix.shape[1:], BF16),
                pltpu.VMEM((layers, 2, kv_heads * rows, head_dim), F32),
                pltpu.VMEM(hidden.shape, BF16),
                dma((layers, 2)), dma((layers, 2)), dma((layers,)), dma((2,)),
            ],
            compiler_params=pltpu.CompilerParams(vmem_limit_bytes=60_000_000),
            name="write_caches",
        )(seq_lens, kv_new.reshape(layers, 2, kv_heads * rows, head_dim), hidden_out, k_suffix, v_suffix)
        return hidden_out, k_out, v_out

    return jax.shard_map(local_step, mesh=mesh, in_specs=(row_spec, lens_spec, whole_spec, whole_spec, whole_spec, whole_spec, prefix_spec, prefix_spec, cache_spec, cache_spec), out_specs=(row_spec, cache_spec, cache_spec), check_vma=False)
```

```python
import functools

import jax
import jax.numpy as jnp
from jax import lax
from jax.experimental import pallas as pl
from jax.experimental.pallas import tpu as pltpu
from jax.sharding import PartitionSpec as P

MESH = pl.DeviceIdType.MESH
BF16 = jnp.bfloat16
F32 = jnp.float32
TILE = 512
CHUNK = 32
PAD = 8
WRITE_LAG = 15
BLOCK = 2
LOG2E = 1.4426950408889634
CHUNKS_PER_TRIP = 1


def decode_kernel(dims, lens_hbm, hidden_hbm, wq_ref, wk_ref, wv_ref, wo_ref, kpre_ref, vpre_ref, ksuf_ref, vsuf_ref,
                  out_ref, kv_out_ref,
                  lens_ref, hidden_ref, wq_buf, wk_buf, wv_buf, wo_first_buf, wo_buf, pre_buf, raw_buf, wide_buf, split_buf, suf_buf, x_buf, own_buf, recv_buf, acc_buf,
                  q_buf, kvn_buf, o_buf, att_buf, lens_buf, kv_mine_buf, kv_send_buf,
                  entry_sem, w_sem, wo_first_sem, suf_load_sem, suf_send_sem, suf_recv_sem, raw_sem, pre_send_sem, pre_recv_sem,
                  part_send_sem, part_recv_sem, lens_sem, kv_sem):
    layers, rows, group, head_dim, slots = dims
    half_heads = 2
    tiles = own_buf.shape[0]
    q_width = wq_buf.shape[1]
    kv_width = wk_buf.shape[1]
    blocks = [(i * BLOCK, (i + 1) * BLOCK if i < tiles // BLOCK - 1 else tiles) for i in range(tiles // BLOCK)]
    both = 2 * rows
    me = lax.axis_index("ctx")
    core = lax.rem(me, 2)
    chip = me // 2
    mate = chip * 2 + (1 - core)
    across = (1 - chip) * 2 + core
    diagonal = (1 - chip) * 2 + (1 - core)
    peers = ((mate, 1 - core), (across, core), (diagonal, 1 - core))
    mine = pl.multiple_of(core * rows, rows)
    other = pl.multiple_of((1 - core) * rows, rows)
    q_col = pl.multiple_of(core * q_width, 128)
    kv_col = pl.multiple_of(core * kv_width, 128)
    scale = head_dim ** -0.5

    def qkv_copies(layer, i):
        a, b = blocks[i]
        r = pl.ds(a * TILE, (b - a) * TILE)
        return (
            pltpu.make_async_copy(wq_ref.at[layer, r, pl.ds(q_col, q_width)], wq_buf.at[r], w_sem.at[0, i]),
            pltpu.make_async_copy(wk_ref.at[layer, r, pl.ds(kv_col, kv_width)], wk_buf.at[r], w_sem.at[1, i]),
            pltpu.make_async_copy(wv_ref.at[layer, r, pl.ds(kv_col, kv_width)], wv_buf.at[r], w_sem.at[2, i]),
        )

    def wo_copy(layer, i):
        a, b = blocks[i]
        src = wo_ref.at[layer, pl.ds(q_col, q_width), pl.ds(a * TILE, (b - a) * TILE)]
        if i == 0:
            return pltpu.make_async_copy(src, wo_first_buf.at[lax.rem(layer, 2)], wo_first_sem.at[lax.rem(layer, 2)])
        return pltpu.make_async_copy(src, wo_buf.at[:, pl.ds((a - BLOCK) * TILE, (b - a) * TILE)], w_sem.at[3, i])

    def suf_loads(layer):
        slot = lax.rem(layer, 3)
        return (
            pltpu.make_async_copy(ksuf_ref.at[layer], suf_buf.at[slot, 0], suf_load_sem.at[slot, 0]),
            pltpu.make_async_copy(vsuf_ref.at[layer], suf_buf.at[slot, 1], suf_load_sem.at[slot, 1]),
        )

    def suf_send(layer):
        return pltpu.make_async_remote_copy(
            src_ref=suf_buf.at[lax.rem(layer, 3)], dst_ref=suf_buf.at[3 + lax.rem(layer, 2)],
            send_sem=suf_send_sem.at[lax.rem(layer, 2)], recv_sem=suf_recv_sem.at[lax.rem(layer, 2)],
            device_id={"ctx": mate}, device_id_type=MESH)

    def raw_loads(layer):
        slot = lax.rem(layer, 2)
        return (
            pltpu.make_async_copy(kpre_ref.at[layer], raw_buf.at[slot, 0], raw_sem.at[slot, 0]),
            pltpu.make_async_copy(vpre_ref.at[layer], raw_buf.at[slot, 1], raw_sem.at[slot, 1]),
        )

    def split_prefix(layer):
        slot = lax.rem(layer, 2)
        heads = 2 * half_heads
        positions = pre_buf.shape[4]
        for copy in raw_loads(layer):
            copy.wait()
        for kv in range(2):
            wide_buf[kv] = raw_buf[slot, kv].astype(F32)
            for h in range(half_heads):
                for half in range(2):
                    split_buf[slot, half, kv, h] = wide_buf[kv, pl.ds(half * half_heads + h, positions, stride=heads), :].astype(BF16)
                pre_buf[layer, kv, h, me] = split_buf[slot, core, kv, h]

    def pre_remote(layer, k):
        device, half = peers[k]
        return pltpu.make_async_remote_copy(
            src_ref=split_buf.at[lax.rem(layer, 2), half], dst_ref=pre_buf.at[layer, :, :, me],
            send_sem=pre_send_sem.at[layer, k], recv_sem=pre_recv_sem.at[layer, k],
            device_id={"ctx": device}, device_id_type=MESH)

    def part_send(parity, j):
        return pltpu.make_async_remote_copy(
            src_ref=own_buf.at[j], dst_ref=recv_buf.at[parity, j],
            send_sem=part_send_sem.at[j], recv_sem=part_recv_sem.at[parity, j],
            device_id={"ctx": mate}, device_id_type=MESH)

    lens_send = pltpu.make_async_remote_copy(
        src_ref=lens_buf.at[pl.ds(mine, rows)], dst_ref=lens_buf.at[pl.ds(mine, rows)], send_sem=lens_sem.at[0], recv_sem=lens_sem.at[1],
        device_id={"ctx": mate}, device_id_type=MESH)
    kv_slice = kv_out_ref.at[:, :, pl.ds(core * half_heads, half_heads)]
    kv_store = pltpu.make_async_copy(kv_mine_buf, kv_slice, kv_sem.at[2])
    kv_send = pltpu.make_async_remote_copy(
        src_ref=kv_send_buf, dst_ref=kv_slice, send_sem=kv_sem.at[0], recv_sem=kv_sem.at[1],
        device_id={"ctx": mate}, device_id_type=MESH)

    barrier = pltpu.get_barrier_semaphore()
    for device, _ in peers:
        pl.semaphore_signal(barrier, inc=1, device_id={"ctx": device}, device_id_type=MESH)
    entry_copies = (pltpu.make_async_copy(hidden_hbm, hidden_ref, entry_sem.at[0]), pltpu.make_async_copy(lens_hbm, lens_ref, entry_sem.at[1]))
    for copy in entry_copies:
        copy.start()
    for layer in range(2):
        for copy in raw_loads(layer):
            copy.start()
    for i in range(len(blocks)):
        for copy in qkv_copies(0, i):
            copy.start()
        if i == 0:
            for copy in suf_loads(0):
                copy.start()
    for i in range(len(blocks)):
        wo_copy(0, i).start()
    for copy in suf_loads(1):
        copy.start()

    x_buf[...] = jnp.zeros_like(x_buf)
    q_buf[...] = jnp.zeros_like(q_buf)
    for copy in entry_copies:
        copy.wait()
    for j in range(tiles):
        own_buf[j] = jnp.zeros_like(own_buf[j])
        own_buf[j, pl.ds(mine, rows), :] = hidden_ref[:, j * TILE:(j + 1) * TILE].astype(F32)
    diagonal_hit = lax.broadcasted_iota(jnp.int32, (rows, rows), 0) == lax.broadcasted_iota(jnp.int32, (rows, rows), 1)
    lens_wide = jnp.broadcast_to(lens_ref[...].astype(F32), (rows, rows))
    lens_wide = jnp.where(diagonal_hit, lens_wide, 0.0).sum(axis=1, keepdims=True)
    lens_wide = jnp.broadcast_to(lens_wide, (rows, 128)).astype(jnp.int32)
    for b in range(rows):
        lens_buf[mine + b] = jnp.broadcast_to(lens_wide[b:b + 1, :], (2 * PAD, 128))
    split_prefix(0)
    for copy in raw_loads(2):
        copy.start()
    split_prefix(1)

    pl.semaphore_wait(barrier, 3)

    for j in range(tiles):
        part_send(1, j).start()
    lens_send.start()
    for layer in range(2):
        for k in range(3):
            pre_remote(layer, k).start()
    for copy in suf_loads(0):
        copy.wait()
    suf_send(0).start()
    lens_send.wait()

    row_ids = lax.broadcasted_iota(jnp.int32, (2 * PAD, 128), 0)
    key_ids = lax.broadcasted_iota(jnp.int32, (2 * PAD, 128), 1)
    key_slot = jnp.where(lax.rem(key_ids, 4) == 2 * core + row_ids // PAD, key_ids // 4, slots)[None]

    def await_part(parity, j):
        copy = part_send(parity, j)
        copy.wait_recv()
        copy.wait_send()

    def update_x(parity, j):
        update = (own_buf[j] + recv_buf[parity, j]).astype(BF16)
        cols = slice(j * TILE, (j + 1) * TILE)
        x_buf[:, cols] = (x_buf[:, cols].astype(F32) + update.astype(F32)).astype(BF16)

    def layer_body(layer, carry):
        parity_in = lax.rem(layer + 1, 2)
        parity_out = lax.rem(layer, 2)

        @pl.when(layer < layers - 3)
        def _():
            for copy in raw_loads(layer + 3):
                copy.start()

        for k in range(3):
            pre_remote(layer, k).wait_send()

        @pl.when(layer < layers - 2)
        def _():
            for copy in suf_loads(layer + 2):
                copy.start()
            split_prefix(layer + 2)

        for i, (a, b) in enumerate(blocks):
            if i == 0:
                for copy in qkv_copies(layer, 0):
                    copy.wait()
            if i + 1 < len(blocks):
                for copy in qkv_copies(layer, i + 1):
                    copy.wait()
            for j in range(a, b):
                await_part(parity_in, j)
            for j in range(a, b):
                update_x(parity_in, j)
            r = slice(a * TILE, b * TILE)
            x = x_buf[:, r]
            parts = ((slice(0, q_width), wq_buf), (slice(q_width, q_width + kv_width), wk_buf),
                     (slice(q_width + kv_width, q_width + 2 * kv_width), wv_buf))
            for cols, w_buf in parts:
                product = jnp.dot(x, w_buf[r, :], preferred_element_type=F32)
                acc_buf[:, cols] = product if i == 0 else acc_buf[:, cols] + product

            @pl.when(layer < layers - 1)
            def _():
                for copy in qkv_copies(layer + 1, i):
                    copy.start()
                if i == 0:
                    for copy in suf_loads(layer + 1):
                        copy.wait()
                    suf_send(layer + 1).start()

            if i == 0:
                @pl.when(layer < layers - 2)
                def _():
                    for k in range(3):
                        pre_remote(layer + 2, k).start()

        @pl.when(layer < layers - 1)
        def _():
            wo_copy(layer + 1, 0).start()

        for h in range(2):
            for g in range(group):
                col = (h * group + g) * head_dim
                q_buf[h, pl.ds(g, both, stride=PAD), :] = acc_buf[:, col:col + head_dim].astype(BF16).astype(F32)
            for kv in range(2):
                col = q_width + kv * kv_width + h * head_dim
                fresh = acc_buf[:, col:col + head_dim].astype(BF16).astype(F32)
                kvn_buf[kv, h] = fresh
        for h in range(2):
            for kv in range(2):
                kv_mine_buf[layer, kv, h] = kvn_buf[kv, h, pl.ds(mine, rows), :].astype(BF16)
                kv_send_buf[layer, kv, h] = kvn_buf[kv, h, pl.ds(other, rows), :].astype(BF16)

        for k in range(3):
            pre_remote(layer, k).wait_recv()
        suf_send(layer).wait()

        per_core = rows // CHUNK

        def unpair(both_seqs):
            first_seq = both_seqs[:, None, 0:2 * PAD, 0:128]
            second_seq = both_seqs[:, None, 2 * PAD:4 * PAD, 128:256]
            return jnp.concatenate([first_seq, second_seq], axis=1).reshape(CHUNK, 2 * PAD, 128)

        def attend(i):
            away = i // per_core
            part = pl.multiple_of(lax.rem(i, per_core) * CHUNK, CHUNK)
            first = pl.multiple_of(lax.rem(core + away, 2) * rows + part, CHUNK)
            slot = (1 - away) * lax.rem(layer, 3) + away * (3 + lax.rem(layer, 2))
            chunk_rows = pl.ds(pl.multiple_of(first * PAD, CHUNK * PAD), CHUNK * PAD)
            q_heads = [q_buf[h, chunk_rows, :] for h in range(2)]
            q3 = jnp.concatenate([q.reshape(CHUNK, PAD, head_dim) for q in q_heads], axis=1)
            k_suf = suf_buf[slot, 0, pl.ds(part, CHUNK)]
            v_suf = suf_buf[slot, 1, pl.ds(part, CHUNK)]
            q_pairs = q3.astype(BF16).reshape(CHUNK // 2, 4 * PAD, head_dim)
            k_pairs = k_suf.reshape(CHUNK // 2, 256, head_dim)
            suf_scores = unpair(lax.dot_general(q_pairs, k_pairs, (((2,), (2,)), ((0,), (0,))), preferred_element_type=F32))
            suf_scores = jnp.where(key_slot < lens_buf[pl.ds(first, CHUNK)], suf_scores, -jnp.inf)
            def spread(kv):
                picked = [jnp.broadcast_to(kvn_buf[kv, h, pl.ds(first + b, 1), :], (PAD, head_dim)) for b in range(CHUNK) for h in range(2)]
                return jnp.concatenate(picked, axis=0).reshape(CHUNK, 2 * PAD, head_dim)

            k_new = spread(0)
            v_new = spread(1)
            new_scores = jnp.sum(q3 * k_new, axis=-1, keepdims=True)
            suf_weights, new_weights, masses, pre_vals = [], [], [], []
            for h in range(2):
                hs = slice(h * PAD, (h + 1) * PAD)
                q_h = q_heads[h].astype(BF16)
                k_pre = pre_buf[layer, 0, h].reshape(-1, head_dim)
                v_pre = pre_buf[layer, 1, h].reshape(-1, head_dim)
                scores = lax.dot_general(q_h, k_pre, (((1,), (1,)), ((), ())), preferred_element_type=F32)
                suf_h = suf_scores[:, hs, :].reshape(CHUNK * PAD, 128)
                new_h = new_scores[:, hs, :].reshape(CHUNK * PAD, 1)
                peak = jnp.maximum(jnp.maximum(scores.max(axis=-1, keepdims=True), suf_h.max(axis=-1, keepdims=True)), new_h)
                pre_w = jnp.exp2((scores - peak) * (scale * LOG2E))
                suf_w = jnp.exp2((suf_h - peak) * (scale * LOG2E))
                new_w = jnp.exp2((new_h - peak) * (scale * LOG2E))
                masses.append(pre_w.sum(axis=-1, keepdims=True) + suf_w.sum(axis=-1, keepdims=True) + new_w)
                pre_vals.append(jnp.dot(pre_w.astype(BF16), v_pre, preferred_element_type=F32))
                suf_weights.append(suf_w.reshape(CHUNK, PAD, 128))
                new_weights.append(new_w)
            suf_w = jnp.concatenate(suf_weights, axis=1).astype(BF16)
            v_suf = v_suf.reshape(CHUNK // 2, 2, 128, head_dim)
            v_pairs = jnp.concatenate([v_suf[:, 0], v_suf[:, 1]], axis=-1)
            suf_w = suf_w.reshape(CHUNK // 2, 4 * PAD, 128)
            suf_vals = unpair(lax.dot_general(suf_w, v_pairs, (((2,), (1,)), ((0,), (0,))), preferred_element_type=F32))
            for h in range(2):
                hs = slice(h * PAD, (h + 1) * PAD)
                mixed = pre_vals[h] + suf_vals[:, hs, :].reshape(CHUNK * PAD, head_dim)
                mixed = mixed + new_weights[h] * v_new[:, hs, :].reshape(CHUNK * PAD, head_dim)
                o_buf[h, chunk_rows, :] = mixed / masses[h]

        def attend_trip(trip, carry):
            for i in range(CHUNKS_PER_TRIP):
                attend(trip * CHUNKS_PER_TRIP + i)
            return carry

        lax.fori_loop(0, 2 * per_core // CHUNKS_PER_TRIP, attend_trip, 0)

        @pl.when(layer == layers - 1)
        def _():
            kv_store.start()
            kv_send.start()

        wo_copy(layer, 0).wait()
        wo_copy(layer, 1).wait()

        for h in range(2):
            for g in range(group):
                col = (h * group + g) * head_dim
                att_buf[:, col:col + head_dim] = o_buf[h, pl.ds(g, both, stride=PAD), :].astype(BF16)

        for i, (a, b) in enumerate(blocks):
            if 0 < i < len(blocks) - 1:
                wo_copy(layer, i + 1).wait()
            weights = wo_first_buf[lax.rem(layer, 2)] if i == 0 else wo_buf[:, (a - BLOCK) * TILE:(b - BLOCK) * TILE]
            product = jnp.dot(att_buf[...], weights, preferred_element_type=F32)
            for j in range(a, b):
                own_buf[j] = product[:, (j - a) * TILE:(j - a + 1) * TILE]

            if i > 0:
                @pl.when(layer < layers - 1)
                def _():
                    wo_copy(layer + 1, i).start()

            for j in range(a, b):
                part_send(parity_out, j).start()

        return carry

    lax.fori_loop(0, layers, layer_body, 0)
    for j in range(tiles):
        await_part((layers - 1) % 2, j)
    for j in range(tiles):
        update_x((layers - 1) % 2, j)
        out_ref[:, j * TILE:(j + 1) * TILE] = x_buf[pl.ds(mine, rows), j * TILE:(j + 1) * TILE]
    kv_store.wait()
    kv_send.wait()


def cache_kernel(lens_hbm, new_ref, hidden_ref, k_ref, v_ref, hidden_out_ref, k_out_ref, v_out_ref,
                 buf, new_buf, wide_buf, lens_ref, hidden_buf, in_sem, out_sem, new_sem, hidden_sem):
    layers, rows, _, heads, _ = k_ref.shape

    def loads(layer):
        return (
            pltpu.make_async_copy(new_ref.at[layer], new_buf.at[layer], new_sem.at[layer]),
            pltpu.make_async_copy(k_ref.at[layer], buf.at[layer, 0], in_sem.at[layer, 0]),
            pltpu.make_async_copy(v_ref.at[layer], buf.at[layer, 1], in_sem.at[layer, 1]),
        )

    def stores(layer):
        return (
            pltpu.make_async_copy(buf.at[layer, 0], k_out_ref.at[layer], out_sem.at[layer, 0]),
            pltpu.make_async_copy(buf.at[layer, 1], v_out_ref.at[layer], out_sem.at[layer, 1]),
        )

    hidden_load = pltpu.make_async_copy(hidden_ref, hidden_buf, hidden_sem.at[0])
    hidden_store = pltpu.make_async_copy(hidden_buf, hidden_out_ref, hidden_sem.at[1])
    lens_load = pltpu.make_async_copy(lens_hbm, lens_ref, hidden_sem.at[2])
    for layer in range(layers):
        for copy in loads(layer):
            copy.start()
        if layer == 0:
            lens_load.start()
            hidden_load.start()
    lens_load.wait()

    def patch(layer, carry):
        for copy in loads(layer):
            copy.wait()
        for kv in range(2):
            wide_buf[kv] = new_buf[layer, kv].astype(F32)
            for b in range(rows):
                buf[layer, kv, b, lens_ref[b]] = wide_buf[kv, pl.ds(b, heads, stride=rows), :].astype(BF16)

        @pl.when(layer >= WRITE_LAG)
        def _():
            for copy in stores(layer - WRITE_LAG):
                copy.start()

        return carry

    lax.fori_loop(0, layers, patch, 0)
    for layer in range(layers - WRITE_LAG, layers):
        for copy in stores(layer):
            copy.start()
    hidden_load.wait()
    hidden_store.start()
    for layer in range(layers):
        for copy in stores(layer):
            copy.wait()
    hidden_store.wait()


def solution(mesh):
    home_axes = ('data', 'ctx')
    row_spec = P(home_axes, None)
    lens_spec = P(home_axes)
    whole_spec = P()
    prefix_spec = P(None, home_axes, None, None)
    cache_spec = P(None, home_axes, None, None, None)

    def local_step(hidden, seq_lens, w_query, w_key, w_value, w_out, k_prefix, v_prefix, k_suffix, v_suffix):
        layers, model_dim = w_query.shape[:2]
        positions, kv_heads, head_dim = k_prefix.shape[1:]
        rows = hidden.shape[0]
        slots = k_suffix.shape[2]
        group = w_query.shape[2] // head_dim // kv_heads
        half_heads = kv_heads // 2
        q_width = w_query.shape[2] // 2
        kv_width = w_key.shape[2] // 2
        tiles = model_dim // TILE
        keys = slots * kv_heads
        both = 2 * rows

        k_flat = k_suffix.reshape(layers, rows, keys, head_dim)
        v_flat = v_suffix.reshape(layers, rows, keys, head_dim)
        k_pre = k_prefix.reshape(layers, positions * kv_heads, head_dim)
        v_pre = v_prefix.reshape(layers, positions * kv_heads, head_dim)

        any_spec = pl.BlockSpec(memory_space=pl.ANY)
        vmem_spec = pl.BlockSpec(memory_space=pltpu.VMEM)
        dma = pltpu.SemaphoreType.DMA
        hidden_out, kv_new = pl.pallas_call(
            functools.partial(decode_kernel, (layers, rows, group, head_dim, slots)),
            out_shape=(jax.ShapeDtypeStruct((rows, model_dim), BF16),
                       jax.ShapeDtypeStruct((layers, 2, kv_heads, rows, head_dim), BF16)),
            in_specs=[any_spec] * 10,
            out_specs=(vmem_spec, any_spec),
            scratch_shapes=[
                pltpu.VMEM((1, rows), jnp.int32),
                pltpu.VMEM(hidden.shape, BF16),
                pltpu.VMEM((model_dim, q_width), BF16),
                pltpu.VMEM((model_dim, kv_width), BF16),
                pltpu.VMEM((model_dim, kv_width), BF16),
                pltpu.VMEM((2, q_width, BLOCK * TILE), BF16),
                pltpu.VMEM((q_width, model_dim - BLOCK * TILE), BF16),
                pltpu.VMEM((layers, 2, half_heads, 4, positions, head_dim), BF16),
                pltpu.VMEM((2, 2, positions * kv_heads, head_dim), BF16),
                pltpu.VMEM((2, positions * kv_heads, head_dim), F32),
                pltpu.VMEM((2, 2, 2, half_heads, positions, head_dim), BF16),
                pltpu.VMEM((5, 2, rows, keys, head_dim), BF16),
                pltpu.VMEM((both, model_dim), BF16),
                pltpu.VMEM((tiles, both, TILE), F32),
                pltpu.VMEM((2, tiles, both, TILE), F32),
                pltpu.VMEM((both, q_width + 2 * kv_width), F32),
                pltpu.VMEM((half_heads, both * PAD, head_dim), F32),
                pltpu.VMEM((2, half_heads, both, head_dim), F32),
                pltpu.VMEM((half_heads, both * PAD, head_dim), F32),
                pltpu.VMEM((both, q_width), BF16),
                pltpu.VMEM((both, 2 * PAD, 128), jnp.int32),
                pltpu.VMEM((layers, 2, half_heads, rows, head_dim), BF16),
                pltpu.VMEM((layers, 2, half_heads, rows, head_dim), BF16),
                dma((2,)), dma((4, tiles // BLOCK)), dma((2,)), dma((3, 2)), dma((2,)), dma((2,)), dma((2, 2)), dma((layers, 3)), dma((layers, 3)),
                dma((tiles,)), dma((2, tiles)), dma((2,)), dma((3,)),
            ],
            compiler_params=pltpu.CompilerParams(collective_id=0, has_side_effects=True, vmem_limit_bytes=66_000_000),
            name="decode_layers",
        )(seq_lens.reshape(1, rows), hidden, w_query, w_key, w_value, w_out, k_pre, v_pre, k_flat, v_flat)

        hidden_out, k_out, v_out = pl.pallas_call(
            cache_kernel,
            out_shape=(jax.ShapeDtypeStruct(hidden.shape, BF16), jax.ShapeDtypeStruct(k_suffix.shape, BF16), jax.ShapeDtypeStruct(v_suffix.shape, BF16)),
            in_specs=[any_spec] * 5,
            out_specs=(any_spec, any_spec, any_spec),
            scratch_shapes=[
                pltpu.VMEM((layers, 2) + k_suffix.shape[1:], BF16),
                pltpu.VMEM((layers, 2, kv_heads * rows, head_dim), BF16),
                pltpu.VMEM((2, kv_heads * rows, head_dim), F32),
                pltpu.SMEM(seq_lens.shape, jnp.int32),
                pltpu.VMEM(hidden.shape, BF16),
                dma((layers, 2)), dma((layers, 2)), dma((layers,)), dma((3,)),
            ],
            compiler_params=pltpu.CompilerParams(vmem_limit_bytes=60_000_000),
            name="write_caches",
        )(seq_lens, kv_new.reshape(layers, 2, kv_heads * rows, head_dim), hidden_out, k_suffix, v_suffix)
        return hidden_out, k_out, v_out

    return jax.shard_map(local_step, mesh=mesh, in_specs=(row_spec, lens_spec, whole_spec, whole_spec, whole_spec, whole_spec, prefix_spec, prefix_spec, cache_spec, cache_spec), out_specs=(row_spec, cache_spec, cache_spec), check_vma=False)
```

```python
import functools

import jax
import jax.numpy as jnp
from jax import lax
from jax.experimental import pallas as pl
from jax.experimental.pallas import tpu as pltpu
from jax.sharding import PartitionSpec as P

MESH = pl.DeviceIdType.MESH
BF16 = jnp.bfloat16
F32 = jnp.float32
TILE = 512
CHUNK = 32
PAD = 8
WRITE_LAG = 8
BLOCK = 2
LOG2E = 1.4426950408889634
CHUNKS_PER_TRIP = 1


def decode_kernel(dims, lens_hbm, hidden_hbm, wq_ref, wk_ref, wv_ref, wo_ref, kpre_ref, vpre_ref, ksuf_ref, vsuf_ref,
                  out_ref, kv_out_ref,
                  lens_ref, hidden_ref, wq_buf, wk_buf, wv_buf, wo_first_buf, wo_buf, pre_buf, raw_buf, wide_buf, split_buf, suf_buf, x_buf, own_buf, recv_buf, acc_buf,
                  q_buf, kvn_buf, o_buf, att_buf, lens_buf, kv_mine_buf, kv_send_buf,
                  entry_sem, w_sem, wo_first_sem, suf_load_sem, suf_send_sem, suf_recv_sem, raw_sem, pre_send_sem, pre_recv_sem,
                  part_send_sem, part_recv_sem, lens_sem, kv_sem):
    layers, rows, group, head_dim, slots = dims
    half_heads = 2
    tiles = own_buf.shape[0]
    q_width = wq_buf.shape[1]
    kv_width = wk_buf.shape[1]
    blocks = [(i * BLOCK, (i + 1) * BLOCK if i < tiles // BLOCK - 1 else tiles) for i in range(tiles // BLOCK)]
    both = 2 * rows
    me = lax.axis_index("ctx")
    core = lax.rem(me, 2)
    chip = me // 2
    mate = chip * 2 + (1 - core)
    across = (1 - chip) * 2 + core
    diagonal = (1 - chip) * 2 + (1 - core)
    peers = ((mate, 1 - core), (across, core), (diagonal, 1 - core))
    mine = pl.multiple_of(core * rows, rows)
    other = pl.multiple_of((1 - core) * rows, rows)
    q_col = pl.multiple_of(core * q_width, 128)
    kv_col = pl.multiple_of(core * kv_width, 128)
    scale = head_dim ** -0.5

    def qkv_copies(layer, i):
        a, b = blocks[i]
        r = pl.ds(a * TILE, (b - a) * TILE)
        return (
            pltpu.make_async_copy(wq_ref.at[layer, r, pl.ds(q_col, q_width)], wq_buf.at[r], w_sem.at[0, i]),
            pltpu.make_async_copy(wk_ref.at[layer, r, pl.ds(kv_col, kv_width)], wk_buf.at[r], w_sem.at[1, i]),
            pltpu.make_async_copy(wv_ref.at[layer, r, pl.ds(kv_col, kv_width)], wv_buf.at[r], w_sem.at[2, i]),
        )

    def wo_copy(layer, i):
        a, b = blocks[i]
        src = wo_ref.at[layer, pl.ds(q_col, q_width), pl.ds(a * TILE, (b - a) * TILE)]
        if i == 0:
            return pltpu.make_async_copy(src, wo_first_buf.at[lax.rem(layer, 2)], wo_first_sem.at[lax.rem(layer, 2)])
        return pltpu.make_async_copy(src, wo_buf.at[:, pl.ds((a - BLOCK) * TILE, (b - a) * TILE)], w_sem.at[3, i])

    def suf_loads(layer):
        slot = lax.rem(layer, 3)
        return (
            pltpu.make_async_copy(ksuf_ref.at[layer], suf_buf.at[slot, 0], suf_load_sem.at[slot, 0]),
            pltpu.make_async_copy(vsuf_ref.at[layer], suf_buf.at[slot, 1], suf_load_sem.at[slot, 1]),
        )

    def suf_send(layer):
        return pltpu.make_async_remote_copy(
            src_ref=suf_buf.at[lax.rem(layer, 3)], dst_ref=suf_buf.at[3 + lax.rem(layer, 2)],
            send_sem=suf_send_sem.at[lax.rem(layer, 2)], recv_sem=suf_recv_sem.at[lax.rem(layer, 2)],
            device_id={"ctx": mate}, device_id_type=MESH)

    def raw_loads(layer):
        slot = lax.rem(layer, 2)
        return (
            pltpu.make_async_copy(kpre_ref.at[layer], raw_buf.at[slot, 0], raw_sem.at[slot, 0]),
            pltpu.make_async_copy(vpre_ref.at[layer], raw_buf.at[slot, 1], raw_sem.at[slot, 1]),
        )

    def split_prefix(layer):
        slot = lax.rem(layer, 2)
        heads = 2 * half_heads
        positions = pre_buf.shape[4]
        for copy in raw_loads(layer):
            copy.wait()
        for kv in range(2):
            wide_buf[kv] = raw_buf[slot, kv].astype(F32)
            for h in range(half_heads):
                for half in range(2):
                    split_buf[slot, half, kv, h] = wide_buf[kv, pl.ds(half * half_heads + h, positions, stride=heads), :].astype(BF16)
                pre_buf[layer, kv, h, me] = split_buf[slot, core, kv, h]

    def pre_remote(layer, k):
        device, half = peers[k]
        return pltpu.make_async_remote_copy(
            src_ref=split_buf.at[lax.rem(layer, 2), half], dst_ref=pre_buf.at[layer, :, :, me],
            send_sem=pre_send_sem.at[layer, k], recv_sem=pre_recv_sem.at[layer, k],
            device_id={"ctx": device}, device_id_type=MESH)

    def part_send(parity, j):
        return pltpu.make_async_remote_copy(
            src_ref=own_buf.at[j], dst_ref=recv_buf.at[parity, j],
            send_sem=part_send_sem.at[j], recv_sem=part_recv_sem.at[parity, j],
            device_id={"ctx": mate}, device_id_type=MESH)

    lens_send = pltpu.make_async_remote_copy(
        src_ref=lens_buf.at[pl.ds(mine, rows)], dst_ref=lens_buf.at[pl.ds(mine, rows)], send_sem=lens_sem.at[0], recv_sem=lens_sem.at[1],
        device_id={"ctx": mate}, device_id_type=MESH)
    kv_slice = kv_out_ref.at[:, :, pl.ds(core * half_heads, half_heads)]
    kv_store = pltpu.make_async_copy(kv_mine_buf, kv_slice, kv_sem.at[2])
    kv_send = pltpu.make_async_remote_copy(
        src_ref=kv_send_buf, dst_ref=kv_slice, send_sem=kv_sem.at[0], recv_sem=kv_sem.at[1],
        device_id={"ctx": mate}, device_id_type=MESH)

    barrier = pltpu.get_barrier_semaphore()
    for device, _ in peers:
        pl.semaphore_signal(barrier, inc=1, device_id={"ctx": device}, device_id_type=MESH)
    entry_copies = (pltpu.make_async_copy(hidden_hbm, hidden_ref, entry_sem.at[0]), pltpu.make_async_copy(lens_hbm, lens_ref, entry_sem.at[1]))
    for copy in entry_copies:
        copy.start()
    for layer in range(2):
        for copy in raw_loads(layer):
            copy.start()
    for i in range(len(blocks)):
        for copy in qkv_copies(0, i):
            copy.start()
        if i == 0:
            for copy in suf_loads(0):
                copy.start()
    for i in range(len(blocks)):
        wo_copy(0, i).start()
    for copy in suf_loads(1):
        copy.start()

    x_buf[...] = jnp.zeros_like(x_buf)
    q_buf[...] = jnp.zeros_like(q_buf)
    for copy in entry_copies:
        copy.wait()
    for j in range(tiles):
        own_buf[j] = jnp.zeros_like(own_buf[j])
        own_buf[j, pl.ds(mine, rows), :] = hidden_ref[:, j * TILE:(j + 1) * TILE].astype(F32)
    diagonal_hit = lax.broadcasted_iota(jnp.int32, (rows, rows), 0) == lax.broadcasted_iota(jnp.int32, (rows, rows), 1)
    lens_wide = jnp.broadcast_to(lens_ref[...].astype(F32), (rows, rows))
    lens_wide = jnp.where(diagonal_hit, lens_wide, 0.0).sum(axis=1, keepdims=True)
    lens_wide = jnp.broadcast_to(lens_wide, (rows, 128)).astype(jnp.int32)
    for b in range(rows):
        lens_buf[mine + b] = jnp.broadcast_to(lens_wide[b:b + 1, :], (2 * PAD, 128))
    split_prefix(0)
    for copy in raw_loads(2):
        copy.start()
    split_prefix(1)

    pl.semaphore_wait(barrier, 3)

    for j in range(tiles):
        part_send(1, j).start()
    lens_send.start()
    for layer in range(2):
        for k in range(3):
            pre_remote(layer, k).start()
    for copy in suf_loads(0):
        copy.wait()
    suf_send(0).start()
    lens_send.wait()

    row_ids = lax.broadcasted_iota(jnp.int32, (2 * PAD, 128), 0)
    key_ids = lax.broadcasted_iota(jnp.int32, (2 * PAD, 128), 1)
    key_slot = jnp.where(lax.rem(key_ids, 4) == 2 * core + row_ids // PAD, key_ids // 4, slots)[None]

    def await_part(parity, j):
        copy = part_send(parity, j)
        copy.wait_recv()
        copy.wait_send()

    def update_x(parity, j):
        update = (own_buf[j] + recv_buf[parity, j]).astype(BF16)
        cols = slice(j * TILE, (j + 1) * TILE)
        x_buf[:, cols] = (x_buf[:, cols].astype(F32) + update.astype(F32)).astype(BF16)

    def layer_body(layer, carry):
        parity_in = lax.rem(layer + 1, 2)
        parity_out = lax.rem(layer, 2)

        @pl.when(layer < layers - 3)
        def _():
            for copy in raw_loads(layer + 3):
                copy.start()

        for k in range(3):
            pre_remote(layer, k).wait_send()

        @pl.when(layer < layers - 2)
        def _():
            for copy in suf_loads(layer + 2):
                copy.start()
            split_prefix(layer + 2)

        for i, (a, b) in enumerate(blocks):
            if i == 0:
                for copy in qkv_copies(layer, 0):
                    copy.wait()
            if i + 1 < len(blocks):
                for copy in qkv_copies(layer, i + 1):
                    copy.wait()
            for j in range(a, b):
                await_part(parity_in, j)
            for j in range(a, b):
                update_x(parity_in, j)
            r = slice(a * TILE, b * TILE)
            x = x_buf[:, r]
            parts = ((slice(0, q_width), wq_buf), (slice(q_width, q_width + kv_width), wk_buf),
                     (slice(q_width + kv_width, q_width + 2 * kv_width), wv_buf))
            for cols, w_buf in parts:
                product = jnp.dot(x, w_buf[r, :], preferred_element_type=F32)
                acc_buf[:, cols] = product if i == 0 else acc_buf[:, cols] + product

            @pl.when(layer < layers - 1)
            def _():
                for copy in qkv_copies(layer + 1, i):
                    copy.start()
                if i == 0:
                    for copy in suf_loads(layer + 1):
                        copy.wait()
                    suf_send(layer + 1).start()

            if i == 0:
                @pl.when(layer < layers - 2)
                def _():
                    for k in range(3):
                        pre_remote(layer + 2, k).start()

        @pl.when(layer < layers - 1)
        def _():
            wo_copy(layer + 1, 0).start()

        for h in range(2):
            for g in range(group):
                col = (h * group + g) * head_dim
                q_buf[h, pl.ds(g, both, stride=PAD), :] = acc_buf[:, col:col + head_dim].astype(BF16).astype(F32)
            for kv in range(2):
                col = q_width + kv * kv_width + h * head_dim
                fresh = acc_buf[:, col:col + head_dim].astype(BF16).astype(F32)
                kvn_buf[kv, h] = fresh
        for h in range(2):
            for kv in range(2):
                kv_mine_buf[layer, kv, h] = kvn_buf[kv, h, pl.ds(mine, rows), :].astype(BF16)
                kv_send_buf[layer, kv, h] = kvn_buf[kv, h, pl.ds(other, rows), :].astype(BF16)

        for k in range(3):
            pre_remote(layer, k).wait_recv()
        suf_send(layer).wait()

        per_core = rows // CHUNK

        def unpair(both_seqs):
            first_seq = both_seqs[:, None, 0:2 * PAD, 0:128]
            second_seq = both_seqs[:, None, 2 * PAD:4 * PAD, 128:256]
            return jnp.concatenate([first_seq, second_seq], axis=1).reshape(CHUNK, 2 * PAD, 128)

        def attend(i):
            away = i // per_core
            part = pl.multiple_of(lax.rem(i, per_core) * CHUNK, CHUNK)
            first = pl.multiple_of(lax.rem(core + away, 2) * rows + part, CHUNK)
            slot = (1 - away) * lax.rem(layer, 3) + away * (3 + lax.rem(layer, 2))
            chunk_rows = pl.ds(pl.multiple_of(first * PAD, CHUNK * PAD), CHUNK * PAD)
            q_heads = [q_buf[h, chunk_rows, :] for h in range(2)]
            q3 = jnp.concatenate([q.reshape(CHUNK, PAD, head_dim) for q in q_heads], axis=1)
            k_suf = suf_buf[slot, 0, pl.ds(part, CHUNK)]
            v_suf = suf_buf[slot, 1, pl.ds(part, CHUNK)]
            q_pairs = q3.astype(BF16).reshape(CHUNK // 2, 4 * PAD, head_dim)
            k_pairs = k_suf.reshape(CHUNK // 2, 256, head_dim)
            suf_scores = unpair(lax.dot_general(q_pairs, k_pairs, (((2,), (2,)), ((0,), (0,))), preferred_element_type=F32))
            suf_scores = jnp.where(key_slot < lens_buf[pl.ds(first, CHUNK)], suf_scores, -jnp.inf)
            def spread(kv):
                picked = [jnp.broadcast_to(kvn_buf[kv, h, pl.ds(first + b, 1), :], (PAD, head_dim)) for b in range(CHUNK) for h in range(2)]
                return jnp.concatenate(picked, axis=0).reshape(CHUNK, 2 * PAD, head_dim)

            k_new = spread(0)
            v_new = spread(1)
            new_scores = jnp.sum(q3 * k_new, axis=-1, keepdims=True)
            suf_weights, new_weights, masses, pre_vals = [], [], [], []
            for h in range(2):
                hs = slice(h * PAD, (h + 1) * PAD)
                q_h = q_heads[h].astype(BF16)
                k_pre = pre_buf[layer, 0, h].reshape(-1, head_dim)
                v_pre = pre_buf[layer, 1, h].reshape(-1, head_dim)
                scores = lax.dot_general(q_h, k_pre, (((1,), (1,)), ((), ())), preferred_element_type=F32)
                suf_h = suf_scores[:, hs, :].reshape(CHUNK * PAD, 128)
                new_h = new_scores[:, hs, :].reshape(CHUNK * PAD, 1)
                peak = jnp.maximum(jnp.maximum(scores.max(axis=-1, keepdims=True), suf_h.max(axis=-1, keepdims=True)), new_h)
                pre_w = jnp.exp2((scores - peak) * (scale * LOG2E))
                suf_w = jnp.exp2((suf_h - peak) * (scale * LOG2E))
                new_w = jnp.exp2((new_h - peak) * (scale * LOG2E))
                masses.append(pre_w.sum(axis=-1, keepdims=True) + suf_w.sum(axis=-1, keepdims=True) + new_w)
                pre_vals.append(jnp.dot(pre_w.astype(BF16), v_pre, preferred_element_type=F32))
                suf_weights.append(suf_w.reshape(CHUNK, PAD, 128))
                new_weights.append(new_w)
            suf_w = jnp.concatenate(suf_weights, axis=1).astype(BF16)
            v_suf = v_suf.reshape(CHUNK // 2, 2, 128, head_dim)
            v_pairs = jnp.concatenate([v_suf[:, 0], v_suf[:, 1]], axis=-1)
            suf_w = suf_w.reshape(CHUNK // 2, 4 * PAD, 128)
            suf_vals = unpair(lax.dot_general(suf_w, v_pairs, (((2,), (1,)), ((0,), (0,))), preferred_element_type=F32))
            for h in range(2):
                hs = slice(h * PAD, (h + 1) * PAD)
                mixed = pre_vals[h] + suf_vals[:, hs, :].reshape(CHUNK * PAD, head_dim)
                mixed = mixed + new_weights[h] * v_new[:, hs, :].reshape(CHUNK * PAD, head_dim)
                o_buf[h, chunk_rows, :] = mixed / masses[h]

        def attend_trip(trip, carry):
            for i in range(CHUNKS_PER_TRIP):
                attend(trip * CHUNKS_PER_TRIP + i)
            return carry

        lax.fori_loop(0, 2 * per_core // CHUNKS_PER_TRIP, attend_trip, 0)

        @pl.when(layer == layers - 1)
        def _():
            kv_store.start()
            kv_send.start()

        wo_copy(layer, 0).wait()
        wo_copy(layer, 1).wait()

        for h in range(2):
            for g in range(group):
                col = (h * group + g) * head_dim
                att_buf[:, col:col + head_dim] = o_buf[h, pl.ds(g, both, stride=PAD), :].astype(BF16)

        for i, (a, b) in enumerate(blocks):
            if 0 < i < len(blocks) - 1:
                wo_copy(layer, i + 1).wait()
            weights = wo_first_buf[lax.rem(layer, 2)] if i == 0 else wo_buf[:, (a - BLOCK) * TILE:(b - BLOCK) * TILE]
            product = jnp.dot(att_buf[...], weights, preferred_element_type=F32)
            for j in range(a, b):
                own_buf[j] = product[:, (j - a) * TILE:(j - a + 1) * TILE]

            if i > 0:
                @pl.when(layer < layers - 1)
                def _():
                    wo_copy(layer + 1, i).start()

            for j in range(a, b):
                part_send(parity_out, j).start()

        return carry

    lax.fori_loop(0, layers, layer_body, 0)
    home = pl.ds(mine, rows)
    for j in range(tiles):
        parity = (layers - 1) % 2
        await_part(parity, j)
        cols = slice(j * TILE, (j + 1) * TILE)
        update = (own_buf[j, home, :] + recv_buf[parity, j, home, :]).astype(BF16)
        out_ref[:, cols] = (x_buf[home, cols].astype(F32) + update.astype(F32)).astype(BF16)
    kv_store.wait()
    kv_send.wait()


def cache_kernel(lens_hbm, new_ref, hidden_ref, k_ref, v_ref, hidden_out_ref, k_out_ref, v_out_ref,
                 buf, new_buf, wide_buf, lens_ref, hidden_buf, in_sem, out_sem, new_sem, hidden_sem):
    layers, rows, _, heads, _ = k_ref.shape

    def loads(layer):
        return (
            pltpu.make_async_copy(new_ref.at[layer], new_buf.at[layer], new_sem.at[layer]),
            pltpu.make_async_copy(k_ref.at[layer], buf.at[layer, 0], in_sem.at[layer, 0]),
            pltpu.make_async_copy(v_ref.at[layer], buf.at[layer, 1], in_sem.at[layer, 1]),
        )

    def stores(layer):
        return (
            pltpu.make_async_copy(buf.at[layer, 0], k_out_ref.at[layer], out_sem.at[layer, 0]),
            pltpu.make_async_copy(buf.at[layer, 1], v_out_ref.at[layer], out_sem.at[layer, 1]),
        )

    hidden_load = pltpu.make_async_copy(hidden_ref, hidden_buf, hidden_sem.at[0])
    hidden_store = pltpu.make_async_copy(hidden_buf, hidden_out_ref, hidden_sem.at[1])
    lens_load = pltpu.make_async_copy(lens_hbm, lens_ref, hidden_sem.at[2])
    for layer in range(layers):
        for copy in loads(layer):
            copy.start()
        if layer == 0:
            lens_load.start()
            hidden_load.start()
    lens_load.wait()

    def patch(layer, carry):
        for copy in loads(layer):
            copy.wait()
        for kv in range(2):
            wide_buf[kv] = new_buf[layer, kv].astype(F32)
            for b in range(rows):
                buf[layer, kv, b, lens_ref[b]] = wide_buf[kv, pl.ds(b, heads, stride=rows), :].astype(BF16)

        @pl.when(layer >= WRITE_LAG)
        def _():
            for copy in stores(layer - WRITE_LAG):
                copy.start()

        return carry

    lax.fori_loop(0, layers, patch, 0)
    for layer in range(layers - WRITE_LAG, layers):
        for copy in stores(layer):
            copy.start()
    hidden_load.wait()
    hidden_store.start()
    for layer in range(layers):
        for copy in stores(layer):
            copy.wait()
    hidden_store.wait()


def solution(mesh):
    home_axes = ('data', 'ctx')
    row_spec = P(home_axes, None)
    lens_spec = P(home_axes)
    whole_spec = P()
    prefix_spec = P(None, home_axes, None, None)
    cache_spec = P(None, home_axes, None, None, None)

    def local_step(hidden, seq_lens, w_query, w_key, w_value, w_out, k_prefix, v_prefix, k_suffix, v_suffix):
        layers, model_dim = w_query.shape[:2]
        positions, kv_heads, head_dim = k_prefix.shape[1:]
        rows = hidden.shape[0]
        slots = k_suffix.shape[2]
        group = w_query.shape[2] // head_dim // kv_heads
        half_heads = kv_heads // 2
        q_width = w_query.shape[2] // 2
        kv_width = w_key.shape[2] // 2
        tiles = model_dim // TILE
        keys = slots * kv_heads
        both = 2 * rows

        k_flat = k_suffix.reshape(layers, rows, keys, head_dim)
        v_flat = v_suffix.reshape(layers, rows, keys, head_dim)
        k_pre = k_prefix.reshape(layers, positions * kv_heads, head_dim)
        v_pre = v_prefix.reshape(layers, positions * kv_heads, head_dim)

        any_spec = pl.BlockSpec(memory_space=pl.ANY)
        vmem_spec = pl.BlockSpec(memory_space=pltpu.VMEM)
        dma = pltpu.SemaphoreType.DMA
        hidden_out, kv_new = pl.pallas_call(
            functools.partial(decode_kernel, (layers, rows, group, head_dim, slots)),
            out_shape=(jax.ShapeDtypeStruct((rows, model_dim), BF16),
                       jax.ShapeDtypeStruct((layers, 2, kv_heads, rows, head_dim), BF16)),
            in_specs=[any_spec] * 10,
            out_specs=(vmem_spec, any_spec),
            scratch_shapes=[
                pltpu.VMEM((1, rows), jnp.int32),
                pltpu.VMEM(hidden.shape, BF16),
                pltpu.VMEM((model_dim, q_width), BF16),
                pltpu.VMEM((model_dim, kv_width), BF16),
                pltpu.VMEM((model_dim, kv_width), BF16),
                pltpu.VMEM((2, q_width, BLOCK * TILE), BF16),
                pltpu.VMEM((q_width, model_dim - BLOCK * TILE), BF16),
                pltpu.VMEM((layers, 2, half_heads, 4, positions, head_dim), BF16),
                pltpu.VMEM((2, 2, positions * kv_heads, head_dim), BF16),
                pltpu.VMEM((2, positions * kv_heads, head_dim), F32),
                pltpu.VMEM((2, 2, 2, half_heads, positions, head_dim), BF16),
                pltpu.VMEM((5, 2, rows, keys, head_dim), BF16),
                pltpu.VMEM((both, model_dim), BF16),
                pltpu.VMEM((tiles, both, TILE), F32),
                pltpu.VMEM((2, tiles, both, TILE), F32),
                pltpu.VMEM((both, q_width + 2 * kv_width), F32),
                pltpu.VMEM((half_heads, both * PAD, head_dim), F32),
                pltpu.VMEM((2, half_heads, both, head_dim), F32),
                pltpu.VMEM((half_heads, both * PAD, head_dim), F32),
                pltpu.VMEM((both, q_width), BF16),
                pltpu.VMEM((both, 2 * PAD, 128), jnp.int32),
                pltpu.VMEM((layers, 2, half_heads, rows, head_dim), BF16),
                pltpu.VMEM((layers, 2, half_heads, rows, head_dim), BF16),
                dma((2,)), dma((4, tiles // BLOCK)), dma((2,)), dma((3, 2)), dma((2,)), dma((2,)), dma((2, 2)), dma((layers, 3)), dma((layers, 3)),
                dma((tiles,)), dma((2, tiles)), dma((2,)), dma((3,)),
            ],
            compiler_params=pltpu.CompilerParams(collective_id=0, has_side_effects=True, vmem_limit_bytes=66_000_000),
            name="decode_layers",
        )(seq_lens.reshape(1, rows), hidden, w_query, w_key, w_value, w_out, k_pre, v_pre, k_flat, v_flat)

        hidden_out, k_out, v_out = pl.pallas_call(
            cache_kernel,
            out_shape=(jax.ShapeDtypeStruct(hidden.shape, BF16), jax.ShapeDtypeStruct(k_suffix.shape, BF16), jax.ShapeDtypeStruct(v_suffix.shape, BF16)),
            in_specs=[any_spec] * 5,
            out_specs=(any_spec, any_spec, any_spec),
            scratch_shapes=[
                pltpu.VMEM((layers, 2) + k_suffix.shape[1:], BF16),
                pltpu.VMEM((layers, 2, kv_heads * rows, head_dim), BF16),
                pltpu.VMEM((2, kv_heads * rows, head_dim), F32),
                pltpu.SMEM(seq_lens.shape, jnp.int32),
                pltpu.VMEM(hidden.shape, BF16),
                dma((layers, 2)), dma((layers, 2)), dma((layers,)), dma((3,)),
            ],
            compiler_params=pltpu.CompilerParams(vmem_limit_bytes=60_000_000),
            name="write_caches",
        )(seq_lens, kv_new.reshape(layers, 2, kv_heads * rows, head_dim), hidden_out, k_suffix, v_suffix)
        return hidden_out, k_out, v_out

    return jax.shard_map(local_step, mesh=mesh, in_specs=(row_spec, lens_spec, whole_spec, whole_spec, whole_spec, whole_spec, prefix_spec, prefix_spec, cache_spec, cache_spec), out_specs=(row_spec, cache_spec, cache_spec), check_vma=False)
```
